8 devices in a mesh: rep: 2 (over z, y), ep: 4 (over x, core).
Axes of the slice: x: 2, y: 2, z: 1, core: 2. Of those that a mesh axis runs over, the one named last changes fastest.
Arguments:
- x: bfloat16 [1024, 2048], P(('rep', 'ep')), parts along dimension 0
- cache: bfloat16 [1024, 256, 576], P(('rep', 'ep')), parts along dimension 0
- lens: int32 [1024], P(('rep', 'ep')), parts along dimension 0
- ids: int32 [1024, 6], P(('rep', 'ep')), parts along dimension 0
- rw: float32 [1024, 6], P(('rep', 'ep')), parts along dimension 0
- w_q: bfloat16 [2048, 3072], replicated
- w_dkv: bfloat16 [2048, 576], replicated
- w_uk: bfloat16 [16, 128, 512], replicated
- w_uv: bfloat16 [16, 512, 128], replicated
- w_o: bfloat16 [2048, 2048], replicated
- s_gate: bfloat16 [2048, 2816], replicated
- s_up: bfloat16 [2048, 2816], replicated
- s_down: bfloat16 [2816, 2048], replicated
- e_gate: bfloat16 [64, 2048, 1408], P('ep')
- e_up: bfloat16 [64, 2048, 1408], P('ep')
- e_down: bfloat16 [64, 1408, 2048], P('ep')
Outputs:
- output 1: bfloat16 [1024, 2048], P(('rep', 'ep')), parts along dimension 0
- output 2: bfloat16 [1024, 576], P(('rep', 'ep')), parts along dimension 0
There are 2 independent parts. The reference program is written for one: setup_inputs(seed, part) draws one part's arguments, and reference() takes and returns one part's arrays. A program takes and returns all parts, laid end to end along the dimension named above; an argument that names none is the same for every part.
All inputs are finite; a program needn't handle non-finite values.
Results may differ from the reference program's by a relative error of at most 0.0118975.
Values are sent between devices in bfloat16 or wider.
A program may use at most 1.5 GiB of HBM per device.

```python
import jax
import jax.numpy as jnp
from jax import lax

EP = 4
B_DEV = 128
L_MAX = 256
H = 2048
HEADS = 16
KV_LORA = 512
ROPE = 64
NOPE = 128
VHEAD = 128
EXPERTS = 64
TOP = 6
INTER = 1408
SHARED = 2816

B = EP * B_DEV
KVD = KV_LORA + ROPE
QKD = NOPE + ROPE
LEN_LO = (3 * L_MAX) // 4
EPS = 1e-6
ROPE_BASE = 1.0e4


def rms(v):
    v = v.astype(jnp.float32)
    return v * lax.rsqrt(jnp.mean(v * v, axis=-1, keepdims=True) + EPS)


def rope(v, pos):
    half = v.shape[-1] // 2
    inv = ROPE_BASE ** (-2.0 * jnp.arange(half, dtype=jnp.float32) / v.shape[-1])
    ang = pos.astype(jnp.float32)[..., None] * inv
    cs = jnp.cos(ang)
    sn = jnp.sin(ang)
    v1 = v[..., :half]
    v2 = v[..., half:]
    return jnp.concatenate([v1 * cs - v2 * sn, v2 * cs + v1 * sn], axis=-1)


def swiglu(u, wg, wu, wd):
    g = jnp.dot(u, wg, preferred_element_type=jnp.float32)
    v = jnp.dot(u, wu, preferred_element_type=jnp.float32)
    return jnp.dot((jax.nn.silu(g) * v).astype(jnp.bfloat16), wd, preferred_element_type=jnp.float32)


def setup_inputs(seed: int = 0, part: int = 0) -> dict:
    kbase = jax.random.fold_in(jax.random.key(seed), part)
    kp = jax.random.split(kbase, 8)
    kd = jax.random.split(jax.random.fold_in(kbase, 7), 3)
    kw = jax.random.split(jax.random.key(seed + 1), 11)

    def draw(k, shape, fan):
        return (jax.random.normal(k, shape, jnp.float32) * fan ** -0.5).astype(jnp.bfloat16)

    x = jax.random.normal(kp[0], (B, H), jnp.float32).astype(jnp.bfloat16)
    span = (L_MAX - LEN_LO) // 8
    dev = jnp.arange(B) // B_DEV
    low = jax.random.randint(kd[0], (B,), LEN_LO, LEN_LO + span)
    high = jax.random.randint(kd[1], (B,), L_MAX - span, L_MAX)
    lens = jnp.where(dev % 2 == 0, low, high).astype(jnp.int32)
    pos = jnp.arange(L_MAX)[None, :, None]
    m_live = 0.7 * jax.random.normal(kp[2], (B, 1, KVD), jnp.float32)
    m_old = 0.7 * jax.random.normal(kp[3], (B, 1, KVD), jnp.float32)
    noise = jax.random.normal(kp[4], (B, L_MAX, KVD), jnp.float32)
    cache = (jnp.where(pos < lens[:, None, None], m_live, m_old) + noise).astype(jnp.bfloat16)

    def route(k):
        k1, k2 = jax.random.split(k)
        perm_e = jax.random.permutation(k1, EXPERTS)
        perm_t = jax.random.permutation(k2, B_DEV)
        j = jnp.arange(B_DEV)[:, None] * TOP + jnp.arange(TOP)[None, :]
        return perm_e[j % (EXPERTS // 2)][perm_t]

    ids = jax.vmap(route)(jax.random.split(kd[2], EP)).reshape(B, TOP).astype(jnp.int32)
    rw = jax.random.uniform(kp[6], (B, TOP), jnp.float32, 0.5, 1.5) * TOP ** -0.5
    return {
        'x': x,
        'cache': cache,
        'lens': lens,
        'ids': ids,
        'rw': rw,
        'w_q': draw(kw[0], (H, HEADS * QKD), H),
        'w_dkv': draw(kw[1], (H, KVD), H),
        'w_uk': draw(kw[2], (HEADS, NOPE, KV_LORA), NOPE),
        'w_uv': draw(kw[3], (HEADS, KV_LORA, VHEAD), KV_LORA),
        'w_o': draw(kw[4], (HEADS * VHEAD, H), HEADS * VHEAD),
        's_gate': draw(kw[5], (H, SHARED), H),
        's_up': draw(kw[6], (H, SHARED), H),
        's_down': draw(kw[7], (SHARED, H), SHARED),
        'e_gate': draw(kw[8], (EXPERTS, H, INTER), H),
        'e_up': draw(kw[9], (EXPERTS, H, INTER), H),
        'e_down': draw(kw[10], (EXPERTS, INTER, H), INTER),
    }


def reference(x, cache, lens, ids, rw, w_q, w_dkv, w_uk, w_uv, w_o, s_gate, s_up, s_down, e_gate, e_up, e_down):
    xn = rms(x).astype(jnp.bfloat16)
    q = jnp.dot(xn, w_q, preferred_element_type=jnp.float32).astype(jnp.bfloat16).reshape(B, HEADS, QKD)
    kv = jnp.dot(xn, w_dkv, preferred_element_type=jnp.float32)
    kv_new = jnp.concatenate([rms(kv[:, :KV_LORA]), rope(kv[:, KV_LORA:], lens)], axis=-1).astype(jnp.bfloat16)
    q_lat = jnp.einsum('bhd,hdc->bhc', q[:, :, :NOPE].astype(jnp.float32), w_uk.astype(jnp.float32)).astype(jnp.bfloat16)
    q_rot = rope(q[:, :, NOPE:].astype(jnp.float32), lens[:, None]).astype(jnp.bfloat16)
    qf = jnp.concatenate([q_lat, q_rot], axis=-1)
    scale = QKD ** -0.5

    def attend(args):
        qb, cb, kb, lb = args
        qs = qb.astype(jnp.float32)
        cs = cb.astype(jnp.float32)
        ks = kb.astype(jnp.float32)
        s = jnp.dot(qs, cs.T) * scale
        s = jnp.where(jnp.arange(L_MAX)[None, :] < lb, s, -jnp.inf)
        s_new = jnp.dot(qs, ks) * scale
        mx = jnp.maximum(jnp.max(s, axis=1), s_new)
        e = jnp.exp(s - mx[:, None])
        e_new = jnp.exp(s_new - mx)
        den = jnp.sum(e, axis=1) + e_new
        p = (e / den[:, None]).astype(jnp.bfloat16).astype(jnp.float32)
        p_new = (e_new / den).astype(jnp.bfloat16).astype(jnp.float32)
        o = jnp.dot(p, cs[:, :KV_LORA]) + p_new[:, None] * ks[None, :KV_LORA]
        return o.astype(jnp.bfloat16)

    o_lat = lax.map(attend, (qf, cache, kv_new, lens))
    o = jnp.einsum('bhc,hcv->bhv', o_lat.astype(jnp.float32), w_uv.astype(jnp.float32)).astype(jnp.bfloat16).reshape(B, HEADS * VHEAD)
    a = jnp.dot(o, w_o, preferred_element_type=jnp.float32)
    h1 = (x.astype(jnp.float32) + a).astype(jnp.bfloat16)
    u = rms(h1).astype(jnp.bfloat16)
    shared = swiglu(u, s_gate, s_up, s_down)
    gate_w = jnp.sum(jnp.where(ids[:, :, None] == jnp.arange(EXPERTS)[None, None, :], rw[:, :, None], 0.0), axis=1)

    def expert(acc, args):
        wg, wu, wd, cw = args
        out = swiglu(u, wg, wu, wd).astype(jnp.bfloat16).astype(jnp.float32)
        return acc + cw[:, None] * out, None

    routed, _ = lax.scan(expert, jnp.zeros((B, H), jnp.float32), (e_gate, e_up, e_down, gate_w.T))
    y = (h1.astype(jnp.float32) + shared + routed).astype(jnp.bfloat16)
    return y, kv_new
```

```python
import functools

import jax
import jax.numpy as jnp
from jax import lax
from jax.experimental import pallas as pl
from jax.experimental.pallas import tpu as pltpu
from jax.sharding import PartitionSpec as P

EPS = 1e-6
ROPE_BASE = 1.0e4
CAP = 32
COLS = 512
DOWN_SLOTS = 3


def rms(v):
    v = v.astype(jnp.float32)
    return v * lax.rsqrt(jnp.mean(v * v, axis=-1, keepdims=True) + EPS)


def rope(v, pos):
    half = v.shape[-1] // 2
    inv = ROPE_BASE ** (-2.0 * jnp.arange(half, dtype=jnp.float32) / v.shape[-1])
    ang = pos.astype(jnp.float32)[..., None] * inv
    cs = jnp.cos(ang)
    sn = jnp.sin(ang)
    v1 = v[..., :half]
    v2 = v[..., half:]
    return jnp.concatenate([v1 * cs - v2 * sn, v2 * cs + v1 * sn], axis=-1)


def attention(x, cache, lens, w_q, w_dkv, w_uk, w_uv, w_o):
    bsz = x.shape[0]
    heads, nope, kvl = w_uk.shape
    kvd = cache.shape[2]
    vh = w_uv.shape[2]
    qkd = nope + kvd - kvl
    xn = rms(x).astype(jnp.bfloat16)
    q = jnp.dot(xn, w_q, preferred_element_type=jnp.float32).astype(jnp.bfloat16).reshape(bsz, heads, qkd)
    kv = jnp.dot(xn, w_dkv, preferred_element_type=jnp.float32)
    kv_new = jnp.concatenate([rms(kv[:, :kvl]), rope(kv[:, kvl:], lens)], axis=-1).astype(jnp.bfloat16)
    q_lat = jnp.einsum('bhd,hdc->bhc', q[:, :, :nope], w_uk, preferred_element_type=jnp.float32).astype(jnp.bfloat16)
    q_rot = rope(q[:, :, nope:].astype(jnp.float32), lens[:, None]).astype(jnp.bfloat16)
    qf = jnp.concatenate([q_lat, q_rot], axis=-1)
    scale = qkd ** -0.5
    s = jnp.einsum('bhc,blc->bhl', qf, cache, preferred_element_type=jnp.float32) * scale
    live = jnp.arange(cache.shape[1])[None, None, :] < lens[:, None, None]
    s = jnp.where(live, s, -jnp.inf)
    s_new = jnp.einsum('bhc,bc->bh', qf, kv_new, preferred_element_type=jnp.float32) * scale
    mx = jnp.maximum(jnp.max(s, axis=2), s_new)
    e = jnp.exp(s - mx[:, :, None])
    e_new = jnp.exp(s_new - mx)
    den = jnp.sum(e, axis=2) + e_new
    p = (e / den[:, :, None]).astype(jnp.bfloat16)
    p_new = (e_new / den).astype(jnp.bfloat16)
    o_all = jnp.einsum('bhl,blc->bhc', p, cache, preferred_element_type=jnp.float32)
    o_lat = (o_all[:, :, :kvl] + p_new.astype(jnp.float32)[:, :, None] * kv_new[:, None, :kvl].astype(jnp.float32)).astype(jnp.bfloat16)
    o = jnp.einsum('bhc,hcv->bhv', o_lat, w_uv, preferred_element_type=jnp.float32).astype(jnp.bfloat16).reshape(bsz, heads * vh)
    a = jnp.dot(o, w_o, preferred_element_type=jnp.float32)
    return (x.astype(jnp.float32) + a).astype(jnp.bfloat16), kv_new


def dot(a, b):
    return jnp.dot(a, b, preferred_element_type=jnp.float32)


def moe_kernel(u_ref, h1_ref, meta_ref, sg, su, sd, eg, eu, ed, y_ref,
               gbuf, ubuf, dbuf, xall, act, sact, gate, outc, comb, uall, mall, s1, r1, s2, r2, own, shf,
               gsem, usem, dsem, us_send, us_recv, ms_send, ms_recv, s1_send, s1_recv, s2_send, s2_recv):
    n_loc = eg.shape[0]
    bsz, hid = u_ref.shape
    inter = eg.shape[2]
    n_col = hid // COLS
    pairs = n_loc // 2
    n_down = n_col * pairs
    half = bsz // 2
    me = lax.axis_index('ep')
    partner = {'ep': me + 1 - 2 * lax.rem(me, 2)}
    across = {'ep': lax.rem(me + 2, 4)}

    def gate_copy(e, slot):
        return pltpu.make_async_copy(eg.at[e], gbuf.at[slot], gsem.at[slot])

    def up_copy(e, slot):
        return pltpu.make_async_copy(eu.at[e], ubuf.at[slot], usem.at[slot])

    def sgate_copy(i):
        return pltpu.make_async_copy(sg.at[:, pl.ds(i * inter, inter)], gbuf.at[i], gsem.at[i])

    def sup_copy(i):
        return pltpu.make_async_copy(su.at[:, pl.ds(i * inter, inter)], ubuf.at[i], usem.at[i])

    def down_copy(j, slot):
        c = j // pairs
        e = lax.rem(j, pairs)
        return pltpu.make_async_copy(
            ed.at[pl.ds(2 * e, 2), :, pl.ds(pl.multiple_of(c * COLS, COLS), COLS)], dbuf.at[slot], dsem.at[slot])

    def sdown_copy(c, slot):
        return pltpu.make_async_copy(sd.at[:, :, pl.ds(c * COLS, COLS)], dbuf.at[slot], dsem.at[slot])

    def remote(src, dst, send, recv, dev):
        return pltpu.make_async_remote_copy(src_ref=src, dst_ref=dst, send_sem=send, recv_sem=recv,
                                            device_id=dev, device_id_type=pl.DeviceIdType.MESH)

    for i in range(2):
        sgate_copy(i).start()
        sup_copy(i).start()

    barrier = pltpu.get_barrier_semaphore()
    for dev in (partner, across):
        pl.semaphore_signal(barrier, inc=1, device_id=dev, device_id_type=pl.DeviceIdType.MESH)
    pl.semaphore_wait(barrier, 2)

    m_across = remote(meta_ref, mall.at[1], ms_send.at[1], ms_recv.at[1], across)
    u_across = [remote(u_ref.at[pl.ds(i * half, half)], uall.at[1, pl.ds(i * half, half)],
                       us_send.at[1 + i], us_recv.at[1 + i], across) for i in range(2)]
    m_partner = remote(meta_ref, mall.at[0], ms_send.at[0], ms_recv.at[0], partner)
    u_partner = remote(u_ref, uall.at[0], us_send.at[0], us_recv.at[0], partner)
    m_relay = remote(mall.at[1], mall.at[2], ms_send.at[2], ms_recv.at[2], partner)
    u_relay = [remote(uall.at[1, pl.ds(i * half, half)], uall.at[2, pl.ds(i * half, half)],
                      us_send.at[3 + i], us_recv.at[3 + i], partner) for i in range(2)]
    m_across.start()
    u_across[0].start()
    u_across[1].start()
    m_partner.start()
    u_partner.start()

    def glu(lhs, e, slot, dst, g_wait, u_wait, g_next, u_next):
        g_wait.wait()
        gate[...] = dot(lhs, gbuf[slot])
        g_next()
        u_wait.wait()
        v = dot(lhs, ubuf[slot])
        dst[...] = (jax.nn.silu(gate[...]) * v).astype(jnp.bfloat16)
        u_next()

    for i in range(2):
        glu(u_ref[...], i, i, sact.at[i], sgate_copy(i), sup_copy(i),
            lambda: gate_copy(i, i).start(), lambda: up_copy(i, i).start())

    for j in range(DOWN_SLOTS):
        down_copy(j, j).start()

    def dispatch(q, m, u):
        first = (me * n_loc).astype(jnp.float32)
        mine = lax.broadcasted_iota(jnp.int32, (n_loc, bsz), 0).astype(jnp.float32) + first
        hit = jnp.zeros((n_loc, bsz), jnp.float32)
        wgt = jnp.zeros((n_loc, bsz), jnp.float32)
        for k in range(6):
            eq = m[k:k + 1, :] == mine
            hit = jnp.where(eq, 1.0, hit)
            wgt = jnp.where(eq, m[8 + k:9 + k, :], wgt)
        row = lax.broadcasted_iota(jnp.int32, (bsz, bsz), 0)
        col = lax.broadcasted_iota(jnp.int32, (bsz, bsz), 1)
        low = jnp.where(row < col, 1.0, 0.0).astype(jnp.bfloat16)
        rank = jnp.where(hit > 0.0, dot(hit.astype(jnp.bfloat16), low), -1.0)
        slot = lax.broadcasted_iota(jnp.int32, (CAP, bsz), 0).astype(jnp.float32)
        sel = []
        ct = []
        for e in range(n_loc):
            at = slot == rank[e:e + 1, :]
            sel.append(jnp.where(at, 1.0, 0.0).astype(jnp.bfloat16))
            ct.append(jnp.where(at, wgt[e:e + 1, :], 0.0))
        c0 = jnp.concatenate(ct, axis=0).T
        for i in range(3):
            ci = c0.astype(jnp.bfloat16)
            comb[q, pl.ds(i * bsz, bsz), :] = ci
            c0 = c0 - ci.astype(jnp.float32)
        xall[q] = dot(jnp.concatenate(sel, axis=0), u).astype(jnp.bfloat16)

    dispatch(0, meta_ref[...], u_ref[...])
    m_partner.wait_recv()
    u_partner.wait_recv()
    dispatch(1, mall[0], uall[0])
    m_across.wait_recv()
    m_relay.start()
    for i in range(2):
        u_across[i].wait_recv()
        u_relay[i].start()
    dispatch(2, mall[1], uall[1])
    m_relay.wait_recv()
    for i in range(2):
        u_relay[i].wait_recv()
    dispatch(3, mall[2], uall[2])

    def expert(e, _):
        slot = lax.rem(e, 2)
        lhs = xall[:, pl.ds(pl.multiple_of(e * CAP, CAP), CAP), :].reshape(4 * CAP, hid)

        def g_next():
            @pl.when(e < n_loc - 2)
            def _():
                gate_copy(e + 2, slot).start()

        def u_next():
            @pl.when(e < n_loc - 2)
            def _():
                up_copy(e + 2, slot).start()

        glu(lhs, e, slot, act.at[e], gate_copy(e, slot), up_copy(e, slot), g_next, u_next)
        return 0

    lax.fori_loop(0, n_loc, expert, 0)

    def ring1(c):
        return remote(s1.at[c], r1.at[c], s1_send.at[c], s1_recv.at[c], partner)

    def ring2(c):
        return remote(s2.at[c], r2.at[c], s2_send.at[c], s2_recv.at[c], across)

    def fold(c):
        ring1(c).wait_recv()
        s2[c] = s2[c] + r1[c, 1]
        own[c] = own[c] + r1[c, 0]

    def down_step(j, c, e):
        slot = lax.rem(j, DOWN_SLOTS)
        down_copy(j, slot).wait()
        for i in range(2):
            res = dot(act[2 * e + i], dbuf[slot, i]).astype(jnp.bfloat16)
            outc[:, pl.ds(pl.multiple_of((2 * e + i) * CAP, CAP), CAP), :] = res.reshape(4, CAP, COLS)

        @pl.when(j + DOWN_SLOTS < n_down)
        def _():
            down_copy(j + DOWN_SLOTS, slot).start()

    def combine(q):
        p = dot(comb[q], outc[q])
        return p[:bsz] + p[bsz:2 * bsz] + p[2 * bsz:]

    def column(c, _):
        def step(e, _):
            down_step(c * pairs + e, c, e)

            @pl.when((c > 0) & (e == 2))
            def _():
                fold(c - 1)

            @pl.when((c > 0) & (e == 3))
            def _():
                ring2(c - 1).start()
            return 0

        lax.fori_loop(0, pairs, step, 0)
        s1[c, 1] = combine(3)
        s1[c, 0] = combine(1)
        s2[c] = combine(2)
        own[c] = combine(0)
        ring1(c).start()
        return 0

    lax.fori_loop(0, n_col, column, 0)

    for c in range(min(DOWN_SLOTS, n_col)):
        sdown_copy(c, (n_down + c) % DOWN_SLOTS).start()
    for c in range(n_col):
        slot = (n_down + c) % DOWN_SLOTS
        sdown_copy(c, slot).wait()
        shf[c] = dot(sact[0], dbuf[slot, 0]) + dot(sact[1], dbuf[slot, 1])
        if c + DOWN_SLOTS < n_col:
            sdown_copy(c + DOWN_SLOTS, slot).start()
        if c == 0:
            fold(n_col - 1)
        if c == 1:
            ring2(n_col - 1).start()

    for c in range(n_col):
        ring2(c).wait_recv()
        cols = pl.ds(c * COLS, COLS)
        y = h1_ref[:, cols].astype(jnp.float32) + shf[c] + (own[c] + r2[c])
        y_ref[:, cols] = y.astype(jnp.bfloat16)

    for copy in (m_across, *u_across, m_partner, u_partner, m_relay, *u_relay):
        copy.wait_send()
    for c in range(n_col):
        ring1(c).wait_send()
        ring2(c).wait_send()


def moe(u, h1, meta, s_gate, s_up, s_down, e_gate, e_up, e_down):
    bsz, hid = u.shape
    n_loc, _, inter = e_gate.shape
    n_col = hid // COLS
    bf16, f32 = jnp.bfloat16, jnp.float32
    vm = pl.BlockSpec(memory_space=pltpu.VMEM)
    hbm = pl.BlockSpec(memory_space=pl.ANY)
    dma = pltpu.SemaphoreType.DMA
    return pl.pallas_call(
        moe_kernel,
        out_shape=jax.ShapeDtypeStruct((bsz, hid), bf16),
        in_specs=[vm] * 3 + [hbm] * 6,
        out_specs=vm,
        scratch_shapes=[
            pltpu.VMEM((2, hid, inter), bf16),
            pltpu.VMEM((2, hid, inter), bf16),
            pltpu.VMEM((DOWN_SLOTS, 2, inter, COLS), bf16),
            pltpu.VMEM((4, n_loc * CAP, hid), bf16),
            pltpu.VMEM((n_loc, 4 * CAP, inter), bf16),
            pltpu.VMEM((2, bsz, inter), bf16),
            pltpu.VMEM((bsz, inter), f32),
            pltpu.VMEM((4, n_loc * CAP, COLS), bf16),
            pltpu.VMEM((4, 3 * bsz, n_loc * CAP), bf16),
            pltpu.VMEM((3, bsz, hid), bf16),
            pltpu.VMEM((3, 16, bsz), f32),
            pltpu.VMEM((n_col, 2, bsz, COLS), f32),
            pltpu.VMEM((n_col, 2, bsz, COLS), f32),
            pltpu.VMEM((n_col, bsz, COLS), f32),
            pltpu.VMEM((n_col, bsz, COLS), f32),
            pltpu.VMEM((n_col, bsz, COLS), f32),
            pltpu.VMEM((n_col, bsz, COLS), f32),
            dma((2,)), dma((2,)), dma((DOWN_SLOTS,)),
            dma((5,)), dma((5,)), dma((3,)), dma((3,)),
            dma((n_col,)), dma((n_col,)), dma((n_col,)), dma((n_col,)),
        ],
        compiler_params=pltpu.CompilerParams(
            collective_id=0, has_side_effects=True, vmem_limit_bytes=67043328),
        name='moe',
    )(u, h1, meta, s_gate, s_up, s_down.reshape(2, inter, hid), e_gate, e_up, e_down)


def solution(mesh):
    tok_spec = P(('rep', 'ep'))
    row_spec = P(('rep', 'ep'), None)
    cache_spec = P(('rep', 'ep'), None, None)
    exp_spec = P('ep', None, None)

    def local(x, cache, lens, ids, rw, w_q, w_dkv, w_uk, w_uv, w_o, s_gate, s_up, s_down, e_gate, e_up, e_down):
        h1, kv_new = attention(x, cache, lens, w_q, w_dkv, w_uk, w_uv, w_o)
        u = rms(h1).astype(jnp.bfloat16)
        meta = jnp.concatenate([jnp.pad(ids.astype(jnp.float32), ((0, 0), (0, 2))), jnp.pad(rw, ((0, 0), (0, 2)))], axis=1).T
        y = moe(u, h1, meta, s_gate, s_up, s_down, e_gate, e_up, e_down)
        return y, kv_new

    in_specs = (row_spec, cache_spec, tok_spec, row_spec, row_spec) + (P(),) * 8 + (exp_spec,) * 3
    return jax.shard_map(local, mesh=mesh, in_specs=in_specs, out_specs=(row_spec, row_spec), check_vma=False)
```

```python
import jax
import jax.numpy as jnp
from jax import lax
from jax.experimental import pallas as pl
from jax.experimental.pallas import tpu as pltpu
from jax.sharding import PartitionSpec as P

EPS = 1e-6
ROPE_BASE = 1.0e4
CAP = 32
COLS = 512
DOWN_SLOTS = 3
GROUP = 8
CACHE_SLOTS = 6
Q_PARTS = 4


def dot(a, b):
    return jnp.dot(a, b, preferred_element_type=jnp.float32)


def attn_kernel(lens_ref, x_ref, tab_ref, cache, wq, wdkv, wuk, wuv, wo, h1_ref, u_ref, kv_ref,
                cbuf, qbuf, dkvbuf, ukbuf, uvbuf, obuf, qf, kvr, sbuf, ol, oall,
                csem, qsem, wsem):
    bsz, hid = x_ref.shape
    heads, nope, lat = wuk.shape
    kvd, rows = cache.shape[1], cache.shape[2]
    rot = kvd - lat
    vh = wuv.shape[2]
    qkd = nope + rot
    steps = bsz // GROUP
    part = heads * qkd // Q_PARTS
    scale = qkd ** -0.5
    f32, bf16 = jnp.float32, jnp.bfloat16

    def c_copy(i, slot):
        return pltpu.make_async_copy(cache.at[pl.ds(i * GROUP, GROUP)], cbuf.at[slot], csem.at[slot])

    q_copies = [pltpu.make_async_copy(wq.at[:, pl.ds(i * part, part)], qbuf.at[i], qsem.at[i]) for i in range(Q_PARTS)]
    dkv_copy = pltpu.make_async_copy(wdkv, dkvbuf, wsem.at[0])
    uk_copy = pltpu.make_async_copy(wuk, ukbuf, wsem.at[1])
    uv_copy = pltpu.make_async_copy(wuv, uvbuf, wsem.at[2])
    o_copy = pltpu.make_async_copy(wo, obuf, wsem.at[3])
    dkv_copy.start()
    uk_copy.start()
    for copy in q_copies:
        copy.start()
    for i in range(CACHE_SLOTS):
        c_copy(i, i).start()
    uv_copy.start()
    o_copy.start()

    x = x_ref[...].astype(f32)
    xn = (x * lax.rsqrt(jnp.mean(x * x, axis=-1, keepdims=True) + EPS)).astype(bf16)
    cos_t = tab_ref[:rot // 2]
    sin_t = tab_ref[rot // 2:]
    cos = jnp.concatenate([cos_t] * 4, axis=0).T
    sin = jnp.concatenate([-sin_t, sin_t] * 2, axis=0).T

    dkv_copy.wait()
    kv = lax.dot_general(dkvbuf[...], xn, (((1,), (1,)), ((), ())), preferred_element_type=f32)
    c = kv[:lat]
    c = c * lax.rsqrt(jnp.mean(c * c, axis=0, keepdims=True) + EPS)
    v1 = kv[lat:lat + rot // 2]
    v2 = kv[lat + rot // 2:]
    kv = jnp.concatenate([c, v1 * cos_t - v2 * sin_t, v2 * cos_t + v1 * sin_t], axis=0).astype(bf16)
    kv_ref[...] = kv
    kvr[...] = jnp.concatenate([kv.astype(f32), jnp.zeros((kvr.shape[1] - kvd, bsz), f32)], axis=0).T

    uk_copy.wait()
    lane = lax.broadcasted_iota(jnp.int32, (bsz, 2 * rot), 1)
    for i in range(Q_PARTS):
        q_copies[i].wait()
        q = dot(xn, qbuf[i]).astype(bf16).astype(f32)
        for j in range(part // (2 * qkd)):
            at = 2 * qkd * j
            h = i * (part // qkd) + 2 * j
            mid = q[:, at + nope:at + 2 * nope]
            last = q[:, at + 2 * nope:at + 3 * nope]
            low = lane < rot
            flip = pltpu.roll(mid, rot, 1)
            n_a = q[:, at:at + nope]
            n_b = jnp.where(low, flip, pltpu.roll(last, rot, 1))
            r = jnp.where(low, mid, last)
            swap = jnp.where(lax.rem(lane, rot) < rot // 2, pltpu.roll(r, 2 * rot - rot // 2, 1), pltpu.roll(r, rot // 2, 1))
            r = (r * cos + swap * sin).astype(bf16).astype(f32)
            for k, n, z in ((0, n_a, r), (1, n_b, pltpu.roll(r, rot, 1))):
                to = pl.ds(h + k, bsz, stride=heads)
                ql = dot(n.astype(bf16), ukbuf[h + k]).astype(bf16).astype(f32)
                for t in range(lat // 128):
                    qf[t, to, :] = ql[:, t * 128:(t + 1) * 128]
                qf[lat // 128, to, :] = jnp.where(low, z, 0.0)

    def query(b):
        to = pl.ds(pl.multiple_of(b * heads, heads), heads)
        return jnp.concatenate([qf[t, to, :] for t in range(qf.shape[0])], axis=1)

    def scores(i, slot):
        for g in range(GROUP):
            qg = query(i * GROUP + g)
            sbuf[pl.ds(g * heads, heads), :] = dot(qg[:, :kvd].astype(bf16), cbuf[slot, g])

    def attend(i, slot):
        col = lax.broadcasted_iota(jnp.int32, (heads, rows), 1)
        for g in range(GROUP):
            b = i * GROUP + g
            to = pl.ds(pl.multiple_of(b * heads, heads), heads)
            new = kvr[pl.ds(b, 1), :]
            s_new = jnp.sum(query(b) * new, axis=1, keepdims=True) * scale
            s = sbuf[pl.ds(g * heads, heads), :] * scale
            s = jnp.where(col < lens_ref[b], s, -jnp.inf)
            mx = jnp.maximum(jnp.max(s, axis=1, keepdims=True), s_new)
            e = jnp.exp(s - mx)
            e_new = jnp.exp(s_new - mx)
            den = jnp.sum(e, axis=1, keepdims=True) + e_new
            p = (e / den).astype(bf16)
            p_new = (e_new / den).astype(bf16).astype(f32)
            o = lax.dot_general(p, cbuf[slot, g, :lat, :], (((1,), (1,)), ((), ())), preferred_element_type=f32)
            o = o + p_new * new[:, :lat]
            for t in range(lat // 128):
                ol[t, to, :] = o[:, t * 128:(t + 1) * 128]

    c_copy(0, 0).wait()
    scores(0, 0)

    def step(i, _):
        slot = lax.rem(i, CACHE_SLOTS)
        attend(i, slot)

        @pl.when(i + 1 < steps)
        def _():
            c_copy(i + 1, lax.rem(i + 1, CACHE_SLOTS)).wait()
            scores(i + 1, lax.rem(i + 1, CACHE_SLOTS))

        @pl.when(i + CACHE_SLOTS < steps)
        def _():
            c_copy(i + CACHE_SLOTS, slot).start()
        return 0

    lax.fori_loop(0, steps, step, 0)

    uv_copy.wait()
    for h in range(heads):
        o = jnp.concatenate([ol[t, pl.ds(h, bsz, stride=heads), :] for t in range(lat // 128)], axis=1).astype(bf16)
        oall[:, h * vh:(h + 1) * vh] = dot(o, uvbuf[h]).astype(bf16)
    o_copy.wait()
    h1 = (x_ref[...].astype(f32) + dot(oall[...], obuf[...])).astype(bf16)
    h1_ref[...] = h1
    h1 = h1.astype(f32)
    u_ref[...] = (h1 * lax.rsqrt(jnp.mean(h1 * h1, axis=-1, keepdims=True) + EPS)).astype(bf16)


def attention(x, cache, lens, w_q, w_dkv, w_uk, w_uv, w_o):
    bsz, hid = x.shape
    heads, nope, lat = w_uk.shape
    rows, kvd = cache.shape[1:]
    rot = kvd - lat
    vh = w_uv.shape[2]
    inv = ROPE_BASE ** (-2.0 * jnp.arange(rot // 2, dtype=jnp.float32) / rot)
    ang = inv[:, None] * lens.astype(jnp.float32)[None, :]
    tab = jnp.concatenate([jnp.cos(ang), jnp.sin(ang)], axis=0)
    bf16, f32 = jnp.bfloat16, jnp.float32
    vm = pl.BlockSpec(memory_space=pltpu.VMEM)
    hbm = pl.BlockSpec(memory_space=pl.ANY)
    dma = pltpu.SemaphoreType.DMA
    wide = (kvd + 127) // 128 * 128
    h1, u, kv = pl.pallas_call(
        attn_kernel,
        out_shape=(jax.ShapeDtypeStruct((bsz, hid), bf16), jax.ShapeDtypeStruct((bsz, hid), bf16),
                   jax.ShapeDtypeStruct((kvd, bsz), bf16)),
        in_specs=[pl.BlockSpec(memory_space=pltpu.SMEM), vm, vm] + [hbm] * 6,
        out_specs=(vm, vm, vm),
        scratch_shapes=[
            pltpu.VMEM((CACHE_SLOTS, GROUP, kvd, rows), bf16),
            pltpu.VMEM((Q_PARTS, hid, w_q.shape[1] // Q_PARTS), bf16),
            pltpu.VMEM((kvd, hid), bf16),
            pltpu.VMEM(w_uk.shape, bf16),
            pltpu.VMEM(w_uv.shape, bf16),
            pltpu.VMEM(w_o.shape, bf16),
            pltpu.VMEM((wide // 128, bsz * heads, 128), f32),
            pltpu.VMEM((bsz, wide), f32),
            pltpu.VMEM((GROUP * heads, rows), f32),
            pltpu.VMEM((lat // 128, bsz * heads, 128), f32),
            pltpu.VMEM((bsz, heads * vh), bf16),
            dma((CACHE_SLOTS,)), dma((Q_PARTS,)), dma((4,)),
        ],
        compiler_params=pltpu.CompilerParams(vmem_limit_bytes=67043328),
        name='attn',
    )(lens, x, tab, cache.transpose(0, 2, 1), w_q, w_dkv.T, w_uk, w_uv, w_o)
    return h1, u, kv.T


def moe_kernel(u_ref, h1_ref, meta_ref, sg, su, sd, eg, eu, ed, y_ref,
               gbuf, ubuf, dbuf, xall, act, sact, gate, outc, comb, uall, mall, s1, r1, s2, r2, own, shf,
               gsem, usem, dsem, us_send, us_recv, ms_send, ms_recv, s1_send, s1_recv, s2_send, s2_recv):
    n_loc = eg.shape[0]
    bsz, hid = u_ref.shape
    inter = eg.shape[2]
    n_col = hid // COLS
    pairs = n_loc // 2
    n_down = n_col * pairs
    half = bsz // 2
    me = lax.axis_index('ep')
    partner = {'ep': me + 1 - 2 * lax.rem(me, 2)}
    across = {'ep': lax.rem(me + 2, 4)}

    def gate_copy(e, slot):
        return pltpu.make_async_copy(eg.at[e], gbuf.at[slot], gsem.at[slot])

    def up_copy(e, slot):
        return pltpu.make_async_copy(eu.at[e], ubuf.at[slot], usem.at[slot])

    def sgate_copy(i):
        return pltpu.make_async_copy(sg.at[:, pl.ds(i * inter, inter)], gbuf.at[i], gsem.at[i])

    def sup_copy(i):
        return pltpu.make_async_copy(su.at[:, pl.ds(i * inter, inter)], ubuf.at[i], usem.at[i])

    def down_copy(j, slot):
        c = j // pairs
        e = lax.rem(j, pairs)
        return pltpu.make_async_copy(
            ed.at[pl.ds(2 * e, 2), :, pl.ds(pl.multiple_of(c * COLS, COLS), COLS)], dbuf.at[slot], dsem.at[slot])

    def sdown_copy(c, slot):
        return pltpu.make_async_copy(sd.at[:, :, pl.ds(c * COLS, COLS)], dbuf.at[slot], dsem.at[slot])

    def remote(src, dst, send, recv, dev):
        return pltpu.make_async_remote_copy(src_ref=src, dst_ref=dst, send_sem=send, recv_sem=recv,
                                            device_id=dev, device_id_type=pl.DeviceIdType.MESH)

    for i in range(2):
        sgate_copy(i).start()
        sup_copy(i).start()

    barrier = pltpu.get_barrier_semaphore()
    for dev in (partner, across):
        pl.semaphore_signal(barrier, inc=1, device_id=dev, device_id_type=pl.DeviceIdType.MESH)
    pl.semaphore_wait(barrier, 2)

    m_across = remote(meta_ref, mall.at[1], ms_send.at[1], ms_recv.at[1], across)
    u_across = [remote(u_ref.at[pl.ds(i * half, half)], uall.at[1, pl.ds(i * half, half)],
                       us_send.at[1 + i], us_recv.at[1 + i], across) for i in range(2)]
    m_partner = remote(meta_ref, mall.at[0], ms_send.at[0], ms_recv.at[0], partner)
    u_partner = remote(u_ref, uall.at[0], us_send.at[0], us_recv.at[0], partner)
    m_relay = remote(mall.at[1], mall.at[2], ms_send.at[2], ms_recv.at[2], partner)
    u_relay = [remote(uall.at[1, pl.ds(i * half, half)], uall.at[2, pl.ds(i * half, half)],
                      us_send.at[3 + i], us_recv.at[3 + i], partner) for i in range(2)]
    m_across.start()
    u_across[0].start()
    u_across[1].start()
    m_partner.start()
    u_partner.start()

    def glu(lhs, e, slot, dst, g_wait, u_wait, g_next, u_next):
        g_wait.wait()
        gate[...] = dot(lhs, gbuf[slot])
        g_next()
        u_wait.wait()
        v = dot(lhs, ubuf[slot])
        dst[...] = (jax.nn.silu(gate[...]) * v).astype(jnp.bfloat16)
        u_next()

    for i in range(2):
        glu(u_ref[...], i, i, sact.at[i], sgate_copy(i), sup_copy(i),
            lambda: gate_copy(i, i).start(), lambda: up_copy(i, i).start())

    for j in range(DOWN_SLOTS):
        down_copy(j, j).start()

    def dispatch(q, m, u):
        first = (me * n_loc).astype(jnp.float32)
        mine = lax.broadcasted_iota(jnp.int32, (n_loc, bsz), 0).astype(jnp.float32) + first
        hit = jnp.zeros((n_loc, bsz), jnp.float32)
        wgt = jnp.zeros((n_loc, bsz), jnp.float32)
        for k in range(6):
            eq = m[k:k + 1, :] == mine
            hit = jnp.where(eq, 1.0, hit)
            wgt = jnp.where(eq, m[8 + k:9 + k, :], wgt)
        row = lax.broadcasted_iota(jnp.int32, (bsz, bsz), 0)
        col = lax.broadcasted_iota(jnp.int32, (bsz, bsz), 1)
        low = jnp.where(row < col, 1.0, 0.0).astype(jnp.bfloat16)
        rank = jnp.where(hit > 0.0, dot(hit.astype(jnp.bfloat16), low), -1.0)
        slot = lax.broadcasted_iota(jnp.int32, (CAP, bsz), 0).astype(jnp.float32)
        sel = []
        ct = []
        for e in range(n_loc):
            at = slot == rank[e:e + 1, :]
            sel.append(jnp.where(at, 1.0, 0.0).astype(jnp.bfloat16))
            ct.append(jnp.where(at, wgt[e:e + 1, :], 0.0))
        c0 = jnp.concatenate(ct, axis=0).T
        for i in range(3):
            ci = c0.astype(jnp.bfloat16)
            comb[q, pl.ds(i * bsz, bsz), :] = ci
            c0 = c0 - ci.astype(jnp.float32)
        xall[q] = dot(jnp.concatenate(sel, axis=0), u).astype(jnp.bfloat16)

    dispatch(0, meta_ref[...], u_ref[...])
    m_partner.wait_recv()
    u_partner.wait_recv()
    dispatch(1, mall[0], uall[0])
    m_across.wait_recv()
    m_relay.start()
    for i in range(2):
        u_across[i].wait_recv()
        u_relay[i].start()
    dispatch(2, mall[1], uall[1])
    m_relay.wait_recv()
    for i in range(2):
        u_relay[i].wait_recv()
    dispatch(3, mall[2], uall[2])

    def expert(e, _):
        slot = lax.rem(e, 2)
        lhs = xall[:, pl.ds(pl.multiple_of(e * CAP, CAP), CAP), :].reshape(4 * CAP, hid)

        def g_next():
            @pl.when(e < n_loc - 2)
            def _():
                gate_copy(e + 2, slot).start()

        def u_next():
            @pl.when(e < n_loc - 2)
            def _():
                up_copy(e + 2, slot).start()

        glu(lhs, e, slot, act.at[e], gate_copy(e, slot), up_copy(e, slot), g_next, u_next)
        return 0

    lax.fori_loop(0, n_loc, expert, 0)

    def ring1(c):
        return remote(s1.at[c], r1.at[c], s1_send.at[c], s1_recv.at[c], partner)

    def ring2(c):
        return remote(s2.at[c], r2.at[c], s2_send.at[c], s2_recv.at[c], across)

    def fold(c):
        ring1(c).wait_recv()
        s2[c] = s2[c] + r1[c, 1]
        own[c] = own[c] + r1[c, 0]

    def down_step(j, c, e):
        slot = lax.rem(j, DOWN_SLOTS)
        down_copy(j, slot).wait()
        for i in range(2):
            res = dot(act[2 * e + i], dbuf[slot, i]).astype(jnp.bfloat16)
            outc[:, pl.ds(pl.multiple_of((2 * e + i) * CAP, CAP), CAP), :] = res.reshape(4, CAP, COLS)

        @pl.when(j + DOWN_SLOTS < n_down)
        def _():
            down_copy(j + DOWN_SLOTS, slot).start()

    def combine(q):
        p = dot(comb[q], outc[q])
        return p[:bsz] + p[bsz:2 * bsz] + p[2 * bsz:]

    def column(c, _):
        def step(e, _):
            down_step(c * pairs + e, c, e)

            @pl.when((c > 0) & (e == 2))
            def _():
                fold(c - 1)

            @pl.when((c > 0) & (e == 3))
            def _():
                ring2(c - 1).start()
            return 0

        lax.fori_loop(0, pairs, step, 0)
        s1[c, 1] = combine(3)
        s1[c, 0] = combine(1)
        s2[c] = combine(2)
        own[c] = combine(0)
        ring1(c).start()
        return 0

    lax.fori_loop(0, n_col, column, 0)

    for c in range(min(DOWN_SLOTS, n_col)):
        sdown_copy(c, (n_down + c) % DOWN_SLOTS).start()
    for c in range(n_col):
        slot = (n_down + c) % DOWN_SLOTS
        sdown_copy(c, slot).wait()
        shf[c] = dot(sact[0], dbuf[slot, 0]) + dot(sact[1], dbuf[slot, 1])
        if c + DOWN_SLOTS < n_col:
            sdown_copy(c + DOWN_SLOTS, slot).start()
        if c == 0:
            fold(n_col - 1)
        if c == 1:
            ring2(n_col - 1).start()

    for c in range(n_col):
        ring2(c).wait_recv()
        cols = pl.ds(c * COLS, COLS)
        y = h1_ref[:, cols].astype(jnp.float32) + shf[c] + (own[c] + r2[c])
        y_ref[:, cols] = y.astype(jnp.bfloat16)

    for copy in (m_across, *u_across, m_partner, u_partner, m_relay, *u_relay):
        copy.wait_send()
    for c in range(n_col):
        ring1(c).wait_send()
        ring2(c).wait_send()


def moe(u, h1, meta, s_gate, s_up, s_down, e_gate, e_up, e_down):
    bsz, hid = u.shape
    n_loc, _, inter = e_gate.shape
    n_col = hid // COLS
    bf16, f32 = jnp.bfloat16, jnp.float32
    vm = pl.BlockSpec(memory_space=pltpu.VMEM)
    hbm = pl.BlockSpec(memory_space=pl.ANY)
    dma = pltpu.SemaphoreType.DMA
    return pl.pallas_call(
        moe_kernel,
        out_shape=jax.ShapeDtypeStruct((bsz, hid), bf16),
        in_specs=[vm] * 3 + [hbm] * 6,
        out_specs=vm,
        scratch_shapes=[
            pltpu.VMEM((2, hid, inter), bf16),
            pltpu.VMEM((2, hid, inter), bf16),
            pltpu.VMEM((DOWN_SLOTS, 2, inter, COLS), bf16),
            pltpu.VMEM((4, n_loc * CAP, hid), bf16),
            pltpu.VMEM((n_loc, 4 * CAP, inter), bf16),
            pltpu.VMEM((2, bsz, inter), bf16),
            pltpu.VMEM((bsz, inter), f32),
            pltpu.VMEM((4, n_loc * CAP, COLS), bf16),
            pltpu.VMEM((4, 3 * bsz, n_loc * CAP), bf16),
            pltpu.VMEM((3, bsz, hid), bf16),
            pltpu.VMEM((3, 16, bsz), f32),
            pltpu.VMEM((n_col, 2, bsz, COLS), f32),
            pltpu.VMEM((n_col, 2, bsz, COLS), f32),
            pltpu.VMEM((n_col, bsz, COLS), f32),
            pltpu.VMEM((n_col, bsz, COLS), f32),
            pltpu.VMEM((n_col, bsz, COLS), f32),
            pltpu.VMEM((n_col, bsz, COLS), f32),
            dma((2,)), dma((2,)), dma((DOWN_SLOTS,)),
            dma((5,)), dma((5,)), dma((3,)), dma((3,)),
            dma((n_col,)), dma((n_col,)), dma((n_col,)), dma((n_col,)),
        ],
        compiler_params=pltpu.CompilerParams(
            collective_id=0, has_side_effects=True, vmem_limit_bytes=67043328),
        name='moe',
    )(u, h1, meta, s_gate, s_up, s_down.reshape(2, inter, hid), e_gate, e_up, e_down)


def solution(mesh):
    tok_spec = P(('rep', 'ep'))
    row_spec = P(('rep', 'ep'), None)
    cache_spec = P(('rep', 'ep'), None, None)
    exp_spec = P('ep', None, None)

    def local(x, cache, lens, ids, rw, w_q, w_dkv, w_uk, w_uv, w_o, s_gate, s_up, s_down, e_gate, e_up, e_down):
        h1, u, kv_new = attention(x, cache, lens, w_q, w_dkv, w_uk, w_uv, w_o)
        meta = jnp.concatenate([jnp.pad(ids.astype(jnp.float32), ((0, 0), (0, 2))), jnp.pad(rw, ((0, 0), (0, 2)))], axis=1).T
        y = moe(u, h1, meta, s_gate, s_up, s_down, e_gate, e_up, e_down)
        return y, kv_new

    in_specs = (row_spec, cache_spec, tok_spec, row_spec, row_spec) + (P(),) * 8 + (exp_spec,) * 3
    return jax.shard_map(local, mesh=mesh, in_specs=in_specs, out_specs=(row_spec, row_spec), check_vma=False)
```

```python
import jax
import jax.numpy as jnp
from jax import lax
from jax.experimental import pallas as pl
from jax.experimental.pallas import tpu as pltpu
from jax.sharding import PartitionSpec as P

EPS = 1e-6
ROPE_BASE = 1.0e4
CAP = 32
COLS = 256
PER = 4
FAR, NEAR, ACROSS, OWN = range(4)
DOWN_SLOTS = 3
GROUP = 8
CACHE_SLOTS = 6
Q_PARTS = 4


def dot(a, b):
    return jnp.dot(a, b, preferred_element_type=jnp.float32)


def attn_kernel(x_ref, pos_ref, inv_ref, ids_ref, rw_ref, cache, wq, wdkv, wuk, wuv, wo, h1_ref, u_ref, kv_ref, meta_ref,
                cbuf, qbuf, dkvbuf, ukbuf, uvbuf, obuf, qf, kvr, lenr, sbuf, nbuf, pbuf, pnbuf, ol, oall,
                csem, qsem, wsem):
    bsz, hid = x_ref.shape
    heads, nope, lat = wuk.shape
    kvd, rows = cache.shape[1], cache.shape[2]
    rot = kvd - lat
    vh = wuv.shape[2]
    qkd = nope + rot
    steps = bsz // GROUP
    part = heads * qkd // Q_PARTS
    scale = qkd ** -0.5
    f32, bf16 = jnp.float32, jnp.bfloat16

    def c_copy(i, slot):
        return pltpu.make_async_copy(cache.at[pl.ds(i * GROUP, GROUP)], cbuf.at[slot], csem.at[slot])

    q_copies = [pltpu.make_async_copy(wq.at[:, pl.ds(i * part, part)], qbuf.at[i], qsem.at[i]) for i in range(Q_PARTS)]
    dkv_copy = pltpu.make_async_copy(wdkv, dkvbuf, wsem.at[0])
    uk_copy = pltpu.make_async_copy(wuk, ukbuf, wsem.at[1])
    uv_copy = pltpu.make_async_copy(wuv, uvbuf, wsem.at[2])
    o_copy = pltpu.make_async_copy(wo, obuf, wsem.at[3])
    dkv_copy.start()
    uk_copy.start()
    for copy in q_copies:
        copy.start()
    for i in range(CACHE_SLOTS):
        c_copy(i, i).start()
    uv_copy.start()
    o_copy.start()

    lane = lax.broadcasted_iota(jnp.int32, (bsz, 2 * rot), 1)
    low = lane < rot
    front = lax.rem(lane, rot) < rot // 2

    def turn(r):
        swap = jnp.where(front, pltpu.roll(r, 2 * rot - rot // 2, 1), pltpu.roll(r, rot // 2, 1))
        return (r * cos + swap * sin).astype(bf16).astype(f32)

    with jax.named_scope('norm'):
        x = x_ref[...].astype(f32)
        xn = (x * lax.rsqrt(jnp.mean(x * x, axis=-1, keepdims=True) + EPS)).astype(bf16)
        ang = inv_ref[...] * pos_ref[...].astype(f32)
        cos_t = jnp.cos(ang)
        sin_t = jnp.sin(ang)
        cos = jnp.concatenate([cos_t] * 4, axis=0).T
        sin = jnp.concatenate([-sin_t, sin_t] * 2, axis=0).T
        top = ids_ref.shape[0]
        lenr[...] = jnp.broadcast_to(pos_ref[...].astype(f32), lenr.shape).T
        meta_ref[...] = jnp.zeros(meta_ref.shape, f32)
        meta_ref[:top, :] = ids_ref[...].astype(f32)
        meta_ref[8:8 + top, :] = rw_ref[...]

    with jax.named_scope('kv_phase'):
        dkv_copy.wait()
        kv = lax.dot_general(xn, dkvbuf[...], (((1,), (1,)), ((), ())), preferred_element_type=f32)
        c = kv[:, :lat]
        c = (c * lax.rsqrt(jnp.mean(c * c, axis=-1, keepdims=True) + EPS)).astype(bf16).astype(f32)
        r = turn(jnp.concatenate([kv[:, lat:], jnp.zeros((bsz, kvr.shape[1] - kvd), f32)], axis=1))
        kvr[:, :lat] = c
        kvr[:, lat:] = r
        kv_ref[:lat, :] = c.T.astype(bf16)
        kv_ref[lat:, :] = r.T[:rot, :].astype(bf16)

    with jax.named_scope('q_phase'):
        uk_copy.wait()
        for i in range(Q_PARTS):
            with jax.named_scope('q_dot'):
                q_copies[i].wait()
                q = dot(xn, qbuf[i]).astype(bf16).astype(f32)
            for j in range(part // (2 * qkd)):
                with jax.named_scope('q_rope'):
                    at = 2 * qkd * j
                    h = i * (part // qkd) + 2 * j
                    mid = q[:, at + nope:at + 2 * nope]
                    last = q[:, at + 2 * nope:at + 3 * nope]
                    n_a = q[:, at:at + nope]
                    n_b = jnp.where(low, pltpu.roll(mid, rot, 1), pltpu.roll(last, rot, 1))
                    r = turn(jnp.where(low, mid, last))
                other = pltpu.roll(r, rot, 1)
                for k, n, z in ((0, n_a, jnp.where(low, r, other)), (1, n_b, jnp.where(low, other, r))):
                    with jax.named_scope('q_lat'):
                        qf[h + k, :, :lat] = dot(n.astype(bf16), ukbuf[h + k]).astype(bf16).astype(f32)
                        qf[h + k, :, lat:] = z

    size = heads * GROUP
    row = lax.rem(lax.broadcasted_iota(jnp.int32, (size, 128), 0), GROUP)
    lane = lax.broadcasted_iota(jnp.int32, (size, 128), 1)

    def spread(v, width):
        keep = [jnp.where(row == g, 1.0, 0.0).astype(bf16) for g in range(GROUP)]
        return jnp.concatenate([v[:, t * 128:(t + 1) * 128] * keep[g]
                                for g in range(GROUP) for t in range(width // 128)], axis=1)

    def scores(i, k):
        slot = lax.rem(i, CACHE_SLOTS)
        at = pl.ds(pl.multiple_of(i * GROUP, GROUP), GROUP)
        q = qf[:, at, :]
        kv = kvr[at, :]
        nbuf[k] = jnp.broadcast_to(jnp.sum(q * kv[None], axis=2, keepdims=True).reshape(size, 1), nbuf.shape[1:])
        q = q.reshape(size, q.shape[2]).astype(bf16)
        tail = q[:, lat:]
        pairs = [tail * jnp.where(row == 2 * j + lane // rot, 1.0, 0.0).astype(bf16) for j in range(GROUP // 2)]
        c = cbuf.at[slot]
        sbuf[k] = (dot(spread(q[:, :lat], lat), c[:, :lat, :].reshape(GROUP * lat, rows))
                   + dot(jnp.concatenate(pairs, axis=1), c[:, lat:, :].reshape(GROUP * rot, rows)))

    def soften(i, k):
        at = pl.ds(pl.multiple_of(i * GROUP, GROUP), GROUP)
        col = lax.broadcasted_iota(jnp.int32, (GROUP, rows), 1).astype(f32)
        live = col < lenr[at, :1]
        s_new = nbuf[k, :, :1] * scale
        s = (sbuf[k] * scale).reshape(heads, GROUP, rows)
        s = jnp.where(live[None], s, -jnp.inf).reshape(size, rows)
        mx = jnp.maximum(jnp.max(s, axis=1, keepdims=True), s_new)
        e = jnp.exp(s - mx)
        e_new = jnp.exp(s_new - mx)
        inv = 1.0 / (jnp.sum(e, axis=1, keepdims=True) + e_new)
        pbuf[k] = (e * inv).astype(bf16)
        pnbuf[k] = jnp.broadcast_to((e_new * inv).astype(bf16).astype(f32), pnbuf.shape[1:])

    def mix(i, k):
        slot = lax.rem(i, CACHE_SLOTS)
        at = pl.ds(pl.multiple_of(i * GROUP, GROUP), GROUP)
        c = jnp.concatenate([cbuf[slot, g, :lat, :] for g in range(GROUP)], axis=1)
        o = lax.dot_general(spread(pbuf[k], rows), c, (((1,), (1,)), ((), ())), preferred_element_type=f32)
        p_new = jnp.concatenate([pnbuf[k]] * (lat // 128), axis=1)
        ol[:, at, :] = (o + p_new * jnp.concatenate([kvr[at, :lat]] * heads, axis=0)).reshape(heads, GROUP, lat)

    with jax.named_scope('attend_loop'):
        for i in range(2):
            c_copy(i, i).wait()
            scores(i, i)
        soften(0, 0)

        def step(j, _):
            for k in (1, 0):
                i = 2 * j + 2 - k
                c_copy(i + 1, lax.rem(i + 1, CACHE_SLOTS)).wait()
            for k in (1, 0):
                i = 2 * j + 2 - k
                mix(i - 1, 1 - k)
                soften(i, k)
                scores(i + 1, 1 - k)

            @pl.when(2 * j + 1 + CACHE_SLOTS < steps)
            def _():
                for k in range(2):
                    i = 2 * j + k
                    c_copy(i + CACHE_SLOTS, lax.rem(i, CACHE_SLOTS)).start()
            return 0

        lax.fori_loop(0, steps // 2 - 1, step, 0)
        mix(steps - 2, 0)
        soften(steps - 1, 1)
        mix(steps - 1, 1)

    with jax.named_scope('out_phase'):
        uv_copy.wait()
        for h in range(heads):
            o = ol[h].astype(bf16)
            oall[:, h * vh:(h + 1) * vh] = dot(o, uvbuf[h]).astype(bf16)
        o_copy.wait()
        h1 = (x_ref[...].astype(f32) + dot(oall[...], obuf[...])).astype(bf16)
        h1_ref[...] = h1
        h1 = h1.astype(f32)
        u_ref[...] = (h1 * lax.rsqrt(jnp.mean(h1 * h1, axis=-1, keepdims=True) + EPS)).astype(bf16)


def attention(x, cache, lens, ids, rw, w_q, w_dkv, w_uk, w_uv, w_o):
    bsz, hid = x.shape
    heads, nope, lat = w_uk.shape
    rows, kvd = cache.shape[1:]
    rot = kvd - lat
    vh = w_uv.shape[2]
    inv = (ROPE_BASE ** (-2.0 * jnp.arange(rot // 2, dtype=jnp.float32) / rot))[:, None]
    bf16, f32 = jnp.bfloat16, jnp.float32
    vm = pl.BlockSpec(memory_space=pltpu.VMEM)
    hbm = pl.BlockSpec(memory_space=pl.ANY)
    dma = pltpu.SemaphoreType.DMA
    wide = (kvd + 127) // 128 * 128
    h1, u, kv, meta = pl.pallas_call(
        attn_kernel,
        out_shape=(jax.ShapeDtypeStruct((bsz, hid), bf16), jax.ShapeDtypeStruct((bsz, hid), bf16),
                   jax.ShapeDtypeStruct((kvd, bsz), bf16), jax.ShapeDtypeStruct((16, bsz), f32)),
        in_specs=[vm] * 5 + [hbm] * 6,
        out_specs=(vm,) * 4,
        scratch_shapes=[
            pltpu.VMEM((CACHE_SLOTS, GROUP, kvd, rows), bf16),
            pltpu.VMEM((Q_PARTS, hid, w_q.shape[1] // Q_PARTS), bf16),
            pltpu.VMEM((kvd, hid), bf16),
            pltpu.VMEM(w_uk.shape, bf16),
            pltpu.VMEM(w_uv.shape, bf16),
            pltpu.VMEM(w_o.shape, bf16),
            pltpu.VMEM((heads, bsz, wide), f32),
            pltpu.VMEM((bsz, wide), f32),
            pltpu.VMEM((bsz, 128), f32),
            pltpu.VMEM((2, GROUP * heads, rows), f32),
            pltpu.VMEM((2, GROUP * heads, 128), f32),
            pltpu.VMEM((2, GROUP * heads, rows), bf16),
            pltpu.VMEM((2, GROUP * heads, 128), f32),
            pltpu.VMEM((heads, bsz, lat), f32),
            pltpu.VMEM((bsz, heads * vh), bf16),
            dma((CACHE_SLOTS,)), dma((Q_PARTS,)), dma((4,)),
        ],
        compiler_params=pltpu.CompilerParams(
            vmem_limit_bytes=67043328),
        name='attn',
    )(x, lens[None, :], inv, ids.T, rw.T, cache.transpose(0, 2, 1), w_q, w_dkv.T, w_uk, w_uv, w_o)
    return h1, u, kv.T, meta


def moe_kernel(u_ref, meta_ref, sg, su, sd, eg, eu, ed, y_ref,
               gbuf, ubuf, dbuf, xall, act, sact, gate, outc, comb, uall, mall, part, r1, r2,
               gsem, usem, dsem, ssem, us_send, us_recv, ms_send, ms_recv, s1_send, s1_recv, s2_send, s2_recv):
    n_loc = eg.shape[0]
    bsz, hid = u_ref.shape
    inter = eg.shape[2]
    n_col = hid // COLS
    blocks = n_loc // PER
    n_down = n_col * blocks
    half = bsz // 2
    me = lax.axis_index('ep')
    partner = {'ep': me + 1 - 2 * lax.rem(me, 2)}
    across = {'ep': lax.rem(me + 2, 4)}

    def gate_copy(e, slot):
        return pltpu.make_async_copy(eg.at[e], gbuf.at[slot], gsem.at[slot])

    def up_copy(e, slot):
        return pltpu.make_async_copy(eu.at[e], ubuf.at[slot], usem.at[slot])

    def sgate_copy(i):
        return pltpu.make_async_copy(sg.at[:, pl.ds(i * inter, inter)], gbuf.at[i], gsem.at[i])

    def sup_copy(i):
        return pltpu.make_async_copy(su.at[:, pl.ds(i * inter, inter)], ubuf.at[i], usem.at[i])

    def down_copy(j, slot):
        c = j // blocks
        e = lax.rem(j, blocks)
        return pltpu.make_async_copy(
            ed.at[pl.ds(PER * e, PER), :, pl.ds(pl.multiple_of(c * COLS, COLS), COLS)], dbuf.at[slot], dsem.at[slot])

    def sdown_copy(c, i, slot):
        at = pl.multiple_of((2 * c + i) * COLS, COLS)
        return pltpu.make_async_copy(sd.at[:, :, pl.ds(at, COLS)], dbuf.at[slot, pl.ds(2 * i, 2)], ssem.at[slot, i])

    def remote(src, dst, send, recv, dev):
        return pltpu.make_async_remote_copy(src_ref=src, dst_ref=dst, send_sem=send, recv_sem=recv,
                                            device_id=dev, device_id_type=pl.DeviceIdType.MESH)

    for i in range(2):
        sgate_copy(i).start()
        sup_copy(i).start()

    with jax.named_scope('barrier'):
        barrier = pltpu.get_barrier_semaphore()
        for dev in (partner, across):
            pl.semaphore_signal(barrier, inc=1, device_id=dev, device_id_type=pl.DeviceIdType.MESH)
        pl.semaphore_wait(barrier, 2)

    m_across = remote(meta_ref, mall.at[1], ms_send.at[1], ms_recv.at[1], across)
    u_across = [remote(u_ref.at[pl.ds(i * half, half)], uall.at[1, pl.ds(i * half, half)],
                       us_send.at[1 + i], us_recv.at[1 + i], across) for i in range(2)]
    m_partner = remote(meta_ref, mall.at[0], ms_send.at[0], ms_recv.at[0], partner)
    u_partner = remote(u_ref, uall.at[0], us_send.at[0], us_recv.at[0], partner)
    m_relay = remote(mall.at[1], mall.at[2], ms_send.at[2], ms_recv.at[2], partner)
    u_relay = [remote(uall.at[1, pl.ds(i * half, half)], uall.at[2, pl.ds(i * half, half)],
                      us_send.at[3 + i], us_recv.at[3 + i], partner) for i in range(2)]
    m_across.start()
    u_across[0].start()
    u_across[1].start()
    m_partner.start()
    u_partner.start()

    def glu(lhs, e, slot, dst, g_wait, u_wait, g_next, u_next):
        g_wait.wait()
        gate[...] = dot(lhs, gbuf[slot])
        g_next()
        u_wait.wait()
        v = dot(lhs, ubuf[slot])
        dst[...] = (jax.nn.silu(gate[...]) * v).astype(jnp.bfloat16)
        u_next()

    with jax.named_scope('shared_up'):
        for i in range(2):
            glu(u_ref[...], i, i, sact.at[i], sgate_copy(i), sup_copy(i),
                lambda: gate_copy(i, i).start(), lambda: up_copy(i, i).start())

    for j in range(DOWN_SLOTS):
        down_copy(j, j).start()

    def dispatch(q, m, u):
        first = (me * n_loc).astype(jnp.float32)
        mine = lax.broadcasted_iota(jnp.int32, (n_loc, bsz), 0).astype(jnp.float32) + first
        hit = jnp.zeros((n_loc, bsz), jnp.float32)
        wgt = jnp.zeros((n_loc, bsz), jnp.float32)
        for k in range(6):
            eq = m[k:k + 1, :] == mine
            hit = jnp.where(eq, 1.0, hit)
            wgt = jnp.where(eq, m[8 + k:9 + k, :], wgt)
        row = lax.broadcasted_iota(jnp.int32, (bsz, bsz), 0)
        col = lax.broadcasted_iota(jnp.int32, (bsz, bsz), 1)
        low = jnp.where(row < col, 1.0, 0.0).astype(jnp.bfloat16)
        rank = jnp.where(hit > 0.0, dot(hit.astype(jnp.bfloat16), low), -1.0)
        slot = lax.broadcasted_iota(jnp.int32, (CAP, bsz), 0).astype(jnp.float32)
        sel = []
        ct = []
        for e in range(n_loc):
            at = slot == rank[e:e + 1, :]
            sel.append(jnp.where(at, 1.0, 0.0).astype(jnp.bfloat16))
            ct.append(jnp.where(at, wgt[e:e + 1, :], 0.0))
        c0 = jnp.concatenate(ct, axis=0).T
        for i in range(3):
            ci = c0.astype(jnp.bfloat16)
            comb[q, pl.ds(i * bsz, bsz), :] = ci
            c0 = c0 - ci.astype(jnp.float32)
        xall[q] = dot(jnp.concatenate(sel, axis=0), u).astype(jnp.bfloat16)

    with jax.named_scope('disp01'):
        dispatch(OWN, meta_ref[...], u_ref[...])
        m_partner.wait_recv()
        u_partner.wait_recv()
        dispatch(NEAR, mall[0], uall[0])
    with jax.named_scope('gather_wait'):
        m_across.wait_recv()
        m_relay.start()
        for i in range(2):
            u_across[i].wait_recv()
            u_relay[i].start()
    with jax.named_scope('disp2'):
        dispatch(ACROSS, mall[1], uall[1])
    with jax.named_scope('relay_wait'):
        m_relay.wait_recv()
        for i in range(2):
            u_relay[i].wait_recv()
    with jax.named_scope('disp3'):
        dispatch(FAR, mall[2], uall[2])

    def expert(e, _):
        slot = lax.rem(e, 2)
        lhs = xall[:, pl.ds(pl.multiple_of(e * CAP, CAP), CAP), :].reshape(4 * CAP, hid)

        def g_next():
            @pl.when(e < n_loc - 2)
            def _():
                gate_copy(e + 2, slot).start()

        def u_next():
            @pl.when(e < n_loc - 2)
            def _():
                up_copy(e + 2, slot).start()

        glu(lhs, e, slot, act.at[e], gate_copy(e, slot), up_copy(e, slot), g_next, u_next)
        return 0

    with jax.named_scope('experts'):
        lax.fori_loop(0, n_loc, expert, 0)

    def ring1(c, i):
        return remote(part.at[c, i], r1.at[c, i], s1_send.at[c, i], s1_recv.at[c, i], partner)

    def ring2(c):
        return remote(part.at[c, ACROSS], r2.at[c], s2_send.at[c], s2_recv.at[c], across)

    def fold(c):
        ring1(c, FAR).wait_recv()
        part[c, ACROSS] = part[c, ACROSS] + r1[c, FAR]

    def combine(c, q):
        p = dot(comb[q], outc[lax.rem(c, 2), q])
        part[c, q] = p[:bsz] + p[bsz:2 * bsz] + p[2 * bsz:]

    def down_step(c, e, early):
        j = c * blocks + e
        slot = lax.rem(j, DOWN_SLOTS)
        down_copy(j, slot).wait()
        if early is not None:
            early()
        for i in range(PER):
            res = dot(act[PER * e + i], dbuf[slot, i]).astype(jnp.bfloat16)
            outc[lax.rem(c, 2), :, pl.ds(pl.multiple_of((PER * e + i) * CAP, CAP), CAP), :] = res.reshape(4, CAP, COLS)

        @pl.when(j + DOWN_SLOTS < n_down)
        def _():
            down_copy(j + DOWN_SLOTS, slot).start()

        @pl.when(j + DOWN_SLOTS >= n_down)
        def _():
            for i in range(2):
                sdown_copy(j + DOWN_SLOTS - n_down, i, slot).start()

    def first(e, _):
        down_step(0, e, None)
        return 0

    def column(c, _):
        def step(e, _):
            for i in (FAR, NEAR):
                @pl.when(e == i + 1)
                def _():
                    ring1(c - 1, i).start()

            @pl.when(e == 3)
            def _():
                fold(c - 1)

            down_step(c, e, lambda: combine(c - 1, e))

            @pl.when(e == 3)
            def _():
                ring2(c - 1).start()
            return 0

        lax.fori_loop(0, blocks, step, 0)
        return 0

    with jax.named_scope('column0'):
        lax.fori_loop(0, blocks, first, 0)
    with jax.named_scope('columns'):
        lax.fori_loop(1, n_col, column, 0)

    last = n_col - 1
    with jax.named_scope('combine'):
        combine(last, FAR)
        combine(last, ACROSS)
        ring1(last, FAR).start()
        combine(last, NEAR)
        combine(last, OWN)
        ring1(last, NEAR).start()

    with jax.named_scope('shared_down'):
        for c in range(n_col // 2):
            slot = (n_down + c) % DOWN_SLOTS
            for i in range(2):
                sdown_copy(c, i, slot).wait()
                part[2 * c + i, OWN] = (part[2 * c + i, OWN] + dot(sact[0], dbuf[slot, 2 * i])
                                        + dot(sact[1], dbuf[slot, 2 * i + 1]))
            if c + DOWN_SLOTS < n_col // 2:
                for i in range(2):
                    sdown_copy(c + DOWN_SLOTS, i, slot).start()
            if c == 0:
                fold(last)
            if c == 1:
                ring2(last).start()

    with jax.named_scope('tail'):
        for c in range(n_col):
            ring1(c, NEAR).wait_recv()
            ring2(c).wait_recv()
            y_ref[:, c * COLS:(c + 1) * COLS] = (part[c, OWN] + r1[c, NEAR]) + r2[c]

    for copy in (m_across, *u_across, m_partner, u_partner, m_relay, *u_relay):
        copy.wait_send()
    for c in range(n_col):
        ring1(c, FAR).wait_send()
        ring1(c, NEAR).wait_send()
        ring2(c).wait_send()


def moe(u, meta, s_gate, s_up, s_down, e_gate, e_up, e_down):
    bsz, hid = u.shape
    n_loc, _, inter = e_gate.shape
    n_col = hid // COLS
    bf16, f32 = jnp.bfloat16, jnp.float32
    vm = pl.BlockSpec(memory_space=pltpu.VMEM)
    hbm = pl.BlockSpec(memory_space=pl.ANY)
    dma = pltpu.SemaphoreType.DMA
    return pl.pallas_call(
        moe_kernel,
        out_shape=jax.ShapeDtypeStruct((bsz, hid), f32),
        in_specs=[vm] * 2 + [hbm] * 6,
        out_specs=vm,
        scratch_shapes=[
            pltpu.VMEM((2, hid, inter), bf16),
            pltpu.VMEM((2, hid, inter), bf16),
            pltpu.VMEM((DOWN_SLOTS, PER, inter, COLS), bf16),
            pltpu.VMEM((4, n_loc * CAP, hid), bf16),
            pltpu.VMEM((n_loc, 4 * CAP, inter), bf16),
            pltpu.VMEM((2, bsz, inter), bf16),
            pltpu.VMEM((bsz, inter), f32),
            pltpu.VMEM((2, 4, n_loc * CAP, COLS), bf16),
            pltpu.VMEM((4, 3 * bsz, n_loc * CAP), bf16),
            pltpu.VMEM((3, bsz, hid), bf16),
            pltpu.VMEM((3, 16, bsz), f32),
            pltpu.VMEM((n_col, 4, bsz, COLS), f32),
            pltpu.VMEM((n_col, 2, bsz, COLS), f32),
            pltpu.VMEM((n_col, bsz, COLS), f32),
            dma((2,)), dma((2,)), dma((DOWN_SLOTS,)), dma((DOWN_SLOTS, 2)),
            dma((5,)), dma((5,)), dma((3,)), dma((3,)),
            dma((n_col, 2)), dma((n_col, 2)), dma((n_col,)), dma((n_col,)),
        ],
        compiler_params=pltpu.CompilerParams(
            collective_id=0, has_side_effects=True, vmem_limit_bytes=67043328),
        name='moe',
    )(u, meta, s_gate, s_up, s_down.reshape(2, inter, hid), e_gate, e_up, e_down)


def solution(mesh):
    tok_spec = P(('rep', 'ep'))
    row_spec = P(('rep', 'ep'), None)
    cache_spec = P(('rep', 'ep'), None, None)
    exp_spec = P('ep', None, None)

    def local(x, cache, lens, ids, rw, w_q, w_dkv, w_uk, w_uv, w_o, s_gate, s_up, s_down, e_gate, e_up, e_down):
        h1, u, kv_new, meta = attention(x, cache, lens, ids, rw, w_q, w_dkv, w_uk, w_uv, w_o)
        mixed = moe(u, meta, s_gate, s_up, s_down, e_gate, e_up, e_down)
        y = (h1.astype(jnp.float32) + mixed).astype(jnp.bfloat16)
        return y, kv_new

    in_specs = (row_spec, cache_spec, tok_spec, row_spec, row_spec) + (P(),) * 8 + (exp_spec,) * 3
    return jax.shard_map(local, mesh=mesh, in_specs=in_specs, out_specs=(row_spec, row_spec), check_vma=False)
```

```python
import jax
import jax.numpy as jnp
from jax import lax
from jax.experimental import pallas as pl
from jax.experimental.pallas import tpu as pltpu
from jax.sharding import PartitionSpec as P

EPS = 1e-6
ROPE_BASE = 1.0e4
CAP = 32
COLS = 256
PER = 4
RING = 3
SLOTS = 6
GROUP = 8
Q_PARTS = 8
FAR, ACROSS, NEAR, OWN = range(4)
LAND = {FAR: 0, NEAR: 1}


def dot(a, b):
    return jnp.dot(a, b, preferred_element_type=jnp.float32)


def dot_t(a, b):
    return lax.dot_general(a, b, (((1,), (1,)), ((), ())), preferred_element_type=jnp.float32)


def layer(x_hbm, pos_ref, ids_ref, rw_ref, cache, wq, wq3, wdkv, wuk, wuv, wo, sg, su, sd, eg, eu, ed,
          y_ref, kv_ref,
          wbuf, dbuf, xall, act, sact, outc, comb, uall, mall, meta, part, r1, r2, ub,
          wsem, dsem, ssem, qsem, asem, us_send, us_recv, ms_send, ms_recv, s1_send, s1_recv, s2_send, s2_recv):
    f32, bf16 = jnp.float32, jnp.bfloat16
    bsz, hid = x_hbm.shape
    kvd, rows = cache.shape[1] // 2, cache.shape[2]
    lat = wuk.shape[1]
    rot = kvd - lat
    vh = wuv.shape[4]
    heads = hid // vh
    nope = wuk.shape[0] // heads
    qkd = nope + rot
    steps = bsz // GROUP
    wide = heads * qkd // Q_PARTS
    scale = qkd ** -0.5
    size = heads * GROUP
    n_loc = eg.shape[0]
    inter = eg.shape[2]
    n_col = hid // COLS
    blocks = n_loc // PER
    n_down = n_col * blocks
    half = bsz // 2
    top = ids_ref.shape[0]
    me = lax.axis_index('ep')
    partner = {'ep': me + 1 - 2 * lax.rem(me, 2)}
    across = {'ep': lax.rem(me + 2, 4)}
    q_wide = (lat // 128 + 1) * 128
    piece = hid // (steps // 2)

    barrier = pltpu.get_barrier_semaphore()
    for dev in (partner, across):
        pl.semaphore_signal(barrier, inc=1, device_id=dev, device_id_type=pl.DeviceIdType.MESH)

    def copy(src, dst, sem):
        return pltpu.make_async_copy(src, dst, sem)

    def c_copy(i):
        slot = lax.rem(i, SLOTS)
        return copy(cache.at[pl.ds(i * (GROUP // 2), GROUP // 2)], dbuf.at[slot, :, pl.ds(0, 2 * kvd), :], dsem.at[slot])

    def s_copy(w, i, slot):
        return copy(w.at[:, pl.ds(i * inter, inter)], wbuf.at[slot], wsem.at[slot])

    def e_copy(w, e, slot):
        return copy(w.at[e], wbuf.at[slot], wsem.at[slot])

    def down_copy(j, slot):
        c = j // blocks
        e = lax.rem(j, blocks)
        return copy(ed.at[pl.ds(PER * e, PER), :, pl.ds(pl.multiple_of(c * COLS, COLS), COLS)], dbuf.at[slot], dsem.at[slot])

    def sdown_copy(c, i, slot):
        at = pl.multiple_of((2 * c + i) * COLS, COLS)
        return copy(sd.at[:, :, pl.ds(at, COLS)], dbuf.at[slot, pl.ds(2 * i, 2)], ssem.at[slot, i])

    def remote(src, dst, send, recv, dev):
        return pltpu.make_async_remote_copy(src_ref=src, dst_ref=dst, send_sem=send, recv_sem=recv,
                                            device_id=dev, device_id_type=pl.DeviceIdType.MESH)

    per_buf = inter // wide
    q_view = []
    for i in range(Q_PARTS):
        if i < 2 * per_buf:
            q_view.append(wbuf.at[1 + i // per_buf, :, pl.ds((i % per_buf) * wide, wide)])
        else:
            q_view.append(act.at[:, :, pl.ds(q_wide + (i - 2 * per_buf) * wide, wide)])
    q_copies = [copy((wq if i < 2 * per_buf else wq3).at[..., pl.ds(i * wide, wide)], q_view[i], qsem.at[i])
                for i in range(Q_PARTS)]
    uk_view = [wbuf.at[1 + i, :, pl.ds(per_buf * wide, lat // 2)] for i in range(2)]
    uk_copies = [copy(wuk.at[:, pl.ds(i * (lat // 2), lat // 2)], uk_view[i], asem.at[i]) for i in range(2)]
    uv_copies = [copy(wuv.at[:, :, i], outc.at[:, :, :, pl.ds(i * vh, vh)], asem.at[2 + i]) for i in range(2)]
    dkv_copies = [copy(wdkv.at[pl.ds(0, lat)], xall.at[0], asem.at[4]),
                  copy(wdkv.at[pl.ds(lat, rot)], xall.at[1, pl.ds(0, rot)], asem.at[5])]
    o_copy = copy(wo, xall, asem.at[6])
    x_copy = copy(x_hbm, y_ref, asem.at[7])
    x_copy.start()
    for c in dkv_copies + uk_copies + q_copies:
        c.start()
    for i in range(SLOTS):
        c_copy(i).start()
    for c in uv_copies:
        c.start()
    s_copy(sg, 0, 0).start()

    lane = lax.broadcasted_iota(jnp.int32, (bsz, 128), 1)
    low = lane < rot
    front = lax.rem(lane, rot) < rot // 2

    with jax.named_scope('norm'):
        x_copy.wait()
        x = y_ref[...].astype(f32)
        xn = (x * lax.rsqrt(jnp.mean(x * x, axis=-1, keepdims=True) + EPS)).astype(bf16)
        turn_i = lax.broadcasted_iota(jnp.int32, (rot // 2, bsz), 0).astype(f32)
        ang = jnp.exp(turn_i * (-2.0 / rot * 9.210340371976184)) * pos_ref[...].astype(f32)
        cos_t = jnp.cos(ang)
        sin_t = jnp.sin(ang)
        cos = jnp.concatenate([cos_t] * 4, axis=0).T
        sin = jnp.concatenate([-sin_t, sin_t] * 2, axis=0).T
        r2[7, :, :128] = jnp.broadcast_to(pos_ref[...].astype(f32), (bsz, bsz)).T
        meta[...] = jnp.zeros(meta.shape, f32)
        meta[:top, :] = ids_ref[...].astype(f32)
        meta[8:8 + top, :] = rw_ref[...]

    def turn(r):
        swap = jnp.where(front, pltpu.roll(r, 128 - rot // 2, 1), pltpu.roll(r, rot // 2, 1))
        return (r * cos + swap * sin).astype(bf16).astype(f32)

    with jax.named_scope('kv_phase'):
        for c in dkv_copies:
            c.wait()
        c = dot_t(xn, xall[0])
        r = dot_t(xn, xall[1, :rot, :])
        o_copy.start()
        c = (c * lax.rsqrt(jnp.mean(c * c, axis=-1, keepdims=True) + EPS)).astype(bf16).astype(f32)
        r = turn(jnp.concatenate([r, jnp.zeros((bsz, 128 - rot), f32)], axis=1))
        r2[4] = c[:, :256]
        r2[5] = c[:, 256:]
        r2[6, :, :128] = r
        kv_ref[:lat, :] = c.T.astype(bf16)
        kv_ref[lat:, :] = r.T[:rot, :].astype(bf16)

    with jax.named_scope('q_phase'):
        for c in uk_copies:
            c.wait()
        for i in range(Q_PARTS):
            q_copies[i].wait()
            q = dot(xn, q_view[i][...].reshape(hid, wide)).astype(bf16).astype(f32)
            for j in range(wide // (2 * qkd)):
                at = 2 * qkd * j
                h = i * (wide // qkd) + 2 * j
                mid = q[:, at + nope:at + 2 * nope]
                last = q[:, at + 2 * nope:at + 3 * nope]
                n_a = q[:, at:at + nope]
                n_b = jnp.where(low, pltpu.roll(mid, rot, 1), pltpu.roll(last, rot, 1))
                r = turn(jnp.where(low, mid, last))
                other = pltpu.roll(r, rot, 1)
                pair = []
                for k, n, z in ((0, n_a, jnp.where(low, r, other)), (1, n_b, jnp.where(low, other, r))):
                    uk = jnp.concatenate([v[pl.ds((h + k) * nope, nope), :] for v in uk_view], axis=1)
                    ql = jnp.concatenate([dot(n.astype(bf16), uk), z], axis=1)
                    pair.append(ql.reshape(steps, GROUP, q_wide))
                act[:, pl.ds(h * GROUP, 2 * GROUP), :q_wide] = jnp.concatenate(pair, axis=1).astype(bf16)

    def ahead_copy(j):
        at = pl.ds(pl.multiple_of(j * piece, piece), piece)
        copy(su.at[at, pl.ds(0, inter)], wbuf.at[1, at], wsem.at[1]).start()
        copy(sg.at[at, pl.ds(inter, inter)], wbuf.at[2, at], wsem.at[2]).start()

    row = lax.rem(lax.broadcasted_iota(jnp.int32, (size, 128), 0), GROUP)

    def spread(v, width):
        keep = [jnp.where(row == g, 1.0, 0.0).astype(bf16) for g in range(GROUP)]
        return jnp.concatenate([v[:, t * 128:(t + 1) * 128] * keep[g]
                                for g in range(GROUP) for t in range(width // 128)], axis=1)

    def ahead(i):
        return pl.ds(pl.multiple_of(i * GROUP, GROUP), GROUP)

    def cached(i, g, first, count):
        return dbuf[lax.rem(i, SLOTS), g // 2, (g % 2) * kvd + first:(g % 2) * kvd + first + count, :]

    def scores(i, k):
        at = ahead(i)
        q = act[i, :, :q_wide]
        kv = jnp.concatenate([r2[4, at, :], r2[5, at, :], r2[6, at, :128]], axis=1)
        new = jnp.sum(q.astype(f32).reshape(heads, GROUP, q_wide) * kv[None], axis=2, keepdims=True)
        r2[2, :, k * 128:(k + 1) * 128] = jnp.broadcast_to(new.reshape(size, 1), (size, 128))
        tail = q[:, lat:]
        pairs = [tail * jnp.where(row == 2 * j + lane // rot, 1.0, 0.0).astype(bf16) for j in range(GROUP // 2)]
        c = jnp.concatenate([cached(i, g, 0, lat) for g in range(GROUP)], axis=0)
        r = jnp.concatenate([cached(i, g, lat, rot) for g in range(GROUP)], axis=0)
        r2[k] = dot(spread(q[:, :lat], lat), c) + dot(jnp.concatenate(pairs, axis=1), r)

    def soften(i, k):
        col = lax.broadcasted_iota(jnp.int32, (GROUP, rows), 1).astype(f32)
        live = col < r2[7, ahead(i), :1]
        s_new = r2[2, :, k * 128:k * 128 + 1] * scale
        s = (r2[k] * scale).reshape(heads, GROUP, rows)
        s = jnp.where(live[None], s, -jnp.inf).reshape(size, rows)
        mx = jnp.maximum(jnp.max(s, axis=1, keepdims=True), s_new)
        e = jnp.exp(s - mx)
        e_new = jnp.exp(s_new - mx)
        inv = 1.0 / (jnp.sum(e, axis=1, keepdims=True) + e_new)
        sact[k, :, :rows] = (e * inv).astype(bf16)
        r2[3, :, k * 128:(k + 1) * 128] = jnp.broadcast_to((e_new * inv).astype(bf16).astype(f32), (size, 128))

    def mix(i, k):
        at = ahead(i)
        c = jnp.concatenate([cached(i, g, 0, lat) for g in range(GROUP)], axis=1)
        o = dot_t(spread(sact[k, :, :rows], rows), c)
        p_new = r2[3, :, k * 128:(k + 1) * 128]
        p_new = jnp.concatenate([p_new, p_new], axis=1)
        for t in range(2):
            new = jnp.concatenate([r2[4 + t, at, :]] * heads, axis=0)
            ot = o[:, t * 256:(t + 1) * 256] + p_new * new
            for h in range(heads):
                part[h // 2, 2 * (h % 2) + t, at, :] = ot[h * GROUP:(h + 1) * GROUP, :]

    m_across = remote(meta, mall.at[1], ms_send.at[1], ms_recv.at[1], across)
    u_across = [remote(ub.at[pl.ds(i * half, half)], uall.at[1, pl.ds(i * half, half)],
                       us_send.at[1 + i], us_recv.at[1 + i], across) for i in range(2)]
    m_partner = remote(meta, mall.at[0], ms_send.at[0], ms_recv.at[0], partner)
    u_partner = remote(ub, uall.at[0], us_send.at[0], us_recv.at[0], partner)
    m_relay = remote(mall.at[1], mall.at[2], ms_send.at[2], ms_recv.at[2], partner)
    u_relay = [remote(uall.at[1, pl.ds(i * half, half)], uall.at[2, pl.ds(i * half, half)],
                      us_send.at[3 + i], us_recv.at[3 + i], partner) for i in range(2)]

    def project(i):
        at = slice(i * half, (i + 1) * half)
        if i == 0:
            for c in uv_copies:
                c.wait()
            o_copy.wait()
        for h in range(heads):
            o = jnp.concatenate([part[h // 2, 2 * (h % 2) + t, at, :] for t in range(2)], axis=1).astype(bf16)
            g = h // 2
            ub[at, h * vh:(h + 1) * vh] = dot(o, outc[g // 4, g % 4, :, (h % 2) * vh:(h % 2 + 1) * vh]).astype(bf16)
        a = dot(ub[at, :], xall[...].reshape(hid, hid))
        h1 = (y_ref[at, :].astype(f32) + a).astype(bf16)
        h = h1.astype(f32)
        ub[at, :] = (h * lax.rsqrt(jnp.mean(h * h, axis=-1, keepdims=True) + EPS)).astype(bf16)
        y_ref[at, :] = h1
        if i == 0:
            pl.semaphore_wait(barrier, 2)
            m_across.start()
            m_partner.start()
        u_across[i].start()
        if i == 1:
            u_partner.start()

    with jax.named_scope('attend_loop'):
        for i in range(2):
            c_copy(i).wait()
            scores(i, i)
        soften(0, 0)

        def attend(j, _):
            for k in (1, 0):
                c_copy(2 * j + 3 - k).wait()
            for k in (1, 0):
                i = 2 * j + 2 - k
                mix(i - 1, 1 - k)
                soften(i, k)
                scores(i + 1, 1 - k)

            @pl.when(2 * j + 1 + SLOTS < steps)
            def _():
                for k in range(2):
                    c_copy(2 * j + k + SLOTS).start()

            ahead_copy(j)

            @pl.when(j == steps // 4 - 1)
            def _():
                project(0)
            return 0

        lax.fori_loop(0, steps // 2 - 1, attend, 0)
        ahead_copy(steps // 2 - 1)
        mix(steps - 2, 0)
        soften(steps - 1, 1)
        mix(steps - 1, 1)

    with jax.named_scope('out_phase'):
        project(1)

    cuts = [(c * 256, min(256, inter - c * 256)) for c in range((inter + 255) // 256)]

    def glu(lhs, dst, g_slot, u_slot, g_copy, u_copy, g_next, u_next):
        g_copy.wait()
        g = dot(lhs, wbuf[g_slot])
        for n, (at, w) in enumerate(cuts):
            part[n // 4, n % 4, :, :w] = g[:, at:at + w]
        g_next()
        u_copy.wait()
        v = dot(lhs, wbuf[u_slot])
        g = jnp.concatenate([part[n // 4, n % 4, :, :w] for n, (at, w) in enumerate(cuts)], axis=1)
        dst[...] = (jax.nn.silu(g) * v).astype(bf16)
        u_next()

    with jax.named_scope('shared_up'):
        glu(ub[...], sact.at[0], 0, 1, s_copy(sg, 0, 0), s_copy(su, 0, 1),
            lambda: s_copy(su, 1, 0).start(), lambda: e_copy(eg, 0, 1).start())
        glu(ub[...], sact.at[1], 2, 0, s_copy(sg, 1, 2), s_copy(su, 1, 0),
            lambda: e_copy(eu, 0, 2).start(), lambda: e_copy(eg, 1, 0).start())

    for j in range(SLOTS):
        down_copy(j, j).start()
    with jax.named_scope('half_wait'):
        m_across.wait_recv()
        m_relay.start()
        u_across[0].wait_recv()
        u_relay[0].start()

    def dispatch(q, m, u):
        first = (me * n_loc).astype(f32)
        mine = lax.broadcasted_iota(jnp.int32, (n_loc, bsz), 0).astype(f32) + first
        hit = jnp.zeros((n_loc, bsz), f32)
        wgt = jnp.zeros((n_loc, bsz), f32)
        for k in range(top):
            eq = m[k:k + 1, :] == mine
            hit = jnp.where(eq, 1.0, hit)
            wgt = jnp.where(eq, m[8 + k:9 + k, :], wgt)
        r = lax.broadcasted_iota(jnp.int32, (bsz, bsz), 0)
        c = lax.broadcasted_iota(jnp.int32, (bsz, bsz), 1)
        before = jnp.where(r < c, 1.0, 0.0).astype(bf16)
        rank = jnp.where(hit > 0.0, dot(hit.astype(bf16), before), -1.0)
        slot = lax.broadcasted_iota(jnp.int32, (CAP, bsz), 0).astype(f32)
        sel = []
        ct = []
        for e in range(n_loc):
            at = slot == rank[e:e + 1, :]
            sel.append(jnp.where(at, 1.0, 0.0).astype(bf16))
            ct.append(jnp.where(at, wgt[e:e + 1, :], 0.0))
        c0 = jnp.concatenate(ct, axis=0).T
        for i in range(3):
            ci = c0.astype(bf16)
            comb[q, pl.ds(i * bsz, bsz), :] = ci
            c0 = c0 - ci.astype(f32)
        xall[q] = dot(jnp.concatenate(sel, axis=0), u).astype(bf16)

    with jax.named_scope('disp01'):
        dispatch(OWN, meta[...], ub[...])
        m_partner.wait_recv()
        u_partner.wait_recv()
        dispatch(NEAR, mall[0], uall[0])
    with jax.named_scope('gather_wait'):
        u_across[1].wait_recv()
        u_relay[1].start()
    with jax.named_scope('disp2'):
        dispatch(ACROSS, mall[1], uall[1])
    with jax.named_scope('relay_wait'):
        m_relay.wait_recv()
        for i in range(2):
            u_relay[i].wait_recv()
    with jax.named_scope('disp3'):
        dispatch(FAR, mall[2], uall[2])

    def expert(e, _):
        g_slot = lax.rem(4 + 2 * e, RING)
        u_slot = lax.rem(5 + 2 * e, RING)
        lhs = xall[:, pl.ds(pl.multiple_of(e * CAP, CAP), CAP), :].reshape(4 * CAP, hid)

        def g_next():
            @pl.when(e + 1 < n_loc)
            def _():
                e_copy(eu, e + 1, g_slot).start()

        def u_next():
            @pl.when(e + 2 < n_loc)
            def _():
                e_copy(eg, e + 2, u_slot).start()

        glu(lhs, act.at[e], g_slot, u_slot, e_copy(eg, e, g_slot), e_copy(eu, e, u_slot), g_next, u_next)
        return 0

    with jax.named_scope('experts'):
        lax.fori_loop(0, n_loc, expert, 0)

    def ring1(c, i):
        return remote(part.at[c, i], r1.at[c, LAND[i]], s1_send.at[c, LAND[i]], s1_recv.at[c, LAND[i]], partner)

    def ring2(c):
        return remote(part.at[c, ACROSS], r2.at[c], s2_send.at[c], s2_recv.at[c], across)

    def fold(c):
        ring1(c, FAR).wait_recv()
        part[c, ACROSS] = part[c, ACROSS] + r1[c, LAND[FAR]]

    def combine(c, q):
        p = dot(comb[q], outc[lax.rem(c, 2), q])
        part[c, q] = p[:bsz] + p[bsz:2 * bsz] + p[2 * bsz:]

    def down_step(c, e, early):
        j = c * blocks + e
        slot = lax.rem(j, SLOTS)
        down_copy(j, slot).wait()
        if early is not None:
            early()
        for i in range(PER):
            res = dot(act[PER * e + i], dbuf[slot, i]).astype(bf16)
            outc[lax.rem(c, 2), :, pl.ds(pl.multiple_of((PER * e + i) * CAP, CAP), CAP), :] = res.reshape(4, CAP, COLS)

        @pl.when(j + SLOTS < n_down)
        def _():
            down_copy(j + SLOTS, slot).start()

        @pl.when((j + SLOTS >= n_down) & (j + SLOTS < n_down + n_col // 2))
        def _():
            for i in range(2):
                sdown_copy(j + SLOTS - n_down, i, slot).start()

    def first(e, _):
        down_step(0, e, None)
        return 0

    def column(c, _):
        def step(e, _):
            @pl.when(e == 1)
            def _():
                ring1(c - 1, FAR).start()

            @pl.when(e == 3)
            def _():
                ring2(c - 1).start()
                ring1(c - 1, NEAR).start()

            down_step(c, e, lambda: combine(c - 1, e))

            @pl.when(e == 2)
            def _():
                fold(c - 1)
            return 0

        lax.fori_loop(0, blocks, step, 0)
        return 0

    with jax.named_scope('column0'):
        lax.fori_loop(0, blocks, first, 0)
    with jax.named_scope('columns'):
        lax.fori_loop(1, n_col, column, 0)

    last = n_col - 1
    with jax.named_scope('combine'):
        combine(last, FAR)
        combine(last, ACROSS)
        ring1(last, FAR).start()
        combine(last, NEAR)
        combine(last, OWN)
        ring1(last, NEAR).start()

    with jax.named_scope('shared_down'):
        for c in range(n_col // 2):
            slot = (n_down + c) % SLOTS
            for i in range(2):
                sdown_copy(c, i, slot).wait()
                part[2 * c + i, OWN] = (part[2 * c + i, OWN] + dot(sact[0], dbuf[slot, 2 * i])
                                        + dot(sact[1], dbuf[slot, 2 * i + 1]))
                if c == 0 and i == 0:
                    fold(last)
                if c == 0 and i == 1:
                    ring2(last).start()

    with jax.named_scope('tail'):
        for c in range(n_col):
            ring1(c, NEAR).wait_recv()
            ring2(c).wait_recv()
            at = slice(c * COLS, (c + 1) * COLS)
            y_ref[:, at] = (y_ref[:, at].astype(f32) + ((part[c, OWN] + r1[c, LAND[NEAR]]) + r2[c])).astype(bf16)

    for c in (m_across, *u_across, m_partner, u_partner, m_relay, *u_relay):
        c.wait_send()
    for c in range(n_col):
        ring1(c, FAR).wait_send()
        ring1(c, NEAR).wait_send()
        ring2(c).wait_send()


def solution(mesh):
    tok_spec = P(('rep', 'ep'))
    row_spec = P(('rep', 'ep'), None)
    cache_spec = P(('rep', 'ep'), None, None)
    exp_spec = P('ep', None, None)

    def local(x, cache, lens, ids, rw, w_q, w_dkv, w_uk, w_uv, w_o, s_gate, s_up, s_down, e_gate, e_up, e_down):
        bsz, hid = x.shape
        heads, nope, lat = w_uk.shape
        rows, kvd = cache.shape[1:]
        vh = w_uv.shape[2]
        n_loc, _, inter = e_gate.shape
        n_col = hid // COLS
        bf16, f32 = jnp.bfloat16, jnp.float32
        vm = pl.BlockSpec(memory_space=pltpu.VMEM)
        hbm = pl.BlockSpec(memory_space=pl.ANY)
        dma = pltpu.SemaphoreType.DMA
        y, kv = pl.pallas_call(
            layer,
            out_shape=(jax.ShapeDtypeStruct((bsz, hid), bf16), jax.ShapeDtypeStruct((kvd, bsz), bf16)),
            in_specs=[hbm] + [vm] * 3 + [hbm] * 13,
            out_specs=(vm, vm),
            scratch_shapes=[
                pltpu.VMEM((RING, hid, inter), bf16),
                pltpu.VMEM((SLOTS, PER, inter, COLS), bf16),
                pltpu.VMEM((4, n_loc * CAP, hid), bf16),
                pltpu.VMEM((n_loc, 4 * CAP, inter), bf16),
                pltpu.VMEM((2, bsz, inter), bf16),
                pltpu.VMEM((2, 4, n_loc * CAP, COLS), bf16),
                pltpu.VMEM((4, 3 * bsz, n_loc * CAP), bf16),
                pltpu.VMEM((3, bsz, hid), bf16),
                pltpu.VMEM((3, 16, bsz), f32),
                pltpu.VMEM((16, bsz), f32),
                pltpu.VMEM((n_col, 4, bsz, COLS), f32),
                pltpu.VMEM((n_col, 2, bsz, COLS), f32),
                pltpu.VMEM((n_col, bsz, COLS), f32),
                pltpu.VMEM((bsz, hid), bf16),
                dma((RING,)), dma((SLOTS,)), dma((SLOTS, 2)), dma((Q_PARTS,)), dma((8,)),
                dma((5,)), dma((5,)), dma((3,)), dma((3,)),
                dma((n_col, 2)), dma((n_col, 2)), dma((n_col,)), dma((n_col,)),
            ],
            compiler_params=pltpu.CompilerParams(
                collective_id=0, has_side_effects=True, vmem_limit_bytes=67043328),
            name='layer',
        )(x, lens[None, :], ids.T, rw.T, cache.transpose(0, 2, 1).reshape(bsz // 2, 2 * kvd, rows),
          w_q, w_q.reshape(n_loc, hid // n_loc, w_q.shape[1]), w_dkv.T, w_uk.reshape(heads * nope, lat),
          w_uv.reshape(2, 4, 2, lat, vh), w_o.reshape(4, hid // 4, hid),
          s_gate, s_up, s_down.reshape(2, inter, hid), e_gate, e_up, e_down)
        return y, kv.T

    in_specs = (row_spec, cache_spec, tok_spec, row_spec, row_spec) + (P(),) * 8 + (exp_spec,) * 3
    return jax.shard_map(local, mesh=mesh, in_specs=in_specs, out_specs=(row_spec, row_spec), check_vma=False)
```

```python
import jax
import jax.numpy as jnp
from jax import lax
from jax.experimental import pallas as pl
from jax.experimental.pallas import tpu as pltpu
from jax.sharding import PartitionSpec as P

EPS = 1e-6
ROPE_BASE = 1.0e4
CAP = 32
COLS = 256
PER = 4
RING = 3
SLOTS = 6
GROUP = 8
Q_PARTS = 8
FAR, ACROSS, NEAR, OWN = range(4)
LAND = {FAR: 0, NEAR: 1}


def dot(a, b):
    return jnp.dot(a, b, preferred_element_type=jnp.float32)


def dot_t(a, b):
    return lax.dot_general(a, b, (((1,), (1,)), ((), ())), preferred_element_type=jnp.float32)


def layer(x_hbm, pos_ref, ids_ref, rw_ref, cache, wq, wq3, wdkv, wuk, wuv, wo, sg, su, sd, eg, eu, ed,
          y_ref, kv_ref,
          wbuf, dbuf, xall, act, sact, outc, comb, uall, mall, meta, part, r1, r2, ub,
          wsem, dsem, ssem, qsem, asem, us_send, us_recv, ms_send, ms_recv, s1_send, s1_recv, s2_send, s2_recv):
    f32, bf16 = jnp.float32, jnp.bfloat16
    bsz, hid = x_hbm.shape
    kvd, rows = cache.shape[1] // 2, cache.shape[2]
    lat = wuk.shape[2]
    rot = kvd - lat
    vh = wuv.shape[4]
    heads = hid // vh
    nope = hid // heads
    qkd = nope + rot
    steps = bsz // GROUP
    wide = heads * qkd // Q_PARTS
    scale = qkd ** -0.5
    size = heads * GROUP
    n_loc = eg.shape[0]
    inter = eg.shape[2]
    n_col = hid // COLS
    blocks = n_loc // PER
    n_down = n_col * blocks
    half = bsz // 2
    top = ids_ref.shape[0]
    me = lax.axis_index('ep')
    partner = {'ep': me + 1 - 2 * lax.rem(me, 2)}
    across = {'ep': lax.rem(me + 2, 4)}
    q_wide = (lat // 128 + 1) * 128
    piece = hid // 4

    barrier = pltpu.get_barrier_semaphore()
    for dev in (partner, across):
        pl.semaphore_signal(barrier, inc=1, device_id=dev, device_id_type=pl.DeviceIdType.MESH)

    def copy(src, dst, sem):
        return pltpu.make_async_copy(src, dst, sem)

    def c_copy(i):
        slot = lax.rem(i, SLOTS)
        return copy(cache.at[pl.ds(i * (GROUP // 2), GROUP // 2)], dbuf.at[slot, :, pl.ds(0, 2 * kvd), :], dsem.at[slot])

    deep = hid // 2

    def s_copy(w, i, slot):
        return [copy(w.at[pl.ds(k * deep, deep), pl.ds(i * inter, inter)], wbuf.at[2 * slot + k], wsem.at[2 * slot + k])
                for k in range(2)]

    def e_copy(w, e, slot):
        return [copy(w.at[e, pl.ds(k * deep, deep)], wbuf.at[2 * slot + k], wsem.at[2 * slot + k]) for k in range(2)]

    def down_copy(j, slot):
        c = j // blocks
        e = lax.rem(j, blocks)
        return copy(ed.at[pl.ds(PER * e, PER), :, pl.ds(pl.multiple_of(c * COLS, COLS), COLS)], dbuf.at[slot], dsem.at[slot])

    def sdown_copy(c, i, slot):
        at = pl.multiple_of((2 * c + i) * COLS, COLS)
        return copy(sd.at[:, :, pl.ds(at, COLS)], dbuf.at[slot, pl.ds(2 * i, 2)], ssem.at[slot, i])

    def remote(src, dst, send, recv, dev):
        return pltpu.make_async_remote_copy(src_ref=src, dst_ref=dst, send_sem=send, recv_sem=recv,
                                            device_id=dev, device_id_type=pl.DeviceIdType.MESH)

    per_buf = inter // wide
    q_view = []
    for i in range(Q_PARTS):
        if i < 2 * per_buf:
            q_view.append(wbuf.at[pl.ds(2 + 2 * (i // per_buf), 2), :, pl.ds((i % per_buf) * wide, wide)])
        else:
            q_view.append(act.at[:, :, pl.ds(q_wide + (i - 2 * per_buf) * wide, wide)])
    q_copies = [copy((wq if i < 2 * per_buf else wq3).at[..., pl.ds(i * wide, wide)], q_view[i], qsem.at[i])
                for i in range(Q_PARTS)]
    uk_view = [wbuf.at[pl.ds(2 + 2 * i, 2), :, pl.ds(per_buf * wide, lat // 2)] for i in range(2)]
    uk_copies = [copy(wuk.at[:, :, pl.ds(i * (lat // 2), lat // 2)], uk_view[i], asem.at[i]) for i in range(2)]
    uv_copies = [copy(wuv.at[:, :, i], outc.at[:, :, :, pl.ds(i * vh, vh)], asem.at[2 + i]) for i in range(2)]
    dkv_copies = [copy(wdkv.at[pl.ds(0, lat)], xall.at[0], asem.at[4]),
                  copy(wdkv.at[pl.ds(lat, rot)], xall.at[1, pl.ds(0, rot)], asem.at[5])]
    o_copy = copy(wo, xall, asem.at[6])
    x_copy = copy(x_hbm, y_ref, asem.at[7])
    x_copy.start()
    for c in dkv_copies + uk_copies + q_copies[:3]:
        c.start()
    later = q_copies[3:] + [c_copy(i) for i in range(SLOTS)] + uv_copies + [copy(wo.at[0], xall.at[0], asem.at[6])]

    lane = lax.broadcasted_iota(jnp.int32, (bsz, 128), 1)
    low = lane < rot
    front = lax.rem(lane, rot) < rot // 2

    with jax.named_scope('norm'):
        x_copy.wait()
        x = y_ref[...].astype(f32)
        xn = (x * lax.rsqrt(jnp.mean(x * x, axis=-1, keepdims=True) + EPS)).astype(bf16)
        turn_i = lax.broadcasted_iota(jnp.int32, (rot // 2, bsz), 0).astype(f32)
        ang = jnp.exp(turn_i * (-2.0 / rot * 9.210340371976184)) * pos_ref[...].astype(f32)
        cos_t = jnp.cos(ang)
        sin_t = jnp.sin(ang)
        cos = jnp.concatenate([cos_t] * 4, axis=0).T
        sin = jnp.concatenate([-sin_t, sin_t] * 2, axis=0).T
        r2[7, :, :128] = jnp.broadcast_to(pos_ref[...].astype(f32), (bsz, bsz)).T
        meta[...] = jnp.zeros(meta.shape, f32)
        meta[:top, :] = ids_ref[...].astype(f32)
        meta[8:8 + top, :] = rw_ref[...]

    def turn(r):
        swap = jnp.where(front, pltpu.roll(r, 128 - rot // 2, 1), pltpu.roll(r, rot // 2, 1))
        return (r * cos + swap * sin).astype(bf16).astype(f32)

    with jax.named_scope('kv_phase'):
        for c in dkv_copies:
            c.wait()
        c = dot_t(xn, xall[0])
        r = dot_t(xn, xall[1, :rot, :])
        later.pop(0).start()
        c = (c * lax.rsqrt(jnp.mean(c * c, axis=-1, keepdims=True) + EPS)).astype(bf16).astype(f32)
        r = turn(jnp.concatenate([r, jnp.zeros((bsz, 128 - rot), f32)], axis=1))
        r2[4] = c[:, :256]
        r2[5] = c[:, 256:]
        r2[6, :, :128] = r
        kv_ref[:lat, :] = c.T.astype(bf16)
        kv_ref[lat:, :] = r.T[:rot, :].astype(bf16)

    with jax.named_scope('q_phase'):
        for c in uk_copies:
            c.wait()
        def project_q(i):
            q_copies[i].wait()
            later.pop(0).start()
            return dot(xn, q_view[i][...].reshape(hid, wide)).astype(bf16).astype(f32)

        def place(i, q):
            for j in range(wide // (2 * qkd)):
                at = 2 * qkd * j
                h = i * (wide // qkd) + 2 * j
                mid = q[:, at + nope:at + 2 * nope]
                last = q[:, at + 2 * nope:at + 3 * nope]
                n_a = q[:, at:at + nope]
                n_b = jnp.where(low, pltpu.roll(mid, rot, 1), pltpu.roll(last, rot, 1))
                r = turn(jnp.where(low, mid, last))
                other = pltpu.roll(r, rot, 1)
                pair = []
                for k, n, z in ((0, n_a, jnp.where(low, r, other)), (1, n_b, jnp.where(low, other, r))):
                    uk = jnp.concatenate([v[(h + k) * nope // deep, pl.ds((h + k) * nope % deep, nope), :] for v in uk_view], axis=1)
                    ql = jnp.concatenate([dot(n.astype(bf16), uk), z], axis=1)
                    pair.append(ql.reshape(steps, GROUP, q_wide))
                act[:, pl.ds(h * GROUP, 2 * GROUP), :q_wide] = jnp.concatenate(pair, axis=1).astype(bf16)

        q = project_q(0)
        for i in range(Q_PARTS):
            then = project_q(i + 1) if i + 1 < Q_PARTS else None
            place(i, q)
            q = then
        for c in later:
            c.start()

    def ahead_copy(j):
        at = pl.ds(pl.multiple_of(j * piece, piece), piece)
        k = j // 2
        to = pl.ds(pl.multiple_of(lax.rem(j, 2) * piece, piece), piece)
        copy(sg.at[at, pl.ds(0, inter)], wbuf.at[k, to], wsem.at[k]).start()
        copy(su.at[at, pl.ds(0, inter)], wbuf.at[2 + k, to], wsem.at[2 + k]).start()

    row = lax.rem(lax.broadcasted_iota(jnp.int32, (size, 128), 0), GROUP)

    def spread(v, width):
        keep = [jnp.where(row == g, 1.0, 0.0).astype(bf16) for g in range(GROUP)]
        return jnp.concatenate([v[:, t * 128:(t + 1) * 128] * keep[g]
                                for g in range(GROUP) for t in range(width // 128)], axis=1)

    def ahead(i):
        return pl.ds(pl.multiple_of(i * GROUP, GROUP), GROUP)

    def cached(i, g, first, count):
        return dbuf[lax.rem(i, SLOTS), g // 2, (g % 2) * kvd + first:(g % 2) * kvd + first + count, :]

    def scores(i, k):
        at = ahead(i)
        q = act[i, :, :q_wide]
        kv = jnp.concatenate([r2[4, at, :], r2[5, at, :], r2[6, at, :128]], axis=1)
        new = jnp.sum(q.astype(f32).reshape(heads, GROUP, q_wide) * kv[None], axis=2, keepdims=True)
        r2[2, :, k * 128:(k + 1) * 128] = jnp.broadcast_to(new.reshape(size, 1), (size, 128))
        tail = q[:, lat:]
        pairs = [tail * jnp.where(row == 2 * j + lane // rot, 1.0, 0.0).astype(bf16) for j in range(GROUP // 2)]
        c = jnp.concatenate([cached(i, g, 0, lat) for g in range(GROUP)], axis=0)
        r = jnp.concatenate([cached(i, g, lat, rot) for g in range(GROUP)], axis=0)
        r2[k] = dot(spread(q[:, :lat], lat), c) + dot(jnp.concatenate(pairs, axis=1), r)

    def soften(i, k):
        col = lax.broadcasted_iota(jnp.int32, (GROUP, rows), 1).astype(f32)
        live = col < r2[7, ahead(i), :1]
        s_new = r2[2, :, k * 128:k * 128 + 1] * scale
        s = (r2[k] * scale).reshape(heads, GROUP, rows)
        s = jnp.where(live[None], s, -jnp.inf).reshape(size, rows)
        mx = jnp.maximum(jnp.max(s, axis=1, keepdims=True), s_new)
        e = jnp.exp(s - mx)
        e_new = jnp.exp(s_new - mx)
        inv = 1.0 / (jnp.sum(e, axis=1, keepdims=True) + e_new)
        sact[k, :, :rows] = (e * inv).astype(bf16)
        r2[3, :, k * 128:(k + 1) * 128] = jnp.broadcast_to((e_new * inv).astype(bf16).astype(f32), (size, 128))

    def mix(i, k):
        at = ahead(i)
        c = jnp.concatenate([cached(i, g, 0, lat) for g in range(GROUP)], axis=1)
        o = dot_t(spread(sact[k, :, :rows], rows), c)
        p_new = r2[3, :, k * 128:(k + 1) * 128]
        p_new = jnp.concatenate([p_new, p_new], axis=1)
        for t in range(2):
            new = jnp.concatenate([r2[4 + t, at, :]] * heads, axis=0)
            ot = o[:, t * 256:(t + 1) * 256] + p_new * new
            for h in range(heads):
                part[h // 2, 2 * (h % 2) + t, at, :] = ot[h * GROUP:(h + 1) * GROUP, :]

    m_across = remote(meta, mall.at[1], ms_send.at[1], ms_recv.at[1], across)
    u_across = [remote(ub.at[pl.ds(i * half, half)], uall.at[1, pl.ds(i * half, half)],
                       us_send.at[1 + i], us_recv.at[1 + i], across) for i in range(2)]
    m_partner = remote(meta, mall.at[0], ms_send.at[0], ms_recv.at[0], partner)
    u_partner = remote(ub, uall.at[0], us_send.at[0], us_recv.at[0], partner)
    m_relay = remote(mall.at[1], mall.at[2], ms_send.at[2], ms_recv.at[2], partner)
    u_relay = [remote(uall.at[1, pl.ds(i * half, half)], uall.at[2, pl.ds(i * half, half)],
                      us_send.at[3 + i], us_recv.at[3 + i], partner) for i in range(2)]

    def project(i):
        at = slice(i * half, (i + 1) * half)
        if i == 0:
            for c in uv_copies:
                c.wait()
            o_copy.wait()
        for h in range(heads):
            o = jnp.concatenate([part[h // 2, 2 * (h % 2) + t, at, :] for t in range(2)], axis=1).astype(bf16)
            g = h // 2
            ub[at, h * vh:(h + 1) * vh] = dot(o, outc[g // 4, g % 4, :, (h % 2) * vh:(h % 2 + 1) * vh]).astype(bf16)
        a = dot(ub[at, :], xall[...].reshape(hid, hid))
        h1 = (y_ref[at, :].astype(f32) + a).astype(bf16)
        h = h1.astype(f32)
        ub[at, :] = (h * lax.rsqrt(jnp.mean(h * h, axis=-1, keepdims=True) + EPS)).astype(bf16)
        y_ref[at, :] = h1
        if i == 0:
            pl.semaphore_wait(barrier, 2)
            m_across.start()
            m_partner.start()
        u_across[i].start()
        if i == 1:
            u_partner.start()

    with jax.named_scope('attend_loop'):
        for i in range(2):
            c_copy(i).wait()
            scores(i, i)
        soften(0, 0)

        def attend(j, _):
            for k in (1, 0):
                c_copy(2 * j + 3 - k).wait()
            for k in (1, 0):
                i = 2 * j + 2 - k
                mix(i - 1, 1 - k)
                soften(i, k)
                scores(i + 1, 1 - k)

            @pl.when(2 * j + 1 + SLOTS < steps)
            def _():
                for k in range(2):
                    c_copy(2 * j + k + SLOTS).start()

            @pl.when(j < 3)
            def _():
                copy(wo.at[j + 1], xall.at[j + 1], asem.at[6]).start()

            @pl.when(j >= 3)
            def _():
                ahead_copy(j - 3)

            @pl.when(j == steps // 4 - 1)
            def _():
                project(0)
            return 0

        lax.fori_loop(0, steps // 2 - 1, attend, 0)
        for c in s_copy(sg, 1, 2):
            c.start()
        mix(steps - 2, 0)
        soften(steps - 1, 1)
        mix(steps - 1, 1)

    with jax.named_scope('out_phase'):
        project(1)

    cuts = [(c * 256, min(256, inter - c * 256)) for c in range((inter + 255) // 256)]

    def glu(lhs, dst, g_slot, u_slot, g_copy, u_copy, g_next, u_next):
        def gate(n, at, w):
            return part.at[n // 4, n % 4, :, pl.ds(0, w)]

        g_copy[0].wait()
        g = dot(lhs(0), wbuf[2 * g_slot])
        for n, (at, w) in enumerate(cuts):
            gate(n, at, w)[...] = g[:, at:at + w]
        g_next(0)
        g_copy[1].wait()
        g = dot(lhs(1), wbuf[2 * g_slot + 1])
        for n, (at, w) in enumerate(cuts):
            gate(n, at, w)[...] += g[:, at:at + w]
        g_next(1)
        u_copy[0].wait()
        v = dot(lhs(0), wbuf[2 * u_slot])
        for n, (at, w) in enumerate(cuts):
            part[2 + n // 4, n % 4, :, :w] = v[:, at:at + w]
        u_next(0)
        u_copy[1].wait()
        v = dot(lhs(1), wbuf[2 * u_slot + 1])
        v = v + jnp.concatenate([part[2 + n // 4, n % 4, :, :w] for n, (at, w) in enumerate(cuts)], axis=1)
        g = jnp.concatenate([gate(n, at, w)[...] for n, (at, w) in enumerate(cuts)], axis=1)
        dst[...] = (jax.nn.silu(g) * v).astype(bf16)
        u_next(1)

    with jax.named_scope('shared_up'):
        def mine(k):
            return ub[:, k * deep:(k + 1) * deep]

        glu(mine, sact.at[0], 0, 1, s_copy(sg, 0, 0), s_copy(su, 0, 1),
            lambda k: s_copy(su, 1, 0)[k].start(), lambda k: e_copy(eg, 0, 1)[k].start())
        glu(mine, sact.at[1], 2, 0, s_copy(sg, 1, 2), s_copy(su, 1, 0),
            lambda k: e_copy(eu, 0, 2)[k].start(), lambda k: e_copy(eg, 1, 0)[k].start())

    for j in range(SLOTS):
        down_copy(j, j).start()
    with jax.named_scope('half_wait'):
        m_across.wait_recv()
        m_relay.start()
        u_across[0].wait_recv()
        u_relay[0].start()

    def dispatch(q, m, u):
        first = (me * n_loc).astype(f32)
        mine = lax.broadcasted_iota(jnp.int32, (n_loc, bsz), 0).astype(f32) + first
        hit = jnp.zeros((n_loc, bsz), f32)
        wgt = jnp.zeros((n_loc, bsz), f32)
        for k in range(top):
            eq = m[k:k + 1, :] == mine
            hit = jnp.where(eq, 1.0, hit)
            wgt = jnp.where(eq, m[8 + k:9 + k, :], wgt)
        r = lax.broadcasted_iota(jnp.int32, (bsz, bsz), 0)
        c = lax.broadcasted_iota(jnp.int32, (bsz, bsz), 1)
        before = jnp.where(r < c, 1.0, 0.0).astype(bf16)
        rank = jnp.where(hit > 0.0, dot(hit.astype(bf16), before), -1.0)
        slot = lax.broadcasted_iota(jnp.int32, (CAP, bsz), 0).astype(f32)
        sel = []
        ct = []
        for e in range(n_loc):
            at = slot == rank[e:e + 1, :]
            sel.append(jnp.where(at, 1.0, 0.0).astype(bf16))
            ct.append(jnp.where(at, wgt[e:e + 1, :], 0.0))
        c0 = jnp.concatenate(ct, axis=0).T
        for i in range(3):
            ci = c0.astype(bf16)
            comb[q, pl.ds(i * bsz, bsz), :] = ci
            c0 = c0 - ci.astype(f32)
        xall[q] = dot(jnp.concatenate(sel, axis=0), u).astype(bf16)

    with jax.named_scope('disp01'):
        dispatch(OWN, meta[...], ub[...])
        m_partner.wait_recv()
        u_partner.wait_recv()
        dispatch(NEAR, mall[0], uall[0])
    with jax.named_scope('gather_wait'):
        u_across[1].wait_recv()
        u_relay[1].start()
    with jax.named_scope('disp2'):
        dispatch(ACROSS, mall[1], uall[1])
    with jax.named_scope('relay_wait'):
        m_relay.wait_recv()
        for i in range(2):
            u_relay[i].wait_recv()
    with jax.named_scope('disp3'):
        dispatch(FAR, mall[2], uall[2])

    def expert(e, _):
        g_slot = lax.rem(4 + 2 * e, RING)
        u_slot = lax.rem(5 + 2 * e, RING)

        def lhs(k):
            at = pl.ds(pl.multiple_of(e * CAP, CAP), CAP)
            return xall[:, at, k * deep:(k + 1) * deep].reshape(4 * CAP, deep)

        def g_next(k):
            @pl.when(e + 1 < n_loc)
            def _():
                e_copy(eu, e + 1, g_slot)[k].start()

        def u_next(k):
            @pl.when(e + 2 < n_loc)
            def _():
                e_copy(eg, e + 2, u_slot)[k].start()

        glu(lhs, act.at[e], g_slot, u_slot, e_copy(eg, e, g_slot), e_copy(eu, e, u_slot), g_next, u_next)
        return 0

    with jax.named_scope('experts'):
        lax.fori_loop(0, n_loc, expert, 0)

    def ring1(c, i):
        return remote(part.at[c, i], r1.at[c, LAND[i]], s1_send.at[c, LAND[i]], s1_recv.at[c, LAND[i]], partner)

    def ring2(c):
        return remote(part.at[c, ACROSS], r2.at[c], s2_send.at[c], s2_recv.at[c], across)

    def fold(c):
        ring1(c, FAR).wait_recv()
        part[c, ACROSS] = part[c, ACROSS] + r1[c, LAND[FAR]]

    def combine(c, q):
        p = dot(comb[q], outc[lax.rem(c, 2), q])
        part[c, q] = p[:bsz] + p[bsz:2 * bsz] + p[2 * bsz:]

    def down_step(c, e, early):
        j = c * blocks + e
        slot = lax.rem(j, SLOTS)
        down_copy(j, slot).wait()
        if early is not None:
            early()
        for i in range(PER):
            res = dot(act[PER * e + i], dbuf[slot, i]).astype(bf16)
            outc[lax.rem(c, 2), :, pl.ds(pl.multiple_of((PER * e + i) * CAP, CAP), CAP), :] = res.reshape(4, CAP, COLS)

        @pl.when(j + SLOTS < n_down)
        def _():
            down_copy(j + SLOTS, slot).start()

        @pl.when((j + SLOTS >= n_down) & (j + SLOTS < n_down + n_col // 2))
        def _():
            for i in range(2):
                sdown_copy(j + SLOTS - n_down, i, slot).start()

    def first(e, _):
        down_step(0, e, None)
        return 0

    def column(c, _):
        def step(e, _):
            @pl.when(e == 1)
            def _():
                ring1(c - 1, FAR).start()

            @pl.when(e == 3)
            def _():
                ring2(c - 1).start()
                ring1(c - 1, NEAR).start()

            down_step(c, e, lambda: combine(c - 1, e))

            @pl.when(e == 2)
            def _():
                fold(c - 1)
            return 0

        lax.fori_loop(0, blocks, step, 0)
        return 0

    with jax.named_scope('column0'):
        lax.fori_loop(0, blocks, first, 0)
    with jax.named_scope('columns'):
        lax.fori_loop(1, n_col, column, 0)

    last = n_col - 1
    with jax.named_scope('combine'):
        combine(last, FAR)
        combine(last, ACROSS)
        ring1(last, FAR).start()
        combine(last, NEAR)
        combine(last, OWN)
        ring1(last, NEAR).start()

    with jax.named_scope('shared_down'):
        for c in range(n_col // 2):
            slot = (n_down + c) % SLOTS
            for i in range(2):
                sdown_copy(c, i, slot).wait()
            for i in range(2):
                part[2 * c + i, OWN] = (part[2 * c + i, OWN] + dot(sact[0], dbuf[slot, 2 * i])
                                        + dot(sact[1], dbuf[slot, 2 * i + 1]))
            if c == 0:
                fold(last)
                ring2(last).start()

    with jax.named_scope('tail'):
        for c in range(n_col):
            ring1(c, NEAR).wait_recv()
            ring2(c).wait_recv()
            at = slice(c * COLS, (c + 1) * COLS)
            y_ref[:, at] = (y_ref[:, at].astype(f32) + ((part[c, OWN] + r1[c, LAND[NEAR]]) + r2[c])).astype(bf16)

    for c in (m_across, *u_across, m_partner, u_partner, m_relay, *u_relay):
        c.wait_send()
    for c in range(n_col):
        ring1(c, FAR).wait_send()
        ring1(c, NEAR).wait_send()
        ring2(c).wait_send()


def settle(y_in, kv_in, y_ref, kv_ref):
    y_ref[...] = y_in[...]
    kv_ref[...] = kv_in[...]


def solution(mesh):
    tok_spec = P(('rep', 'ep'))
    row_spec = P(('rep', 'ep'), None)
    cache_spec = P(('rep', 'ep'), None, None)
    exp_spec = P('ep', None, None)

    def local(x, cache, lens, ids, rw, w_q, w_dkv, w_uk, w_uv, w_o, s_gate, s_up, s_down, e_gate, e_up, e_down):
        bsz, hid = x.shape
        heads, nope, lat = w_uk.shape
        rows, kvd = cache.shape[1:]
        vh = w_uv.shape[2]
        n_loc, _, inter = e_gate.shape
        n_col = hid // COLS
        bf16, f32 = jnp.bfloat16, jnp.float32
        vm = pl.BlockSpec(memory_space=pltpu.VMEM)
        hbm = pl.BlockSpec(memory_space=pl.ANY)
        dma = pltpu.SemaphoreType.DMA
        y, kv = pl.pallas_call(
            layer,
            out_shape=(jax.ShapeDtypeStruct((bsz, hid), bf16), jax.ShapeDtypeStruct((kvd, bsz), bf16)),
            in_specs=[hbm] + [vm] * 3 + [hbm] * 13,
            out_specs=(vm, vm),
            scratch_shapes=[
                pltpu.VMEM((2 * RING, hid // 2, inter), bf16),
                pltpu.VMEM((SLOTS, PER, inter, COLS), bf16),
                pltpu.VMEM((4, n_loc * CAP, hid), bf16),
                pltpu.VMEM((n_loc, 4 * CAP, inter), bf16),
                pltpu.VMEM((2, bsz, inter), bf16),
                pltpu.VMEM((2, 4, n_loc * CAP, COLS), bf16),
                pltpu.VMEM((4, 3 * bsz, n_loc * CAP), bf16),
                pltpu.VMEM((3, bsz, hid), bf16),
                pltpu.VMEM((3, 16, bsz), f32),
                pltpu.VMEM((16, bsz), f32),
                pltpu.VMEM((n_col, 4, bsz, COLS), f32),
                pltpu.VMEM((n_col, 2, bsz, COLS), f32),
                pltpu.VMEM((n_col, bsz, COLS), f32),
                pltpu.VMEM((bsz, hid), bf16),
                dma((2 * RING,)), dma((SLOTS,)), dma((SLOTS, 2)), dma((Q_PARTS,)), dma((8,)),
                dma((5,)), dma((5,)), dma((3,)), dma((3,)),
                dma((n_col, 2)), dma((n_col, 2)), dma((n_col,)), dma((n_col,)),
            ],
            compiler_params=pltpu.CompilerParams(
                collective_id=0, has_side_effects=True, vmem_limit_bytes=67043328),
            name='layer',
        )(x, lens[None, :], ids.T, rw.T, cache.transpose(0, 2, 1).reshape(bsz // 2, 2 * kvd, rows),
          w_q.reshape(2, hid // 2, w_q.shape[1]), w_q.reshape(n_loc, hid // n_loc, w_q.shape[1]), w_dkv.T, w_uk.reshape(2, heads * nope // 2, lat),
          w_uv.reshape(2, 4, 2, lat, vh), w_o.reshape(4, hid // 4, hid),
          s_gate, s_up, s_down.reshape(2, inter, hid), e_gate, e_up, e_down)
        y, kv = pl.pallas_call(
            settle,
            out_shape=(jax.ShapeDtypeStruct(y.shape, bf16), jax.ShapeDtypeStruct(kv.shape, bf16)),
            in_specs=[vm, vm],
            out_specs=(vm, vm),
            name='settle',
        )(y, kv)
        return y, kv.T

    in_specs = (row_spec, cache_spec, tok_spec, row_spec, row_spec) + (P(),) * 8 + (exp_spec,) * 3
    return jax.shard_map(local, mesh=mesh, in_specs=in_specs, out_specs=(row_spec, row_spec), check_vma=False)
```

```python
import jax
import jax.numpy as jnp
from jax import lax
from jax.experimental import pallas as pl
from jax.experimental.pallas import tpu as pltpu
from jax.sharding import PartitionSpec as P

EPS = 1e-6
ROPE_BASE = 1.0e4
CAP = 32
COLS = 256
PER = 4
RING = 3
SLOTS = 6
GROUP = 8
Q_PARTS = 8
FAR, ACROSS, NEAR, OWN = range(4)
LAND = {FAR: 0, NEAR: 1}


def dot(a, b):
    return jnp.dot(a, b, preferred_element_type=jnp.float32)


def dot_t(a, b):
    return lax.dot_general(a, b, (((1,), (1,)), ((), ())), preferred_element_type=jnp.float32)


def layer(x_hbm, pos_ref, ids_ref, rw_ref, cache, wq, wq3, wdkv, wuk, wuv, wo, sg, su, sd, eg, eu, ed,
          y_ref, kv_ref,
          wbuf, dbuf, xall, act, sact, outc, comb, uall, mall, meta, part, r1, r2, ub,
          wsem, dsem, ssem, qsem, asem, us_send, us_recv, ms_send, ms_recv, s1_send, s1_recv, s2_send, s2_recv):
    f32, bf16 = jnp.float32, jnp.bfloat16
    bsz, hid = x_hbm.shape
    kvd, rows = cache.shape[1] // 2, cache.shape[2]
    lat = wuk.shape[2]
    rot = kvd - lat
    vh = wuv.shape[4]
    heads = hid // vh
    nope = hid // heads
    qkd = nope + rot
    steps = bsz // GROUP
    wide = heads * qkd // Q_PARTS
    scale = qkd ** -0.5
    size = heads * GROUP
    n_loc = eg.shape[0]
    inter = eg.shape[2]
    n_col = hid // COLS
    blocks = n_loc // PER
    n_down = n_col * blocks
    half = bsz // 2
    top = ids_ref.shape[0]
    me = lax.axis_index('ep')
    partner = {'ep': me + 1 - 2 * lax.rem(me, 2)}
    across = {'ep': lax.rem(me + 2, 4)}
    q_wide = (lat // 128 + 1) * 128
    piece = hid // 4

    barrier = pltpu.get_barrier_semaphore()
    for dev in (partner, across):
        pl.semaphore_signal(barrier, inc=1, device_id=dev, device_id_type=pl.DeviceIdType.MESH)

    def copy(src, dst, sem):
        return pltpu.make_async_copy(src, dst, sem)

    def c_copy(i):
        slot = lax.rem(i, SLOTS)
        return copy(cache.at[pl.ds(i * (GROUP // 2), GROUP // 2)], dbuf.at[slot, :, pl.ds(0, 2 * kvd), :], dsem.at[slot])

    deep = hid // 2

    def s_copy(w, i, slot):
        return [copy(w.at[pl.ds(k * deep, deep), pl.ds(i * inter, inter)], wbuf.at[2 * slot + k], wsem.at[2 * slot + k])
                for k in range(2)]

    def e_copy(w, e, slot):
        return [copy(w.at[e, pl.ds(k * deep, deep)], wbuf.at[2 * slot + k], wsem.at[2 * slot + k]) for k in range(2)]

    def down_copy(j, slot):
        c = j // blocks
        e = lax.rem(j, blocks)
        return copy(ed.at[pl.ds(PER * e, PER), :, pl.ds(pl.multiple_of(c * COLS, COLS), COLS)], dbuf.at[slot], dsem.at[slot])

    def sdown_copy(c, i, slot):
        at = pl.multiple_of((2 * c + i) * COLS, COLS)
        return copy(sd.at[:, :, pl.ds(at, COLS)], dbuf.at[slot, pl.ds(2 * i, 2)], ssem.at[slot, i])

    def remote(src, dst, send, recv, dev):
        return pltpu.make_async_remote_copy(src_ref=src, dst_ref=dst, send_sem=send, recv_sem=recv,
                                            device_id=dev, device_id_type=pl.DeviceIdType.MESH)

    per_buf = inter // wide
    q_view = []
    for i in range(Q_PARTS):
        if i < 2 * per_buf:
            q_view.append(wbuf.at[pl.ds(2 + 2 * (i // per_buf), 2), :, pl.ds((i % per_buf) * wide, wide)])
        else:
            q_view.append(act.at[:, :, pl.ds(q_wide + (i - 2 * per_buf) * wide, wide)])
    q_copies = [copy((wq if i < 2 * per_buf else wq3).at[..., pl.ds(i * wide, wide)], q_view[i], qsem.at[i])
                for i in range(Q_PARTS)]
    uk_view = [wbuf.at[pl.ds(2 + 2 * i, 2), :, pl.ds(per_buf * wide, lat // 2)] for i in range(2)]
    uk_copies = [copy(wuk.at[:, :, pl.ds(i * (lat // 2), lat // 2)], uk_view[i], asem.at[i]) for i in range(2)]
    uv_copies = [copy(wuv.at[:, :, i], outc.at[:, :, :, pl.ds(i * vh, vh)], asem.at[2 + i]) for i in range(2)]
    dkv_copies = [copy(wdkv.at[pl.ds(0, lat)], xall.at[0], asem.at[4]),
                  copy(wdkv.at[pl.ds(lat, rot)], xall.at[1, pl.ds(0, rot)], asem.at[5])]
    o_copy = copy(wo, xall, asem.at[6])
    x_copy = copy(x_hbm, y_ref, asem.at[7])
    x_copy.start()
    for c in dkv_copies + uk_copies + q_copies[:3]:
        c.start()
    later = q_copies[3:] + [c_copy(i) for i in range(SLOTS)] + uv_copies + [copy(wo.at[0], xall.at[0], asem.at[6])]

    lane = lax.broadcasted_iota(jnp.int32, (bsz, 128), 1)
    low = lane < rot
    front = lax.rem(lane, rot) < rot // 2

    with jax.named_scope('norm'):
        x_copy.wait()
        x = y_ref[...].astype(f32)
        xn = (x * lax.rsqrt(jnp.mean(x * x, axis=-1, keepdims=True) + EPS)).astype(bf16)
        turn_i = lax.broadcasted_iota(jnp.int32, (rot // 2, bsz), 0).astype(f32)
        ang = jnp.exp(turn_i * (-2.0 / rot * 9.210340371976184)) * pos_ref[...].astype(f32)
        cos_t = jnp.cos(ang)
        sin_t = jnp.sin(ang)
        cos = jnp.concatenate([cos_t] * 4, axis=0).T
        sin = jnp.concatenate([-sin_t, sin_t] * 2, axis=0).T
        r2[7, :, :128] = jnp.broadcast_to(pos_ref[...].astype(f32), (bsz, bsz)).T
        meta[...] = jnp.zeros(meta.shape, f32)
        meta[:top, :] = ids_ref[...].astype(f32)
        meta[8:8 + top, :] = rw_ref[...]

    def turn(r):
        swap = jnp.where(front, pltpu.roll(r, 128 - rot // 2, 1), pltpu.roll(r, rot // 2, 1))
        return (r * cos + swap * sin).astype(bf16).astype(f32)

    with jax.named_scope('kv_phase'):
        for c in dkv_copies:
            c.wait()
        c = dot_t(xn, xall[0])
        r = dot_t(xn, xall[1, :rot, :])
        later.pop(0).start()
        c = (c * lax.rsqrt(jnp.mean(c * c, axis=-1, keepdims=True) + EPS)).astype(bf16).astype(f32)
        r = turn(jnp.concatenate([r, jnp.zeros((bsz, 128 - rot), f32)], axis=1))
        r2[4] = c[:, :256]
        r2[5] = c[:, 256:]
        r2[6, :, :128] = r
        kv_ref[:lat, :] = c.T.astype(bf16)
        kv_ref[lat:, :] = r.T[:rot, :].astype(bf16)

    with jax.named_scope('q_phase'):
        for c in uk_copies:
            c.wait()
        def project_q(i):
            q_copies[i].wait()
            later.pop(0).start()
            return dot(xn, q_view[i][...].reshape(hid, wide)).astype(bf16).astype(f32)

        def place(i, q):
            for j in range(wide // (2 * qkd)):
                at = 2 * qkd * j
                h = i * (wide // qkd) + 2 * j
                mid = q[:, at + nope:at + 2 * nope]
                last = q[:, at + 2 * nope:at + 3 * nope]
                n_a = q[:, at:at + nope]
                n_b = jnp.where(low, pltpu.roll(mid, rot, 1), pltpu.roll(last, rot, 1))
                r = turn(jnp.where(low, mid, last))
                other = pltpu.roll(r, rot, 1)
                pair = []
                for k, n, z in ((0, n_a, jnp.where(low, r, other)), (1, n_b, jnp.where(low, other, r))):
                    uk = jnp.concatenate([v[(h + k) * nope // deep, pl.ds((h + k) * nope % deep, nope), :] for v in uk_view], axis=1)
                    ql = jnp.concatenate([dot(n.astype(bf16), uk), z], axis=1)
                    pair.append(ql.reshape(steps, GROUP, q_wide))
                act[:, pl.ds(h * GROUP, 2 * GROUP), :q_wide] = jnp.concatenate(pair, axis=1).astype(bf16)

        q = project_q(0)
        for i in range(Q_PARTS):
            then = project_q(i + 1) if i + 1 < Q_PARTS else None
            place(i, q)
            q = then
        for c in later:
            c.start()

    def ahead_copy(j):
        at = pl.ds(pl.multiple_of(j * piece, piece), piece)
        k = j // 2
        to = pl.ds(pl.multiple_of(lax.rem(j, 2) * piece, piece), piece)
        copy(sg.at[at, pl.ds(0, inter)], wbuf.at[k, to], wsem.at[k]).start()
        copy(su.at[at, pl.ds(0, inter)], wbuf.at[2 + k, to], wsem.at[2 + k]).start()

    row = lax.rem(lax.broadcasted_iota(jnp.int32, (size, 128), 0), GROUP)

    def spread(v, width):
        keep = [jnp.where(row == g, 1.0, 0.0).astype(bf16) for g in range(GROUP)]
        return jnp.concatenate([v[:, t * 128:(t + 1) * 128] * keep[g]
                                for g in range(GROUP) for t in range(width // 128)], axis=1)

    def ahead(i):
        return pl.ds(pl.multiple_of(i * GROUP, GROUP), GROUP)

    def cached(i, g, first, count):
        return dbuf[lax.rem(i, SLOTS), g // 2, (g % 2) * kvd + first:(g % 2) * kvd + first + count, :]

    def scores(i, k):
        at = ahead(i)
        q = act[i, :, :q_wide]
        kv = jnp.concatenate([r2[4, at, :], r2[5, at, :], r2[6, at, :128]], axis=1)
        new = jnp.sum(q.astype(f32).reshape(heads, GROUP, q_wide) * kv[None], axis=2, keepdims=True)
        r2[2, :, k * 128:(k + 1) * 128] = jnp.broadcast_to(new.reshape(size, 1), (size, 128))
        tail = q[:, lat:]
        pairs = [tail * jnp.where(row == 2 * j + lane // rot, 1.0, 0.0).astype(bf16) for j in range(GROUP // 2)]
        c = jnp.concatenate([cached(i, g, 0, lat) for g in range(GROUP)], axis=0)
        r = jnp.concatenate([cached(i, g, lat, rot) for g in range(GROUP)], axis=0)
        r2[k] = dot(spread(q[:, :lat], lat), c) + dot(jnp.concatenate(pairs, axis=1), r)

    def soften(i, k):
        col = lax.broadcasted_iota(jnp.int32, (GROUP, rows), 1).astype(f32)
        live = col < r2[7, ahead(i), :1]
        s_new = r2[2, :, k * 128:k * 128 + 1] * scale
        s = (r2[k] * scale).reshape(heads, GROUP, rows)
        s = jnp.where(live[None], s, -jnp.inf).reshape(size, rows)
        mx = jnp.maximum(jnp.max(s, axis=1, keepdims=True), s_new)
        e = jnp.exp(s - mx)
        e_new = jnp.exp(s_new - mx)
        inv = 1.0 / (jnp.sum(e, axis=1, keepdims=True) + e_new)
        sact[k, :, :rows] = (e * inv).astype(bf16)
        r2[3, :, k * 128:(k + 1) * 128] = jnp.broadcast_to((e_new * inv).astype(bf16).astype(f32), (size, 128))

    def mix(i, k):
        at = ahead(i)
        c = jnp.concatenate([cached(i, g, 0, lat) for g in range(GROUP)], axis=1)
        o = dot_t(spread(sact[k, :, :rows], rows), c)
        p_new = r2[3, :, k * 128:(k + 1) * 128]
        p_new = jnp.concatenate([p_new, p_new], axis=1)
        for t in range(2):
            new = jnp.concatenate([r2[4 + t, at, :]] * heads, axis=0)
            ot = o[:, t * 256:(t + 1) * 256] + p_new * new
            for h in range(heads):
                part[h // 2, 2 * (h % 2) + t, at, :] = ot[h * GROUP:(h + 1) * GROUP, :]

    m_across = remote(meta, mall.at[1], ms_send.at[1], ms_recv.at[1], across)
    u_across = [remote(ub.at[pl.ds(i * half, half)], uall.at[1, pl.ds(i * half, half)],
                       us_send.at[1 + i], us_recv.at[1 + i], across) for i in range(2)]
    m_partner = remote(meta, mall.at[0], ms_send.at[0], ms_recv.at[0], partner)
    u_partner = remote(ub, uall.at[0], us_send.at[0], us_recv.at[0], partner)
    m_relay = remote(mall.at[1], mall.at[2], ms_send.at[2], ms_recv.at[2], partner)
    u_relay = [remote(uall.at[1, pl.ds(i * half, half)], uall.at[2, pl.ds(i * half, half)],
                      us_send.at[3 + i], us_recv.at[3 + i], partner) for i in range(2)]

    def project(i):
        at = slice(i * half, (i + 1) * half)
        if i == 0:
            for c in uv_copies:
                c.wait()
            o_copy.wait()
        for h in range(heads):
            o = jnp.concatenate([part[h // 2, 2 * (h % 2) + t, at, :] for t in range(2)], axis=1).astype(bf16)
            g = h // 2
            ub[at, h * vh:(h + 1) * vh] = dot(o, outc[g // 4, g % 4, :, (h % 2) * vh:(h % 2 + 1) * vh]).astype(bf16)
        a = dot(ub[at, :], xall[...].reshape(hid, hid))
        h1 = (y_ref[at, :].astype(f32) + a).astype(bf16)
        h = h1.astype(f32)
        ub[at, :] = (h * lax.rsqrt(jnp.mean(h * h, axis=-1, keepdims=True) + EPS)).astype(bf16)
        y_ref[at, :] = h1
        if i == 0:
            pl.semaphore_wait(barrier, 2)
            m_across.start()
            m_partner.start()
        u_across[i].start()
        if i == 1:
            u_partner.start()

    with jax.named_scope('attend_loop'):
        for i in range(2):
            c_copy(i).wait()
            scores(i, i)
        soften(0, 0)

        def attend(j, _):
            for k in (1, 0):
                c_copy(2 * j + 3 - k).wait()
            for k in (1, 0):
                i = 2 * j + 2 - k
                mix(i - 1, 1 - k)
                soften(i, k)
                scores(i + 1, 1 - k)

            @pl.when(2 * j + 1 + SLOTS < steps)
            def _():
                for k in range(2):
                    c_copy(2 * j + k + SLOTS).start()

            @pl.when(2 * j + 1 + SLOTS >= steps)
            def _():
                for k in range(2):
                    free = lax.rem(2 * j + k, SLOTS)
                    down_copy(free, free).start()

            @pl.when(j < 3)
            def _():
                copy(wo.at[j + 1], xall.at[j + 1], asem.at[6]).start()

            @pl.when(j >= 3)
            def _():
                ahead_copy(j - 3)

            @pl.when(j == steps // 4 - 1)
            def _():
                project(0)
            return 0

        lax.fori_loop(0, steps // 2 - 1, attend, 0)
        for c in s_copy(sg, 1, 2):
            c.start()
        mix(steps - 2, 0)
        soften(steps - 1, 1)
        mix(steps - 1, 1)
        for k in (2, 1):
            down_copy((steps - k) % SLOTS, (steps - k) % SLOTS).start()

    with jax.named_scope('out_phase'):
        project(1)

    cuts = [(c * 256, min(256, inter - c * 256)) for c in range((inter + 255) // 256)]

    def glu(lhs, dst, g_slot, u_slot, g_copy, u_copy, g_next, u_next):
        def gate(n, at, w):
            return part.at[n // 4, n % 4, :, pl.ds(0, w)]

        g_copy[0].wait()
        g = dot(lhs(0), wbuf[2 * g_slot])
        for n, (at, w) in enumerate(cuts):
            gate(n, at, w)[...] = g[:, at:at + w]
        g_next(0)
        g_copy[1].wait()
        g = dot(lhs(1), wbuf[2 * g_slot + 1])
        for n, (at, w) in enumerate(cuts):
            gate(n, at, w)[...] += g[:, at:at + w]
        g_next(1)
        u_copy[0].wait()
        v = dot(lhs(0), wbuf[2 * u_slot])
        for n, (at, w) in enumerate(cuts):
            part[2 + n // 4, n % 4, :, :w] = v[:, at:at + w]
        u_next(0)
        u_copy[1].wait()
        v = dot(lhs(1), wbuf[2 * u_slot + 1])
        v = v + jnp.concatenate([part[2 + n // 4, n % 4, :, :w] for n, (at, w) in enumerate(cuts)], axis=1)
        g = jnp.concatenate([gate(n, at, w)[...] for n, (at, w) in enumerate(cuts)], axis=1)
        dst[...] = (jax.nn.silu(g) * v).astype(bf16)
        u_next(1)

    with jax.named_scope('shared_up'):
        def mine(k):
            return ub[:, k * deep:(k + 1) * deep]

        glu(mine, sact.at[0], 0, 1, s_copy(sg, 0, 0), s_copy(su, 0, 1),
            lambda k: s_copy(su, 1, 0)[k].start(), lambda k: e_copy(eg, 0, 1)[k].start())
        glu(mine, sact.at[1], 2, 0, s_copy(sg, 1, 2), s_copy(su, 1, 0),
            lambda k: e_copy(eu, 0, 2)[k].start(), lambda k: e_copy(eg, 1, 0)[k].start())

    with jax.named_scope('half_wait'):
        m_across.wait_recv()
        m_relay.start()
        u_across[0].wait_recv()
        u_relay[0].start()

    def dispatch(q, m, u):
        first = (me * n_loc).astype(f32)
        mine = lax.broadcasted_iota(jnp.int32, (n_loc, bsz), 0).astype(f32) + first
        hit = jnp.zeros((n_loc, bsz), f32)
        wgt = jnp.zeros((n_loc, bsz), f32)
        for k in range(top):
            eq = m[k:k + 1, :] == mine
            hit = jnp.where(eq, 1.0, hit)
            wgt = jnp.where(eq, m[8 + k:9 + k, :], wgt)
        r = lax.broadcasted_iota(jnp.int32, (bsz, bsz), 0)
        c = lax.broadcasted_iota(jnp.int32, (bsz, bsz), 1)
        before = jnp.where(r < c, 1.0, 0.0).astype(bf16)
        rank = jnp.where(hit > 0.0, dot(hit.astype(bf16), before), -1.0)
        slot = lax.broadcasted_iota(jnp.int32, (CAP, bsz), 0).astype(f32)
        sel = []
        ct = []
        for e in range(n_loc):
            at = slot == rank[e:e + 1, :]
            sel.append(jnp.where(at, 1.0, 0.0).astype(bf16))
            ct.append(jnp.where(at, wgt[e:e + 1, :], 0.0))
        c0 = jnp.concatenate(ct, axis=0).T
        for i in range(3):
            ci = c0.astype(bf16)
            comb[q, pl.ds(i * bsz, bsz), :] = ci
            c0 = c0 - ci.astype(f32)
        xall[q] = dot(jnp.concatenate(sel, axis=0), u).astype(bf16)

    with jax.named_scope('disp01'):
        dispatch(OWN, meta[...], ub[...])
        m_partner.wait_recv()
        u_partner.wait_recv()
        dispatch(NEAR, mall[0], uall[0])
    with jax.named_scope('gather_wait'):
        u_across[1].wait_recv()
        u_relay[1].start()
    with jax.named_scope('disp2'):
        dispatch(ACROSS, mall[1], uall[1])
    with jax.named_scope('relay_wait'):
        m_relay.wait_recv()
        for i in range(2):
            u_relay[i].wait_recv()
    with jax.named_scope('disp3'):
        dispatch(FAR, mall[2], uall[2])

    def expert(e, _):
        g_slot = lax.rem(4 + 2 * e, RING)
        u_slot = lax.rem(5 + 2 * e, RING)

        def lhs(k):
            at = pl.ds(pl.multiple_of(e * CAP, CAP), CAP)
            return xall[:, at, k * deep:(k + 1) * deep].reshape(4 * CAP, deep)

        def g_next(k):
            @pl.when(e + 1 < n_loc)
            def _():
                e_copy(eu, e + 1, g_slot)[k].start()

        def u_next(k):
            @pl.when(e + 2 < n_loc)
            def _():
                e_copy(eg, e + 2, u_slot)[k].start()

        glu(lhs, act.at[e], g_slot, u_slot, e_copy(eg, e, g_slot), e_copy(eu, e, u_slot), g_next, u_next)
        return 0

    with jax.named_scope('experts'):
        lax.fori_loop(0, n_loc, expert, 0)

    def ring1(c, i):
        return remote(part.at[c, i], r1.at[c, LAND[i]], s1_send.at[c, LAND[i]], s1_recv.at[c, LAND[i]], partner)

    def ring2(c):
        return remote(part.at[c, ACROSS], r2.at[c], s2_send.at[c], s2_recv.at[c], across)

    def fold(c):
        ring1(c, FAR).wait_recv()
        part[c, ACROSS] = part[c, ACROSS] + r1[c, LAND[FAR]]

    def combine(c, q):
        p = dot(comb[q], outc[lax.rem(c, 2), q])
        part[c, q] = p[:bsz] + p[bsz:2 * bsz] + p[2 * bsz:]

    def down_step(c, e, early):
        j = c * blocks + e
        slot = lax.rem(j, SLOTS)
        down_copy(j, slot).wait()
        if early is not None:
            early()
        for i in range(PER):
            res = dot(act[PER * e + i], dbuf[slot, i]).astype(bf16)
            outc[lax.rem(c, 2), :, pl.ds(pl.multiple_of((PER * e + i) * CAP, CAP), CAP), :] = res.reshape(4, CAP, COLS)

        @pl.when(j + SLOTS < n_down)
        def _():
            down_copy(j + SLOTS, slot).start()

        @pl.when((j + SLOTS >= n_down) & (j + SLOTS < n_down + n_col // 2))
        def _():
            for i in range(2):
                sdown_copy(j + SLOTS - n_down, i, slot).start()

    def first(e, _):
        down_step(0, e, None)
        return 0

    def column(c, _):
        def step(e, _):
            @pl.when(e == 1)
            def _():
                ring1(c - 1, FAR).start()

            @pl.when(e == 3)
            def _():
                ring2(c - 1).start()
                ring1(c - 1, NEAR).start()

            down_step(c, e, lambda: combine(c - 1, e))

            @pl.when(e == 2)
            def _():
                fold(c - 1)
            return 0

        lax.fori_loop(0, blocks, step, 0)
        return 0

    with jax.named_scope('column0'):
        lax.fori_loop(0, blocks, first, 0)
    with jax.named_scope('columns'):
        lax.fori_loop(1, n_col, column, 0)

    last = n_col - 1
    with jax.named_scope('combine'):
        combine(last, FAR)
        combine(last, ACROSS)
        ring1(last, FAR).start()
        combine(last, NEAR)
        combine(last, OWN)
        ring1(last, NEAR).start()

    with jax.named_scope('shared_down'):
        for c in range(n_col // 2):
            slot = (n_down + c) % SLOTS
            for i in range(2):
                sdown_copy(c, i, slot).wait()
            for i in range(2):
                part[2 * c + i, OWN] = (part[2 * c + i, OWN] + dot(sact[0], dbuf[slot, 2 * i])
                                        + dot(sact[1], dbuf[slot, 2 * i + 1]))
            if c == 0:
                fold(last)
                ring2(last).start()

    with jax.named_scope('tail'):
        for c in range(n_col):
            ring1(c, NEAR).wait_recv()
            ring2(c).wait_recv()
            at = slice(c * COLS, (c + 1) * COLS)
            y_ref[:, at] = (y_ref[:, at].astype(f32) + ((part[c, OWN] + r1[c, LAND[NEAR]]) + r2[c])).astype(bf16)

    for c in (m_across, *u_across, m_partner, u_partner, m_relay, *u_relay):
        c.wait_send()
    for c in range(n_col):
        ring1(c, FAR).wait_send()
        ring1(c, NEAR).wait_send()
        ring2(c).wait_send()


def settle(y_in, kv_in, y_ref, kv_ref):
    y_ref[...] = y_in[...]
    kv_ref[...] = kv_in[...]


def solution(mesh):
    tok_spec = P(('rep', 'ep'))
    row_spec = P(('rep', 'ep'), None)
    cache_spec = P(('rep', 'ep'), None, None)
    exp_spec = P('ep', None, None)

    def local(x, cache, lens, ids, rw, w_q, w_dkv, w_uk, w_uv, w_o, s_gate, s_up, s_down, e_gate, e_up, e_down):
        bsz, hid = x.shape
        heads, nope, lat = w_uk.shape
        rows, kvd = cache.shape[1:]
        vh = w_uv.shape[2]
        n_loc, _, inter = e_gate.shape
        n_col = hid // COLS
        bf16, f32 = jnp.bfloat16, jnp.float32
        vm = pl.BlockSpec(memory_space=pltpu.VMEM)
        hbm = pl.BlockSpec(memory_space=pl.ANY)
        dma = pltpu.SemaphoreType.DMA
        y, kv = pl.pallas_call(
            layer,
            out_shape=(jax.ShapeDtypeStruct((bsz, hid), bf16), jax.ShapeDtypeStruct((kvd, bsz), bf16)),
            in_specs=[hbm] + [vm] * 3 + [hbm] * 13,
            out_specs=(vm, vm),
            scratch_shapes=[
                pltpu.VMEM((2 * RING, hid // 2, inter), bf16),
                pltpu.VMEM((SLOTS, PER, inter, COLS), bf16),
                pltpu.VMEM((4, n_loc * CAP, hid), bf16),
                pltpu.VMEM((n_loc, 4 * CAP, inter), bf16),
                pltpu.VMEM((2, bsz, inter), bf16),
                pltpu.VMEM((2, 4, n_loc * CAP, COLS), bf16),
                pltpu.VMEM((4, 3 * bsz, n_loc * CAP), bf16),
                pltpu.VMEM((3, bsz, hid), bf16),
                pltpu.VMEM((3, 16, bsz), f32),
                pltpu.VMEM((16, bsz), f32),
                pltpu.VMEM((n_col, 4, bsz, COLS), f32),
                pltpu.VMEM((n_col, 2, bsz, COLS), f32),
                pltpu.VMEM((n_col, bsz, COLS), f32),
                pltpu.VMEM((bsz, hid), bf16),
                dma((2 * RING,)), dma((SLOTS,)), dma((SLOTS, 2)), dma((Q_PARTS,)), dma((8,)),
                dma((5,)), dma((5,)), dma((3,)), dma((3,)),
                dma((n_col, 2)), dma((n_col, 2)), dma((n_col,)), dma((n_col,)),
            ],
            compiler_params=pltpu.CompilerParams(
                collective_id=0, has_side_effects=True, vmem_limit_bytes=67043328),
            name='layer',
        )(x, lens[None, :], ids.T, rw.T, cache.transpose(0, 2, 1).reshape(bsz // 2, 2 * kvd, rows),
          w_q.reshape(2, hid // 2, w_q.shape[1]), w_q.reshape(n_loc, hid // n_loc, w_q.shape[1]), w_dkv.T, w_uk.reshape(2, heads * nope // 2, lat),
          w_uv.reshape(2, 4, 2, lat, vh), w_o.reshape(4, hid // 4, hid),
          s_gate, s_up, s_down.reshape(2, inter, hid), e_gate, e_up, e_down)
        y, kv = pl.pallas_call(
            settle,
            out_shape=(jax.ShapeDtypeStruct(y.shape, bf16), jax.ShapeDtypeStruct(kv.shape, bf16)),
            in_specs=[vm, vm],
            out_specs=(vm, vm),
            name='settle',
        )(y, kv)
        return y, kv.T

    in_specs = (row_spec, cache_spec, tok_spec, row_spec, row_spec) + (P(),) * 8 + (exp_spec,) * 3
    return jax.shard_map(local, mesh=mesh, in_specs=in_specs, out_specs=(row_spec, row_spec), check_vma=False)
```

```python
import jax
import jax.numpy as jnp
from jax import lax
from jax.experimental import pallas as pl
from jax.experimental.pallas import tpu as pltpu
from jax.sharding import PartitionSpec as P

EPS = 1e-6
ROPE_BASE = 1.0e4
CAP = 32
COLS = 256
LANES = 128
COL, ROW = range(2)
PER = 4
RING = 3
SLOTS = 6
GROUP = 8
Q_PARTS = 8
FAR, ACROSS, NEAR, OWN = range(4)
LAND = {FAR: 0, NEAR: 1}


def dot(a, b):
    return jnp.dot(a, b, preferred_element_type=jnp.float32)


def dot_t(a, b):
    return lax.dot_general(a, b, (((1,), (1,)), ((), ())), preferred_element_type=jnp.float32)


def layer(x_hbm, pos_ref, ids_ref, rw_ref, cache, wq, wq3, wdkv, wuk, wuv, wo, sg, su, sd, eg, eu, ed,
          y_ref, kv_ref,
          wbuf, dbuf, xall, act, sact, outc, comb, uall, mall, meta, part, r1, r2, ub,
          wsem, dsem, ssem, qsem, asem, us_send, us_recv, ms_send, ms_recv, s1_send, s1_recv, s2_send, s2_recv):
    f32, bf16 = jnp.float32, jnp.bfloat16
    bsz, hid = x_hbm.shape
    kvd, rows = cache.shape[1] // 2, cache.shape[2]
    lat = wuk.shape[2]
    rot = kvd - lat
    vh = wuv.shape[4]
    heads = hid // vh
    nope = hid // heads
    qkd = nope + rot
    steps = bsz // GROUP
    wide = heads * qkd // Q_PARTS
    scale = qkd ** -0.5
    size = heads * GROUP
    n_loc = eg.shape[0]
    inter = eg.shape[2]
    n_col = hid // COLS
    blocks = n_loc // PER
    n_down = n_col * blocks
    half = bsz // 2
    top = ids_ref.shape[0]
    me = lax.axis_index('ep')
    partner = {'ep': me + 1 - 2 * lax.rem(me, 2)}
    across = {'ep': lax.rem(me + 2, 4)}
    q_wide = (lat // LANES + 1) * LANES
    piece = hid // 4

    barrier = pltpu.get_barrier_semaphore()
    for dev in (partner, across):
        pl.semaphore_signal(barrier, inc=1, device_id=dev, device_id_type=pl.DeviceIdType.MESH)

    def copy(src, dst, sem):
        return pltpu.make_async_copy(src, dst, sem)

    def c_copy(i):
        slot = lax.rem(i, SLOTS)
        return copy(cache.at[pl.ds(i * (GROUP // 2), GROUP // 2)], dbuf.at[slot, :, pl.ds(0, 2 * kvd), :], dsem.at[slot])

    deep = hid // 2

    def s_copy(w, i, slot):
        return [copy(w.at[pl.ds(k * deep, deep), pl.ds(i * inter, inter)], wbuf.at[2 * slot + k], wsem.at[2 * slot + k])
                for k in range(2)]

    def e_copy(w, e, slot):
        return [copy(w.at[e, pl.ds(k * deep, deep)], wbuf.at[2 * slot + k], wsem.at[2 * slot + k]) for k in range(2)]

    def down_copy(j, slot):
        c = j // blocks
        e = lax.rem(j, blocks)
        return copy(ed.at[pl.ds(PER * e, PER), :, pl.ds(pl.multiple_of(c * COLS, COLS), COLS)], dbuf.at[slot], dsem.at[slot])

    def sdown_copy(c, i, slot):
        at = pl.multiple_of((2 * c + i) * COLS, COLS)
        return copy(sd.at[:, :, pl.ds(at, COLS)], dbuf.at[slot, pl.ds(2 * i, 2)], ssem.at[slot, i])

    def remote(src, dst, send, recv, dev):
        return pltpu.make_async_remote_copy(src_ref=src, dst_ref=dst, send_sem=send, recv_sem=recv,
                                            device_id=dev, device_id_type=pl.DeviceIdType.MESH)

    per_buf = inter // wide
    q_view = []
    for i in range(Q_PARTS):
        if i < 2 * per_buf:
            q_view.append(wbuf.at[pl.ds(2 + 2 * (i // per_buf), 2), :, pl.ds((i % per_buf) * wide, wide)])
        else:
            q_view.append(act.at[:, :, pl.ds(q_wide + (i - 2 * per_buf) * wide, wide)])
    q_copies = [copy((wq if i < 2 * per_buf else wq3).at[..., pl.ds(i * wide, wide)], q_view[i], qsem.at[i])
                for i in range(Q_PARTS)]
    uk_view = [wbuf.at[pl.ds(2 + 2 * i, 2), :, pl.ds(per_buf * wide, lat // 2)] for i in range(2)]
    uk_copies = [copy(wuk.at[:, :, pl.ds(i * (lat // 2), lat // 2)], uk_view[i], asem.at[i]) for i in range(2)]
    uv_copies = [copy(wuv.at[:, :, i], outc.at[:, :, :, pl.ds(i * vh, vh)], asem.at[2 + i]) for i in range(2)]
    dkv_copies = [copy(wdkv.at[pl.ds(0, lat)], xall.at[0], asem.at[4]),
                  copy(wdkv.at[pl.ds(lat, rot)], xall.at[1, pl.ds(0, rot)], asem.at[5])]
    o_copy = copy(wo, xall, asem.at[6])
    x_copy = copy(x_hbm, y_ref, asem.at[7])
    x_copy.start()
    for c in dkv_copies + uk_copies + q_copies[:3]:
        c.start()
    later = q_copies[3:] + [c_copy(i) for i in range(SLOTS)] + uv_copies + [copy(wo.at[0], xall.at[0], asem.at[6])]

    lane = lax.broadcasted_iota(jnp.int32, (bsz, LANES), 1)
    low = lane < rot
    front = lax.rem(lane, rot) < rot // 2

    with jax.named_scope('norm'):
        x_copy.wait()
        x = y_ref[...].astype(f32)
        xn = (x * lax.rsqrt(jnp.mean(x * x, axis=-1, keepdims=True) + EPS)).astype(bf16)
        turn_i = lax.broadcasted_iota(jnp.int32, (rot // 2, bsz), 0).astype(f32)
        ang = jnp.exp(turn_i * (-2.0 / rot * 9.210340371976184)) * pos_ref[...].astype(f32)
        cos_t = jnp.cos(ang)
        sin_t = jnp.sin(ang)
        cos = jnp.concatenate([cos_t] * 4, axis=COL).T
        sin = jnp.concatenate([-sin_t, sin_t] * 2, axis=COL).T
        r2[7, :, :LANES] = jnp.broadcast_to(pos_ref[...].astype(f32), (bsz, bsz)).T
        meta[...] = jnp.zeros(meta.shape, f32)
        meta[:top, :] = ids_ref[...].astype(f32)
        meta[8:8 + top, :] = rw_ref[...]

    def turn(r):
        swap = jnp.where(front, pltpu.roll(r, LANES - rot // 2, 1), pltpu.roll(r, rot // 2, 1))
        return (r * cos + swap * sin).astype(bf16).astype(f32)

    with jax.named_scope('kv_phase'):
        for c in dkv_copies:
            c.wait()
        c = dot_t(xn, xall[0])
        r = dot_t(xn, xall[1, :rot, :])
        later.pop(0).start()
        c = (c * lax.rsqrt(jnp.mean(c * c, axis=-1, keepdims=True) + EPS)).astype(bf16).astype(f32)
        r = turn(jnp.concatenate([r, jnp.zeros((bsz, LANES - rot), f32)], axis=ROW))
        r2[4] = c[:, :COLS]
        r2[5] = c[:, COLS:]
        r2[6, :, :LANES] = r
        kv_ref[:lat, :] = c.T.astype(bf16)
        kv_ref[lat:, :] = r.T[:rot, :].astype(bf16)

    with jax.named_scope('q_phase'):
        for c in uk_copies:
            c.wait()
        def project_q(i):
            q_copies[i].wait()
            later.pop(0).start()
            return dot(xn, q_view[i][...].reshape(hid, wide)).astype(bf16).astype(f32)

        def place(i, q):
            for j in range(wide // (2 * qkd)):
                at = 2 * qkd * j
                h = i * (wide // qkd) + 2 * j
                mid = q[:, at + nope:at + 2 * nope]
                last = q[:, at + 2 * nope:at + 3 * nope]
                n_a = q[:, at:at + nope]
                n_b = jnp.where(low, pltpu.roll(mid, rot, 1), pltpu.roll(last, rot, 1))
                r = turn(jnp.where(low, mid, last))
                other = pltpu.roll(r, rot, 1)
                pair = []
                for k, n, z in ((0, n_a, jnp.where(low, r, other)), (1, n_b, jnp.where(low, other, r))):
                    uk = jnp.concatenate([v[(h + k) * nope // deep, pl.ds((h + k) * nope % deep, nope), :] for v in uk_view], axis=ROW)
                    ql = jnp.concatenate([dot(n.astype(bf16), uk), z], axis=ROW)
                    pair.append(ql.reshape(steps, GROUP, q_wide))
                act[:, pl.ds(h * GROUP, 2 * GROUP), :q_wide] = jnp.concatenate(pair, axis=ROW).astype(bf16)

        q = project_q(0)
        for i in range(Q_PARTS):
            then = project_q(i + 1) if i + 1 < Q_PARTS else None
            place(i, q)
            q = then
        for c in later:
            c.start()

    def ahead_copy(j):
        at = pl.ds(pl.multiple_of(j * piece, piece), piece)
        k = j // 2
        to = pl.ds(pl.multiple_of(lax.rem(j, 2) * piece, piece), piece)
        copy(sg.at[at, pl.ds(0, inter)], wbuf.at[k, to], wsem.at[k]).start()
        copy(su.at[at, pl.ds(0, inter)], wbuf.at[2 + k, to], wsem.at[2 + k]).start()

    row = lax.rem(lax.broadcasted_iota(jnp.int32, (size, LANES), 0), GROUP)

    def spread(v, width):
        keep = [jnp.where(row == g, 1.0, 0.0).astype(bf16) for g in range(GROUP)]
        return jnp.concatenate([v[:, t * LANES:(t + 1) * LANES] * keep[g]
                                for g in range(GROUP) for t in range(width // LANES)], axis=ROW)

    def ahead(i):
        return pl.ds(pl.multiple_of(i * GROUP, GROUP), GROUP)

    def cached(i, g, first, count):
        return dbuf[lax.rem(i, SLOTS), g // 2, (g % 2) * kvd + first:(g % 2) * kvd + first + count, :]

    def scores(i, k):
        at = ahead(i)
        q = act[i, :, :q_wide]
        kv = jnp.concatenate([r2[4, at, :], r2[5, at, :], r2[6, at, :LANES]], axis=ROW)
        new = jnp.sum(q.astype(f32).reshape(heads, GROUP, q_wide) * kv[None], axis=2, keepdims=True)
        r2[2, :, k * LANES:(k + 1) * LANES] = jnp.broadcast_to(new.reshape(size, 1), (size, LANES))
        tail = q[:, lat:]
        pairs = [tail * jnp.where(row == 2 * j + lane // rot, 1.0, 0.0).astype(bf16) for j in range(GROUP // 2)]
        c = jnp.concatenate([cached(i, g, 0, lat) for g in range(GROUP)], axis=COL)
        r = jnp.concatenate([cached(i, g, lat, rot) for g in range(GROUP)], axis=COL)
        r2[k] = dot(spread(q[:, :lat], lat), c) + dot(jnp.concatenate(pairs, axis=ROW), r)

    def soften(i, k):
        col = lax.broadcasted_iota(jnp.int32, (GROUP, rows), 1).astype(f32)
        live = col < r2[7, ahead(i), :1]
        s_new = r2[2, :, k * LANES:k * LANES + 1] * scale
        s = (r2[k] * scale).reshape(heads, GROUP, rows)
        s = jnp.where(live[None], s, -jnp.inf).reshape(size, rows)
        mx = jnp.maximum(jnp.max(s, axis=ROW, keepdims=True), s_new)
        e = jnp.exp(s - mx)
        e_new = jnp.exp(s_new - mx)
        inv = 1.0 / (jnp.sum(e, axis=ROW, keepdims=True) + e_new)
        sact[k, :, :rows] = (e * inv).astype(bf16)
        r2[3, :, k * LANES:(k + 1) * LANES] = jnp.broadcast_to((e_new * inv).astype(bf16).astype(f32), (size, LANES))

    def mix(i, k):
        at = ahead(i)
        c = jnp.concatenate([cached(i, g, 0, lat) for g in range(GROUP)], axis=ROW)
        o = dot_t(spread(sact[k, :, :rows], rows), c)
        p_new = r2[3, :, k * LANES:(k + 1) * LANES]
        p_new = jnp.concatenate([p_new, p_new], axis=ROW)
        for t in range(2):
            new = jnp.concatenate([r2[4 + t, at, :]] * heads, axis=COL)
            ot = o[:, t * COLS:(t + 1) * COLS] + p_new * new
            for h in range(heads):
                part[h // 2, 2 * (h % 2) + t, at, :] = ot[h * GROUP:(h + 1) * GROUP, :]

    m_across = remote(meta, mall.at[1], ms_send.at[1], ms_recv.at[1], across)
    u_across = [remote(ub.at[pl.ds(i * half, half)], uall.at[1, pl.ds(i * half, half)],
                       us_send.at[1 + i], us_recv.at[1 + i], across) for i in range(2)]
    m_partner = remote(meta, mall.at[0], ms_send.at[0], ms_recv.at[0], partner)
    u_partner = remote(ub, uall.at[0], us_send.at[0], us_recv.at[0], partner)
    m_relay = remote(mall.at[1], mall.at[2], ms_send.at[2], ms_recv.at[2], partner)
    u_relay = [remote(uall.at[1, pl.ds(i * half, half)], uall.at[2, pl.ds(i * half, half)],
                      us_send.at[3 + i], us_recv.at[3 + i], partner) for i in range(2)]

    def project(i):
        at = slice(i * half, (i + 1) * half)
        if i == 0:
            for c in uv_copies:
                c.wait()
            o_copy.wait()
        for h in range(heads):
            o = jnp.concatenate([part[h // 2, 2 * (h % 2) + t, at, :] for t in range(2)], axis=ROW).astype(bf16)
            g = h // 2
            ub[at, h * vh:(h + 1) * vh] = dot(o, outc[g // 4, g % 4, :, (h % 2) * vh:(h % 2 + 1) * vh]).astype(bf16)
        a = dot(ub[at, :], xall[...].reshape(hid, hid))
        h1 = (y_ref[at, :].astype(f32) + a).astype(bf16)
        h = h1.astype(f32)
        ub[at, :] = (h * lax.rsqrt(jnp.mean(h * h, axis=-1, keepdims=True) + EPS)).astype(bf16)
        y_ref[at, :] = h1
        if i == 0:
            pl.semaphore_wait(barrier, 2)
            m_across.start()
            m_partner.start()
        u_across[i].start()
        if i == 1:
            u_partner.start()

    with jax.named_scope('attend_loop'):
        for i in range(2):
            c_copy(i).wait()
            scores(i, i)
        soften(0, 0)

        def attend(j, _):
            for k in (1, 0):
                c_copy(2 * j + 3 - k).wait()
            for k in (1, 0):
                i = 2 * j + 2 - k
                mix(i - 1, 1 - k)
                soften(i, k)
                scores(i + 1, 1 - k)

            @pl.when(2 * j + 1 + SLOTS < steps)
            def _():
                for k in range(2):
                    c_copy(2 * j + k + SLOTS).start()

            @pl.when(2 * j + 1 + SLOTS >= steps)
            def _():
                for k in range(2):
                    free = lax.rem(2 * j + k, SLOTS)
                    down_copy(free, free).start()

            @pl.when(j < 3)
            def _():
                copy(wo.at[j + 1], xall.at[j + 1], asem.at[6]).start()

            @pl.when(j >= 3)
            def _():
                ahead_copy(j - 3)

            @pl.when(j == steps // 4 - 1)
            def _():
                project(0)
            return 0

        lax.fori_loop(0, steps // 2 - 1, attend, 0)
        for c in s_copy(sg, 1, 2):
            c.start()
        mix(steps - 2, 0)
        soften(steps - 1, 1)
        mix(steps - 1, 1)
        for k in (2, 1):
            down_copy((steps - k) % SLOTS, (steps - k) % SLOTS).start()

    with jax.named_scope('out_phase'):
        project(1)

    cuts = [(c * COLS, min(COLS, inter - c * COLS)) for c in range((inter + 255) // COLS)]

    def glu(lhs, dst, g_slot, u_slot, g_copy, u_copy, g_next, u_next):
        def gate(n, at, w):
            return part.at[n // 4, n % 4, :, pl.ds(0, w)]

        g_copy[0].wait()
        g = dot(lhs(0), wbuf[2 * g_slot])
        for n, (at, w) in enumerate(cuts):
            gate(n, at, w)[...] = g[:, at:at + w]
        g_next(0)
        g_copy[1].wait()
        g = dot(lhs(1), wbuf[2 * g_slot + 1])
        for n, (at, w) in enumerate(cuts):
            gate(n, at, w)[...] += g[:, at:at + w]
        g_next(1)
        u_copy[0].wait()
        v = dot(lhs(0), wbuf[2 * u_slot])
        for n, (at, w) in enumerate(cuts):
            part[2 + n // 4, n % 4, :, :w] = v[:, at:at + w]
        u_next(0)
        u_copy[1].wait()
        v = dot(lhs(1), wbuf[2 * u_slot + 1])
        v = v + jnp.concatenate([part[2 + n // 4, n % 4, :, :w] for n, (at, w) in enumerate(cuts)], axis=ROW)
        g = jnp.concatenate([gate(n, at, w)[...] for n, (at, w) in enumerate(cuts)], axis=ROW)
        dst[...] = (jax.nn.silu(g) * v).astype(bf16)
        u_next(1)

    with jax.named_scope('shared_up'):
        def mine(k):
            return ub[:, k * deep:(k + 1) * deep]

        glu(mine, sact.at[0], 0, 1, s_copy(sg, 0, 0), s_copy(su, 0, 1),
            lambda k: s_copy(su, 1, 0)[k].start(), lambda k: e_copy(eg, 0, 1)[k].start())
        glu(mine, sact.at[1], 2, 0, s_copy(sg, 1, 2), s_copy(su, 1, 0),
            lambda k: e_copy(eu, 0, 2)[k].start(), lambda k: e_copy(eg, 1, 0)[k].start())

    with jax.named_scope('half_wait'):
        m_across.wait_recv()
        m_relay.start()
        u_across[0].wait_recv()
        u_relay[0].start()

    def dispatch(q, m, u):
        first = (me * n_loc).astype(f32)
        mine = lax.broadcasted_iota(jnp.int32, (n_loc, bsz), 0).astype(f32) + first
        hit = jnp.zeros((n_loc, bsz), f32)
        wgt = jnp.zeros((n_loc, bsz), f32)
        for k in range(top):
            eq = m[k:k + 1, :] == mine
            hit = jnp.where(eq, 1.0, hit)
            wgt = jnp.where(eq, m[8 + k:9 + k, :], wgt)
        r = lax.broadcasted_iota(jnp.int32, (bsz, bsz), 0)
        c = lax.broadcasted_iota(jnp.int32, (bsz, bsz), 1)
        before = jnp.where(r < c, 1.0, 0.0).astype(bf16)
        rank = jnp.where(hit > 0.0, dot(hit.astype(bf16), before), -1.0)
        slot = lax.broadcasted_iota(jnp.int32, (CAP, bsz), 0).astype(f32)
        sel = []
        ct = []
        for e in range(n_loc):
            at = slot == rank[e:e + 1, :]
            sel.append(jnp.where(at, 1.0, 0.0).astype(bf16))
            ct.append(jnp.where(at, wgt[e:e + 1, :], 0.0))
        c0 = jnp.concatenate(ct, axis=COL).T
        for i in range(3):
            ci = c0.astype(bf16)
            comb[q, pl.ds(i * bsz, bsz), :] = ci
            c0 = c0 - ci.astype(f32)
        xall[q] = dot(jnp.concatenate(sel, axis=COL), u).astype(bf16)

    with jax.named_scope('disp01'):
        dispatch(OWN, meta[...], ub[...])
        m_partner.wait_recv()
        u_partner.wait_recv()
        dispatch(NEAR, mall[0], uall[0])
    with jax.named_scope('gather_wait'):
        u_across[1].wait_recv()
        u_relay[1].start()
    with jax.named_scope('disp2'):
        dispatch(ACROSS, mall[1], uall[1])
    with jax.named_scope('relay_wait'):
        m_relay.wait_recv()
        for i in range(2):
            u_relay[i].wait_recv()
    with jax.named_scope('disp3'):
        dispatch(FAR, mall[2], uall[2])

    def expert(e, _):
        g_slot = lax.rem(4 + 2 * e, RING)
        u_slot = lax.rem(5 + 2 * e, RING)

        def lhs(k):
            at = pl.ds(pl.multiple_of(e * CAP, CAP), CAP)
            return xall[:, at, k * deep:(k + 1) * deep].reshape(4 * CAP, deep)

        def g_next(k):
            @pl.when(e + 1 < n_loc)
            def _():
                e_copy(eu, e + 1, g_slot)[k].start()

        def u_next(k):
            @pl.when(e + 2 < n_loc)
            def _():
                e_copy(eg, e + 2, u_slot)[k].start()

        glu(lhs, act.at[e], g_slot, u_slot, e_copy(eg, e, g_slot), e_copy(eu, e, u_slot), g_next, u_next)
        return 0

    with jax.named_scope('experts'):
        lax.fori_loop(0, n_loc, expert, 0)

    def ring1(c, i):
        return remote(part.at[c, i], r1.at[c, LAND[i]], s1_send.at[c, LAND[i]], s1_recv.at[c, LAND[i]], partner)

    def ring2(c):
        return remote(part.at[c, ACROSS], r2.at[c], s2_send.at[c], s2_recv.at[c], across)

    def fold(c):
        ring1(c, FAR).wait_recv()
        part[c, ACROSS] = part[c, ACROSS] + r1[c, LAND[FAR]]

    def combine(c, q):
        p = dot(comb[q], outc[lax.rem(c, 2), q])
        part[c, q] = p[:bsz] + p[bsz:2 * bsz] + p[2 * bsz:]

    def down_step(c, e, early):
        j = c * blocks + e
        slot = lax.rem(j, SLOTS)
        down_copy(j, slot).wait()
        if early is not None:
            early()
        for i in range(PER):
            res = dot(act[PER * e + i], dbuf[slot, i]).astype(bf16)
            outc[lax.rem(c, 2), :, pl.ds(pl.multiple_of((PER * e + i) * CAP, CAP), CAP), :] = res.reshape(4, CAP, COLS)

        @pl.when(j + SLOTS < n_down)
        def _():
            down_copy(j + SLOTS, slot).start()

        @pl.when((j + SLOTS >= n_down) & (j + SLOTS < n_down + n_col // 2))
        def _():
            for i in range(2):
                sdown_copy(j + SLOTS - n_down, i, slot).start()

    def first(e, _):
        down_step(0, e, None)
        return 0

    def column(c, _):
        def step(e, _):
            @pl.when(e == 1)
            def _():
                ring1(c - 1, FAR).start()

            @pl.when(e == 3)
            def _():
                ring2(c - 1).start()
                ring1(c - 1, NEAR).start()

            down_step(c, e, lambda: combine(c - 1, e))

            @pl.when(e == 2)
            def _():
                fold(c - 1)
            return 0

        lax.fori_loop(0, blocks, step, 0)
        return 0

    with jax.named_scope('column0'):
        lax.fori_loop(0, blocks, first, 0)
    with jax.named_scope('columns'):
        lax.fori_loop(1, n_col, column, 0)

    last = n_col - 1
    with jax.named_scope('combine'):
        combine(last, FAR)
        combine(last, ACROSS)
        ring1(last, FAR).start()
        combine(last, NEAR)
        combine(last, OWN)
        ring1(last, NEAR).start()

    with jax.named_scope('shared_down'):
        for c in range(n_col // 2):
            slot = (n_down + c) % SLOTS
            for i in range(2):
                sdown_copy(c, i, slot).wait()
            for i in range(2):
                part[2 * c + i, OWN] = (part[2 * c + i, OWN] + dot(sact[0], dbuf[slot, 2 * i])
                                        + dot(sact[1], dbuf[slot, 2 * i + 1]))
            if c == 0:
                fold(last)
                ring2(last).start()

    with jax.named_scope('tail'):
        for c in range(n_col):
            ring1(c, NEAR).wait_recv()
            ring2(c).wait_recv()
            at = slice(c * COLS, (c + 1) * COLS)
            y_ref[:, at] = (y_ref[:, at].astype(f32) + ((part[c, OWN] + r1[c, LAND[NEAR]]) + r2[c])).astype(bf16)

    for c in (m_across, *u_across, m_partner, u_partner, m_relay, *u_relay):
        c.wait_send()
    for c in range(n_col):
        ring1(c, FAR).wait_send()
        ring1(c, NEAR).wait_send()
        ring2(c).wait_send()


def settle(y_in, kv_in, y_ref, kv_ref):
    y_ref[...] = y_in[...]
    kv_ref[...] = kv_in[...]


def solution(mesh):
    tok_spec = P(('rep', 'ep'))
    row_spec = P(('rep', 'ep'), None)
    cache_spec = P(('rep', 'ep'), None, None)
    exp_spec = P('ep', None, None)

    def local(x, cache, lens, ids, rw, w_q, w_dkv, w_uk, w_uv, w_o, s_gate, s_up, s_down, e_gate, e_up, e_down):
        bsz, hid = x.shape
        heads, nope, lat = w_uk.shape
        rows, kvd = cache.shape[1:]
        vh = w_uv.shape[2]
        n_loc, _, inter = e_gate.shape
        n_col = hid // COLS
        bf16, f32 = jnp.bfloat16, jnp.float32
        vm = pl.BlockSpec(memory_space=pltpu.VMEM)
        hbm = pl.BlockSpec(memory_space=pl.ANY)
        dma = pltpu.SemaphoreType.DMA
        y, kv = pl.pallas_call(
            layer,
            out_shape=(jax.ShapeDtypeStruct((bsz, hid), bf16), jax.ShapeDtypeStruct((kvd, bsz), bf16)),
            in_specs=[hbm] + [vm] * 3 + [hbm] * 13,
            out_specs=(vm, vm),
            scratch_shapes=[
                pltpu.VMEM((2 * RING, hid // 2, inter), bf16),
                pltpu.VMEM((SLOTS, PER, inter, COLS), bf16),
                pltpu.VMEM((4, n_loc * CAP, hid), bf16),
                pltpu.VMEM((n_loc, 4 * CAP, inter), bf16),
                pltpu.VMEM((2, bsz, inter), bf16),
                pltpu.VMEM((2, 4, n_loc * CAP, COLS), bf16),
                pltpu.VMEM((4, 3 * bsz, n_loc * CAP), bf16),
                pltpu.VMEM((3, bsz, hid), bf16),
                pltpu.VMEM((3, 16, bsz), f32),
                pltpu.VMEM((16, bsz), f32),
                pltpu.VMEM((n_col, 4, bsz, COLS), f32),
                pltpu.VMEM((n_col, 2, bsz, COLS), f32),
                pltpu.VMEM((n_col, bsz, COLS), f32),
                pltpu.VMEM((bsz, hid), bf16),
                dma((2 * RING,)), dma((SLOTS,)), dma((SLOTS, 2)), dma((Q_PARTS,)), dma((8,)),
                dma((5,)), dma((5,)), dma((3,)), dma((3,)),
                dma((n_col, 2)), dma((n_col, 2)), dma((n_col,)), dma((n_col,)),
            ],
            compiler_params=pltpu.CompilerParams(
                collective_id=0, has_side_effects=True, vmem_limit_bytes=67043328),
            name='layer',
        )(x, lens[None, :], ids.T, rw.T, cache.transpose(0, 2, 1).reshape(bsz // 2, 2 * kvd, rows),
          w_q.reshape(2, hid // 2, w_q.shape[1]), w_q.reshape(n_loc, hid // n_loc, w_q.shape[1]), w_dkv.T, w_uk.reshape(2, heads * nope // 2, lat),
          w_uv.reshape(2, 4, 2, lat, vh), w_o.reshape(4, hid // 4, hid),
          s_gate, s_up, s_down.reshape(2, inter, hid), e_gate, e_up, e_down)
        y, kv = pl.pallas_call(
            settle,
            out_shape=(jax.ShapeDtypeStruct(y.shape, bf16), jax.ShapeDtypeStruct(kv.shape, bf16)),
            in_specs=[vm, vm],
            out_specs=(vm, vm),
            name='settle',
        )(y, kv)
        return y, kv.T

    in_specs = (row_spec, cache_spec, tok_spec, row_spec, row_spec) + (P(),) * 8 + (exp_spec,) * 3
    return jax.shard_map(local, mesh=mesh, in_specs=in_specs, out_specs=(row_spec, row_spec), check_vma=False)
```

```python
import jax
import jax.numpy as jnp
from jax import lax
from jax.experimental import pallas as pl
from jax.experimental.pallas import tpu as pltpu
from jax.sharding import PartitionSpec as P

EPS = 1e-6
ROPE_BASE = 1.0e4
CAP = 32
COLS = 256
LANES = 128
COL, ROW = range(2)
PER = 4
RING = 3
SLOTS = 6
GROUP = 8
Q_PARTS = 8
FAR, ACROSS, NEAR, OWN = range(4)
LAND = {FAR: 0, NEAR: 1}


def dot(a, b):
    return jnp.dot(a, b, preferred_element_type=jnp.float32)


def dot_t(a, b):
    return lax.dot_general(a, b, (((1,), (1,)), ((), ())), preferred_element_type=jnp.float32)


def layer(x_hbm, pos_ref, ids_ref, rw_ref, cache, wq, wq3, wdkv, wuk, wuv, wo, sg, su, sd, eg, eu, ed,
          y_ref, kv_ref,
          wbuf, dbuf, xall, act, sact, outc, comb, uall, mall, meta, part, r1, r2, ub,
          wsem, dsem, ssem, qsem, asem, us_send, us_recv, ms_send, ms_recv, s1_send, s1_recv, s2_send, s2_recv):
    f32, bf16 = jnp.float32, jnp.bfloat16
    bsz, hid = x_hbm.shape
    kvd, rows = cache.shape[1] // 2, cache.shape[2]
    lat = wuk.shape[2]
    rot = kvd - lat
    vh = wuv.shape[4]
    heads = hid // vh
    nope = hid // heads
    qkd = nope + rot
    steps = bsz // GROUP
    wide = heads * qkd // Q_PARTS
    scale = qkd ** -0.5
    size = heads * GROUP
    n_loc = eg.shape[0]
    inter = eg.shape[2]
    n_col = hid // COLS
    blocks = n_loc // PER
    n_down = n_col * blocks
    half = bsz // 2
    top = ids_ref.shape[0]
    me = lax.axis_index('ep')
    partner = {'ep': me + 1 - 2 * lax.rem(me, 2)}
    across = {'ep': lax.rem(me + 2, 4)}
    q_wide = (lat // LANES + 1) * LANES
    piece = hid // 4

    barrier = pltpu.get_barrier_semaphore()
    for dev in (partner, across):
        pl.semaphore_signal(barrier, inc=1, device_id=dev, device_id_type=pl.DeviceIdType.MESH)

    def copy(src, dst, sem):
        return pltpu.make_async_copy(src, dst, sem)

    def c_copy(i):
        slot = lax.rem(i, SLOTS)
        return copy(cache.at[pl.ds(i * (GROUP // 2), GROUP // 2)], dbuf.at[slot, :, pl.ds(0, 2 * kvd), :], dsem.at[slot])

    deep = hid // 2

    def s_copy(w, i, slot):
        return [copy(w.at[pl.ds(k * deep, deep), pl.ds(i * inter, inter)], wbuf.at[2 * slot + k], wsem.at[2 * slot + k])
                for k in range(2)]

    def e_copy(w, e, slot):
        return [copy(w.at[e, pl.ds(k * deep, deep)], wbuf.at[2 * slot + k], wsem.at[2 * slot + k]) for k in range(2)]

    def down_copy(j, slot):
        c = j // blocks
        e = lax.rem(j, blocks)
        return copy(ed.at[pl.ds(PER * e, PER), :, pl.ds(pl.multiple_of(c * COLS, COLS), COLS)], dbuf.at[slot], dsem.at[slot])

    def sdown_copy(c, i, slot):
        at = pl.multiple_of((2 * c + i) * COLS, COLS)
        return copy(sd.at[:, :, pl.ds(at, COLS)], dbuf.at[slot, pl.ds(2 * i, 2)], ssem.at[slot, i])

    def remote(src, dst, send, recv, dev):
        return pltpu.make_async_remote_copy(src_ref=src, dst_ref=dst, send_sem=send, recv_sem=recv,
                                            device_id=dev, device_id_type=pl.DeviceIdType.MESH)

    per_buf = inter // wide
    q_view = []
    for i in range(Q_PARTS):
        if i < 2 * per_buf:
            q_view.append(wbuf.at[pl.ds(2 + 2 * (i // per_buf), 2), :, pl.ds((i % per_buf) * wide, wide)])
        else:
            q_view.append(act.at[:, :, pl.ds(q_wide + (i - 2 * per_buf) * wide, wide)])
    q_copies = [copy((wq if i < 2 * per_buf else wq3).at[..., pl.ds(i * wide, wide)], q_view[i], qsem.at[i])
                for i in range(Q_PARTS)]
    uk_view = [wbuf.at[pl.ds(2 + 2 * i, 2), :, pl.ds(per_buf * wide, lat // 2)] for i in range(2)]
    uk_copies = [copy(wuk.at[:, :, pl.ds(i * (lat // 2), lat // 2)], uk_view[i], asem.at[i]) for i in range(2)]
    uv_copies = [copy(wuv.at[:, :, i], outc.at[:, :, :, pl.ds(i * vh, vh)], asem.at[2 + i]) for i in range(2)]
    dkv_copies = [copy(wdkv.at[pl.ds(0, lat)], xall.at[0], asem.at[4]),
                  copy(wdkv.at[pl.ds(lat, rot)], xall.at[1, pl.ds(0, rot)], asem.at[5])]
    o_copy = copy(wo, xall, asem.at[6])
    x_copy = copy(x_hbm, y_ref, asem.at[7])
    x_copy.start()
    for c in dkv_copies + uk_copies + q_copies[:3]:
        c.start()
    later = q_copies[3:] + [c_copy(i) for i in range(SLOTS)] + uv_copies + [copy(wo.at[0], xall.at[0], asem.at[6])]

    lane = lax.broadcasted_iota(jnp.int32, (bsz, LANES), 1)
    low = lane < rot
    front = lax.rem(lane, rot) < rot // 2

    with jax.named_scope('norm'):
        x_copy.wait()
        x = y_ref[...].astype(f32)
        xn = (x * lax.rsqrt(jnp.mean(x * x, axis=-1, keepdims=True) + EPS)).astype(bf16)
        turn_i = lax.broadcasted_iota(jnp.int32, (rot // 2, bsz), 0).astype(f32)
        ang = jnp.exp(turn_i * (-2.0 / rot * 9.210340371976184)) * pos_ref[...].astype(f32)
        cos_t = jnp.cos(ang)
        sin_t = jnp.sin(ang)
        cos = jnp.concatenate([cos_t] * 4, axis=COL).T
        sin = jnp.concatenate([-sin_t, sin_t] * 2, axis=COL).T
        r2[7, :, :LANES] = jnp.broadcast_to(pos_ref[...].astype(f32), (bsz, bsz)).T
        meta[...] = jnp.zeros(meta.shape, f32)
        meta[:top, :] = ids_ref[...].astype(f32)
        meta[8:8 + top, :] = rw_ref[...]

    def turn(r):
        swap = jnp.where(front, pltpu.roll(r, LANES - rot // 2, 1), pltpu.roll(r, rot // 2, 1))
        return (r * cos + swap * sin).astype(bf16).astype(f32)

    with jax.named_scope('kv_phase'):
        for c in dkv_copies:
            c.wait()
        c = dot_t(xn, xall[0])
        r = dot_t(xn, xall[1, :rot, :])
        later.pop(0).start()
        c = (c * lax.rsqrt(jnp.mean(c * c, axis=-1, keepdims=True) + EPS)).astype(bf16).astype(f32)
        r = turn(jnp.concatenate([r, jnp.zeros((bsz, LANES - rot), f32)], axis=ROW))
        r2[4] = c[:, :COLS]
        r2[5] = c[:, COLS:]
        r2[6, :, :LANES] = r
        kv_ref[:lat, :] = c.T.astype(bf16)
        kv_ref[lat:, :] = r.T[:rot, :].astype(bf16)

    with jax.named_scope('q_phase'):
        for c in uk_copies:
            c.wait()
        def project_q(i):
            q_copies[i].wait()
            later.pop(0).start()
            return dot(xn, q_view[i][...].reshape(hid, wide)).astype(bf16).astype(f32)

        def place(i, q):
            for j in range(wide // (2 * qkd)):
                at = 2 * qkd * j
                h = i * (wide // qkd) + 2 * j
                mid = q[:, at + nope:at + 2 * nope]
                last = q[:, at + 2 * nope:at + 3 * nope]
                n_a = q[:, at:at + nope]
                n_b = jnp.where(low, pltpu.roll(mid, rot, 1), pltpu.roll(last, rot, 1))
                r = turn(jnp.where(low, mid, last))
                other = pltpu.roll(r, rot, 1)
                pair = []
                for k, n, z in ((0, n_a, jnp.where(low, r, other)), (1, n_b, jnp.where(low, other, r))):
                    uk = jnp.concatenate([v[(h + k) * nope // deep, pl.ds((h + k) * nope % deep, nope), :] for v in uk_view], axis=ROW)
                    ql = jnp.concatenate([dot(n.astype(bf16), uk), z], axis=ROW)
                    pair.append(ql.reshape(steps, GROUP, q_wide))
                act[:, pl.ds(h * GROUP, 2 * GROUP), :q_wide] = jnp.concatenate(pair, axis=ROW).astype(bf16)

        q = project_q(0)
        for i in range(Q_PARTS):
            then = project_q(i + 1) if i + 1 < Q_PARTS else None
            place(i, q)
            q = then
        for c in later:
            c.start()

    def ahead_copy(j):
        at = pl.ds(pl.multiple_of(j * piece, piece), piece)
        k = j // 2
        to = pl.ds(pl.multiple_of(lax.rem(j, 2) * piece, piece), piece)
        copy(sg.at[at, pl.ds(0, inter)], wbuf.at[k, to], wsem.at[k]).start()
        copy(su.at[at, pl.ds(0, inter)], wbuf.at[2 + k, to], wsem.at[2 + k]).start()

    row = lax.rem(lax.broadcasted_iota(jnp.int32, (size, LANES), 0), GROUP)

    def spread(v, width):
        keep = [jnp.where(row == g, 1.0, 0.0).astype(bf16) for g in range(GROUP)]
        return jnp.concatenate([v[:, t * LANES:(t + 1) * LANES] * keep[g]
                                for g in range(GROUP) for t in range(width // LANES)], axis=ROW)

    def ahead(i):
        return pl.ds(pl.multiple_of(i * GROUP, GROUP), GROUP)

    def cached(i, g, first, count):
        return dbuf[lax.rem(i, SLOTS), g // 2, (g % 2) * kvd + first:(g % 2) * kvd + first + count, :]

    def scores(i, k):
        at = ahead(i)
        q = act[i, :, :q_wide]
        kv = jnp.concatenate([r2[4, at, :], r2[5, at, :], r2[6, at, :LANES]], axis=ROW)
        new = jnp.sum(q.astype(f32).reshape(heads, GROUP, q_wide) * kv[None], axis=2, keepdims=True)
        r2[2, :, k * LANES:(k + 1) * LANES] = jnp.broadcast_to(new.reshape(size, 1), (size, LANES))
        tail = q[:, lat:]
        pairs = [tail * jnp.where(row == 2 * j + lane // rot, 1.0, 0.0).astype(bf16) for j in range(GROUP // 2)]
        c = jnp.concatenate([cached(i, g, 0, lat) for g in range(GROUP)], axis=COL)
        r = jnp.concatenate([cached(i, g, lat, rot) for g in range(GROUP)], axis=COL)
        r2[k] = dot(spread(q[:, :lat], lat), c) + dot(jnp.concatenate(pairs, axis=ROW), r)

    def soften(i, k):
        col = lax.broadcasted_iota(jnp.int32, (GROUP, rows), 1).astype(f32)
        live = col < r2[7, ahead(i), :1]
        s_new = r2[2, :, k * LANES:k * LANES + 1] * scale
        s = (r2[k] * scale).reshape(heads, GROUP, rows)
        s = jnp.where(live[None], s, -jnp.inf).reshape(size, rows)
        mx = jnp.maximum(jnp.max(s, axis=ROW, keepdims=True), s_new)
        e = jnp.exp(s - mx)
        e_new = jnp.exp(s_new - mx)
        inv = 1.0 / (jnp.sum(e, axis=ROW, keepdims=True) + e_new)
        sact[k, :, :rows] = (e * inv).astype(bf16)
        r2[3, :, k * LANES:(k + 1) * LANES] = jnp.broadcast_to((e_new * inv).astype(bf16).astype(f32), (size, LANES))

    def mix(i, k):
        at = ahead(i)
        c = jnp.concatenate([cached(i, g, 0, lat) for g in range(GROUP)], axis=ROW)
        o = dot_t(spread(sact[k, :, :rows], rows), c)
        p_new = r2[3, :, k * LANES:(k + 1) * LANES]
        p_new = jnp.concatenate([p_new, p_new], axis=ROW)
        for t in range(2):
            new = jnp.concatenate([r2[4 + t, at, :]] * heads, axis=COL)
            ot = o[:, t * COLS:(t + 1) * COLS] + p_new * new
            for h in range(heads):
                part[h // 2, 2 * (h % 2) + t, at, :] = ot[h * GROUP:(h + 1) * GROUP, :]

    m_across = remote(meta, mall.at[1], ms_send.at[1], ms_recv.at[1], across)
    u_across = [remote(ub.at[pl.ds(i * half, half)], uall.at[1, pl.ds(i * half, half)],
                       us_send.at[1 + i], us_recv.at[1 + i], across) for i in range(2)]
    m_partner = remote(meta, mall.at[0], ms_send.at[0], ms_recv.at[0], partner)
    u_partner = remote(ub, uall.at[0], us_send.at[0], us_recv.at[0], partner)
    m_relay = remote(mall.at[1], mall.at[2], ms_send.at[2], ms_recv.at[2], partner)
    u_relay = [remote(uall.at[1, pl.ds(i * half, half)], uall.at[2, pl.ds(i * half, half)],
                      us_send.at[3 + i], us_recv.at[3 + i], partner) for i in range(2)]

    def project(i):
        at = slice(i * half, (i + 1) * half)
        if i == 0:
            for c in uv_copies:
                c.wait()
            o_copy.wait()
        for h in range(heads):
            o = jnp.concatenate([part[h // 2, 2 * (h % 2) + t, at, :] for t in range(2)], axis=ROW).astype(bf16)
            g = h // 2
            ub[at, h * vh:(h + 1) * vh] = dot(o, outc[g // 4, g % 4, :, (h % 2) * vh:(h % 2 + 1) * vh]).astype(bf16)
        a = dot(ub[at, :], xall[...].reshape(hid, hid))
        h1 = (y_ref[at, :].astype(f32) + a).astype(bf16)
        h = h1.astype(f32)
        ub[at, :] = (h * lax.rsqrt(jnp.mean(h * h, axis=-1, keepdims=True) + EPS)).astype(bf16)
        y_ref[at, :] = h1
        if i == 0:
            pl.semaphore_wait(barrier, 2)
            m_across.start()
            m_partner.start()
        u_across[i].start()
        if i == 1:
            u_partner.start()

    with jax.named_scope('attend_loop'):
        for i in range(2):
            c_copy(i).wait()
            scores(i, i)
        soften(0, 0)

        def attend(j, _):
            for k in (1, 0):
                c_copy(2 * j + 3 - k).wait()
            for k in (1, 0):
                i = 2 * j + 2 - k
                mix(i - 1, 1 - k)
                soften(i, k)
                scores(i + 1, 1 - k)

            @pl.when(2 * j + 1 + SLOTS < steps)
            def _():
                for k in range(2):
                    c_copy(2 * j + k + SLOTS).start()

            @pl.when(2 * j + 1 + SLOTS >= steps)
            def _():
                for k in range(2):
                    free = lax.rem(2 * j + k, SLOTS)
                    down_copy(free, free).start()

            @pl.when(j < 3)
            def _():
                copy(wo.at[j + 1], xall.at[j + 1], asem.at[6]).start()

            @pl.when(j >= 3)
            def _():
                ahead_copy(j - 3)

            @pl.when(j == steps // 4 - 1)
            def _():
                project(0)
            return 0

        lax.fori_loop(0, steps // 2 - 1, attend, 0)
        for c in s_copy(sg, 1, 2):
            c.start()
        mix(steps - 2, 0)
        soften(steps - 1, 1)
        mix(steps - 1, 1)
        for k in (2, 1):
            down_copy((steps - k) % SLOTS, (steps - k) % SLOTS).start()

    with jax.named_scope('out_phase'):
        project(1)

    cuts = [(c * COLS, min(COLS, inter - c * COLS)) for c in range((inter + 255) // COLS)]

    def glu(lhs, dst, g_slot, u_slot, g_copy, u_copy, g_next, u_next):
        def gate(n, at, w):
            return part.at[n // 4, n % 4, :, pl.ds(0, w)]

        g_copy[0].wait()
        g = dot(lhs(0), wbuf[2 * g_slot])
        for n, (at, w) in enumerate(cuts):
            gate(n, at, w)[...] = g[:, at:at + w]
        g_next(0)
        g_copy[1].wait()
        g = dot(lhs(1), wbuf[2 * g_slot + 1])
        for n, (at, w) in enumerate(cuts):
            gate(n, at, w)[...] += g[:, at:at + w]
        g_next(1)
        u_copy[0].wait()
        v = dot(lhs(0), wbuf[2 * u_slot])
        for n, (at, w) in enumerate(cuts):
            part[2 + n // 4, n % 4, :, :w] = v[:, at:at + w]
        u_next(0)
        u_copy[1].wait()
        v = dot(lhs(1), wbuf[2 * u_slot + 1])
        v = v + jnp.concatenate([part[2 + n // 4, n % 4, :, :w] for n, (at, w) in enumerate(cuts)], axis=ROW)
        g = jnp.concatenate([gate(n, at, w)[...] for n, (at, w) in enumerate(cuts)], axis=ROW)
        dst[...] = (jax.nn.silu(g) * v).astype(bf16)
        u_next(1)

    with jax.named_scope('shared_up'):
        def mine(k):
            return ub[:, k * deep:(k + 1) * deep]

        glu(mine, sact.at[0], 0, 1, s_copy(sg, 0, 0), s_copy(su, 0, 1),
            lambda k: s_copy(su, 1, 0)[k].start(), lambda k: e_copy(eg, 0, 1)[k].start())
        glu(mine, sact.at[1], 2, 0, s_copy(sg, 1, 2), s_copy(su, 1, 0),
            lambda k: e_copy(eu, 0, 2)[k].start(), lambda k: e_copy(eg, 1, 0)[k].start())

    with jax.named_scope('half_wait'):
        m_across.wait_recv()
        m_relay.start()
        u_across[0].wait_recv()
        u_relay[0].start()

    def dispatch(q, m, u):
        first = (me * n_loc).astype(f32)
        mine = lax.broadcasted_iota(jnp.int32, (n_loc, bsz), 0).astype(f32) + first
        hit = jnp.zeros((n_loc, bsz), f32)
        wgt = jnp.zeros((n_loc, bsz), f32)
        for k in range(top):
            eq = m[k:k + 1, :] == mine
            hit = jnp.where(eq, 1.0, hit)
            wgt = jnp.where(eq, m[8 + k:9 + k, :], wgt)
        r = lax.broadcasted_iota(jnp.int32, (bsz, bsz), 0)
        c = lax.broadcasted_iota(jnp.int32, (bsz, bsz), 1)
        before = jnp.where(r < c, 1.0, 0.0).astype(bf16)
        rank = jnp.where(hit > 0.0, dot(hit.astype(bf16), before), -1.0)
        slot = lax.broadcasted_iota(jnp.int32, (CAP, bsz), 0).astype(f32)
        sel = []
        ct = []
        for e in range(n_loc):
            at = slot == rank[e:e + 1, :]
            sel.append(jnp.where(at, 1.0, 0.0).astype(bf16))
            ct.append(jnp.where(at, wgt[e:e + 1, :], 0.0))
        c0 = jnp.concatenate(ct, axis=COL).T
        for i in range(3):
            ci = c0.astype(bf16)
            comb[q, pl.ds(i * bsz, bsz), :] = ci
            c0 = c0 - ci.astype(f32)
        xall[q] = dot(jnp.concatenate(sel, axis=COL), u).astype(bf16)

    with jax.named_scope('disp01'):
        dispatch(OWN, meta[...], ub[...])
        m_partner.wait_recv()
        u_partner.wait_recv()
        dispatch(NEAR, mall[0], uall[0])
    with jax.named_scope('gather_wait'):
        u_across[1].wait_recv()
        u_relay[1].start()
    with jax.named_scope('disp2'):
        dispatch(ACROSS, mall[1], uall[1])
    with jax.named_scope('relay_wait'):
        m_relay.wait_recv()
        for i in range(2):
            u_relay[i].wait_recv()
    with jax.named_scope('disp3'):
        dispatch(FAR, mall[2], uall[2])

    def expert(e, _):
        g_slot = lax.rem(4 + 2 * e, RING)
        u_slot = lax.rem(5 + 2 * e, RING)

        def lhs(k):
            at = pl.ds(pl.multiple_of(e * CAP, CAP), CAP)
            return xall[:, at, k * deep:(k + 1) * deep].reshape(4 * CAP, deep)

        def g_next(k):
            @pl.when(e + 1 < n_loc)
            def _():
                e_copy(eu, e + 1, g_slot)[k].start()

        def u_next(k):
            @pl.when(e + 2 < n_loc)
            def _():
                e_copy(eg, e + 2, u_slot)[k].start()

        glu(lhs, act.at[e], g_slot, u_slot, e_copy(eg, e, g_slot), e_copy(eu, e, u_slot), g_next, u_next)
        return 0

    with jax.named_scope('experts'):
        lax.fori_loop(0, n_loc, expert, 0)

    def ring1(c, i):
        return remote(part.at[c, i], r1.at[c, LAND[i]], s1_send.at[c, LAND[i]], s1_recv.at[c, LAND[i]], partner)

    def ring2(c):
        return remote(part.at[c, ACROSS], r2.at[c], s2_send.at[c], s2_recv.at[c], across)

    def fold(c):
        ring1(c, FAR).wait_recv()
        part[c, ACROSS] = part[c, ACROSS] + r1[c, LAND[FAR]]

    def combine(c, q):
        p = dot(comb[q], outc[lax.rem(c, 2), q])
        part[c, q] = p[:bsz] + p[bsz:2 * bsz] + p[2 * bsz:]

    def down_step(c, e, early):
        j = c * blocks + e
        slot = lax.rem(j, SLOTS)
        down_copy(j, slot).wait()
        if early is not None:
            early()
        for i in range(PER):
            res = dot(act[PER * e + i], dbuf[slot, i]).astype(bf16)
            outc[lax.rem(c, 2), :, pl.ds(pl.multiple_of((PER * e + i) * CAP, CAP), CAP), :] = res.reshape(4, CAP, COLS)

        @pl.when(j + SLOTS < n_down)
        def _():
            down_copy(j + SLOTS, slot).start()

        @pl.when((j + SLOTS >= n_down) & (j + SLOTS < n_down + n_col // 2))
        def _():
            for i in range(2):
                sdown_copy(j + SLOTS - n_down, i, slot).start()

    def first(e, _):
        down_step(0, e, None)
        return 0

    def column(c, _):
        def step(e, _):
            @pl.when(e == 1)
            def _():
                ring1(c - 1, FAR).start()

            @pl.when(e == jnp.where(c == n_col - 1, 2, 3))
            def _():
                ring2(c - 1).start()

            @pl.when(e == 3)
            def _():
                ring1(c - 1, NEAR).start()

            down_step(c, e, lambda: combine(c - 1, e))

            @pl.when(e == jnp.where(c == n_col - 1, 1, 2))
            def _():
                fold(c - 1)
            return 0

        lax.fori_loop(0, blocks, step, 0)
        return 0

    with jax.named_scope('column0'):
        lax.fori_loop(0, blocks, first, 0)
    with jax.named_scope('columns'):
        lax.fori_loop(1, n_col, column, 0)

    last = n_col - 1
    with jax.named_scope('combine'):
        combine(last, FAR)
        ring1(last, FAR).start()
        combine(last, ACROSS)
        combine(last, NEAR)
        combine(last, OWN)
        ring1(last, NEAR).start()

    with jax.named_scope('shared_down'):
        for c in range(n_col // 2):
            slot = (n_down + c) % SLOTS
            for i in range(2):
                sdown_copy(c, i, slot).wait()
            for i in range(2):
                part[2 * c + i, OWN] = (part[2 * c + i, OWN] + dot(sact[0], dbuf[slot, 2 * i])
                                        + dot(sact[1], dbuf[slot, 2 * i + 1]))
            if c == 0:
                fold(last)
                ring2(last).start()

    with jax.named_scope('tail'):
        for c in range(n_col):
            ring1(c, NEAR).wait_recv()
            ring2(c).wait_recv()
            at = slice(c * COLS, (c + 1) * COLS)
            y_ref[:, at] = (y_ref[:, at].astype(f32) + ((part[c, OWN] + r1[c, LAND[NEAR]]) + r2[c])).astype(bf16)

    for c in (m_across, *u_across, m_partner, u_partner, m_relay, *u_relay):
        c.wait_send()
    for c in range(n_col):
        ring1(c, FAR).wait_send()
        ring1(c, NEAR).wait_send()
        ring2(c).wait_send()


def settle(y_in, kv_in, y_ref, kv_ref, y_buf, kv_buf, in_sem, out_sem):
    rows = y_in.shape[0] // PER
    cut = [pl.ds(i * rows, rows) for i in range(PER)]
    legs = [(kv_in, kv_buf, kv_ref)] + [(y_in.at[at], y_buf.at[at], y_ref.at[at]) for at in cut]
    into = [pltpu.make_async_copy(a, b, in_sem.at[i]) for i, (a, b, _) in enumerate(legs)]
    away = [pltpu.make_async_copy(b, c, out_sem.at[i]) for i, (_, b, c) in enumerate(legs)]
    for c in into:
        c.start()
    for a, b in zip(into, away):
        a.wait()
        b.start()
    for c in away:
        c.wait()


def solution(mesh):
    tok_spec = P(('rep', 'ep'))
    row_spec = P(('rep', 'ep'), None)
    cache_spec = P(('rep', 'ep'), None, None)
    exp_spec = P('ep', None, None)

    def local(x, cache, lens, ids, rw, w_q, w_dkv, w_uk, w_uv, w_o, s_gate, s_up, s_down, e_gate, e_up, e_down):
        bsz, hid = x.shape
        heads, nope, lat = w_uk.shape
        rows, kvd = cache.shape[1:]
        vh = w_uv.shape[2]
        n_loc, _, inter = e_gate.shape
        n_col = hid // COLS
        bf16, f32 = jnp.bfloat16, jnp.float32
        vm = pl.BlockSpec(memory_space=pltpu.VMEM)
        hbm = pl.BlockSpec(memory_space=pl.ANY)
        dma = pltpu.SemaphoreType.DMA
        y, kv = pl.pallas_call(
            layer,
            out_shape=(jax.ShapeDtypeStruct((bsz, hid), bf16), jax.ShapeDtypeStruct((kvd, bsz), bf16)),
            in_specs=[hbm] + [vm] * 3 + [hbm] * 13,
            out_specs=(vm, vm),
            scratch_shapes=[
                pltpu.VMEM((2 * RING, hid // 2, inter), bf16),
                pltpu.VMEM((SLOTS, PER, inter, COLS), bf16),
                pltpu.VMEM((4, n_loc * CAP, hid), bf16),
                pltpu.VMEM((n_loc, 4 * CAP, inter), bf16),
                pltpu.VMEM((2, bsz, inter), bf16),
                pltpu.VMEM((2, 4, n_loc * CAP, COLS), bf16),
                pltpu.VMEM((4, 3 * bsz, n_loc * CAP), bf16),
                pltpu.VMEM((3, bsz, hid), bf16),
                pltpu.VMEM((3, 16, bsz), f32),
                pltpu.VMEM((16, bsz), f32),
                pltpu.VMEM((n_col, 4, bsz, COLS), f32),
                pltpu.VMEM((n_col, 2, bsz, COLS), f32),
                pltpu.VMEM((n_col, bsz, COLS), f32),
                pltpu.VMEM((bsz, hid), bf16),
                dma((2 * RING,)), dma((SLOTS,)), dma((SLOTS, 2)), dma((Q_PARTS,)), dma((8,)),
                dma((5,)), dma((5,)), dma((3,)), dma((3,)),
                dma((n_col, 2)), dma((n_col, 2)), dma((n_col,)), dma((n_col,)),
            ],
            compiler_params=pltpu.CompilerParams(
                collective_id=0, has_side_effects=True, vmem_limit_bytes=67043328),
            name='layer',
        )(x, lens[None, :], ids.T, rw.T, cache.transpose(0, 2, 1).reshape(bsz // 2, 2 * kvd, rows),
          w_q.reshape(2, hid // 2, w_q.shape[1]), w_q.reshape(n_loc, hid // n_loc, w_q.shape[1]), w_dkv.T, w_uk.reshape(2, heads * nope // 2, lat),
          w_uv.reshape(2, 4, 2, lat, vh), w_o.reshape(4, hid // 4, hid),
          s_gate, s_up, s_down.reshape(2, inter, hid), e_gate, e_up, e_down)
        y, kv = pl.pallas_call(
            settle,
            out_shape=(jax.ShapeDtypeStruct(y.shape, bf16), jax.ShapeDtypeStruct(kv.shape, bf16)),
            in_specs=[hbm, hbm],
            out_specs=(hbm, hbm),
            scratch_shapes=[pltpu.VMEM(y.shape, bf16), pltpu.VMEM(kv.shape, bf16), dma((PER + 1,)), dma((PER + 1,))],
            name='settle',
        )(y, kv)
        return y, kv.T

    in_specs = (row_spec, cache_spec, tok_spec, row_spec, row_spec) + (P(),) * 8 + (exp_spec,) * 3
    return jax.shard_map(local, mesh=mesh, in_specs=in_specs, out_specs=(row_spec, row_spec), check_vma=False)
```
